32 devices in a mesh: client: 8 (over z, x), head: 4 (over y, core).
Axes of the slice: x: 2, y: 2, z: 4, core: 2. Of those that a mesh axis runs over, the one named last changes fastest.
Arguments:
- pre: bfloat16 [10240, 4096], P('client'), may hold values from -40 to 40
- delta: float32 [10240, 4096], P('client', 'head'), may hold values from -300 to 300
- head_weight: bfloat16 [4096, 4096], P(None, 'head'), may hold values from -0.09375 to 0.09375
- client_ids: int32 [128], P('client'), may hold values from 0 to 127, as said below
Outputs:
- head_grad: float32 [4096, 4096], P('client', 'head')
- bias_grad: float32 [4096], P('head')
- embed_grad: float32 [128, 4096], P('client', 'head')
- span_grad: float32 [80, 4096], P(None, 'head')
The draws below stay inside these ranges and needn't reach their ends.
Inputs may be any that keep to these rules, and one draw needn't show every extreme that they name: `client_ids`: each of the 128 clients appears exactly once.
All inputs are finite; a program needn't handle non-finite values.
Results may differ from the reference program's by a relative error of at most 0.024.
Values may be sent and summed in bfloat16 or wider, within the bound.
A program may use at most 128 MiB of HBM per device.

```python
import jax
import jax.numpy as jnp
from jax import lax

HID = 4096
EMIT = 4096
SPANS = 80
CLIENTS = 128
ROWS = 10240
N_HEAD = 4


def shuffled_clients(key):
    return jax.random.permutation(jax.random.fold_in(key, 31), CLIENTS).astype(jnp.int32)


def draw_client_ids(key, part):
    return shuffled_clients(key)


def draw_pre(key, part):
    key_base = jax.random.fold_in(key, 11)
    key_level = jax.random.fold_in(key, 12)
    levels = jax.random.uniform(key_level, (HID,), jnp.float32, 0.0, 0.8)
    levels = levels + 0.48 * jnp.arange(HID, dtype=jnp.float32) / HID
    scales = 0.5 * 10.0 ** levels
    base = jnp.clip(jax.random.normal(key_base, (ROWS, HID), jnp.float32), -4.0, 4.0)
    return (base * scales[None, :]).astype(jnp.bfloat16)


def draw_delta(key, part):
    key_base = jax.random.fold_in(key, 21)
    key_rows = jax.random.fold_in(key, 22)
    key_cols = jax.random.fold_in(key, 23)
    owners = shuffled_clients(key).astype(jnp.float32) / CLIENTS
    col_levels = jax.random.uniform(key_cols, (EMIT,), jnp.float32, 0.0, 0.5)
    row_levels = jnp.repeat(owners, SPANS, total_repeat_length=ROWS)
    row_levels = row_levels + jax.random.uniform(key_rows, (ROWS,), jnp.float32, 0.0, 0.3)
    base = jnp.clip(jax.random.normal(key_base, (ROWS, EMIT), jnp.float32), -4.0, 4.0)
    values = base * (10.0 ** row_levels)[:, None] * (10.0 ** col_levels)[None, :]
    return values.astype(jnp.float32)


def shard_levels(stream_key, dims, shards, low, high):
    level, own = 1.0, jax.random.fold_in(stream_key, 6)
    for position, blocks in shards:
        heights = jnp.exp(jax.random.uniform(jax.random.fold_in(own, position), (blocks,), jnp.float32, low / len(shards), high / len(shards)))
        level = level * jnp.repeat(heights, dims[position] // blocks).reshape([-1 if axis == position else 1 for axis in range(len(dims))])
    return level


def gaussian(rng, shape, deviation, reach, cuts=(), kind=jnp.bfloat16):
    drawn = jax.random.normal(rng, shape, jnp.float32) * deviation
    if len(cuts) > 0:
        drawn = shard_levels(rng, shape, cuts, -0.22, 0.18) * drawn
    return jnp.clip(drawn, min=-reach, max=reach).astype(kind)


def setup_inputs(seed: int = 0) -> dict:
    key_of = jax.random.split(jax.random.key(seed), 5)
    pre = draw_pre(jax.random.fold_in(key_of[4], 71), 0)
    delta = draw_delta(jax.random.fold_in(key_of[4], 71), 0)
    head_weight = gaussian(key_of[2], (HID, EMIT), HID ** -0.5, 0.09375, ((1, 4),))
    client_ids = draw_client_ids(jax.random.fold_in(key_of[4], 71), 0)
    return {"pre": pre, "delta": delta, "head_weight": head_weight, "client_ids": client_ids}


def silu_slope(values):
    sigma = jax.nn.sigmoid(values)
    return sigma * (1.0 + values * (1.0 - sigma))

def clip_factor(total, number):
    return jnp.minimum(1.0, 1.0 / jnp.sqrt(total / number + 1e-06))

def reference(pre, delta, head_weight, client_ids):
    pre_wide = pre.astype(jnp.float32)
    hidden = jax.nn.silu(pre_wide).astype(jnp.bfloat16)
    delta_low = delta.astype(jnp.bfloat16)
    head_raw = jnp.dot(hidden.T, delta_low, preferred_element_type=jnp.float32)
    bias_raw = lax.optimization_barrier(jnp.sum(delta, axis=0))
    block = EMIT // N_HEAD
    hidden_grad = jnp.zeros((ROWS, HID), jnp.float32)
    for which in range(N_HEAD):
        partial_sum = jnp.dot(delta_low[:, which * block:(which + 1) * block], head_weight[:, which * block:(which + 1) * block].T, preferred_element_type=jnp.float32)
        rounded = lax.optimization_barrier(partial_sum.astype(jnp.bfloat16))
        hidden_grad = hidden_grad + rounded.astype(jnp.float32)
    pre_grad = hidden_grad * silu_slope(pre_wide)
    grouped = pre_grad.reshape(CLIENTS, SPANS, HID)
    client_part = lax.optimization_barrier(jnp.sum(grouped, axis=1))
    span_raw = lax.optimization_barrier(jnp.sum(grouped, axis=0))
    embed_raw = jnp.zeros((CLIENTS, HID), jnp.float32).at[client_ids.astype(jnp.int32)].add(client_part)
    head_factor = clip_factor(jnp.sum(head_raw * head_raw), HID * EMIT)
    embed_factor = clip_factor(jnp.sum(embed_raw * embed_raw), CLIENTS * HID)
    rest_total = jnp.sum(span_raw * span_raw) + jnp.sum(bias_raw * bias_raw)
    rest_factor = clip_factor(rest_total, SPANS * HID + EMIT)
    return (head_factor * head_raw, rest_factor * bias_raw, embed_factor * embed_raw, rest_factor * span_raw)
```

```python
import functools
import math

import jax
import jax.numpy as jnp
from jax import lax
from jax.experimental import pallas as pl
from jax.experimental.pallas import tpu as pltpu
from jax.sharding import PartitionSpec as P

EPSILON = 1e-06
MESH = pl.DeviceIdType.MESH
F32 = jnp.float32
BF16 = jnp.bfloat16


def clip_factor(total, number):
    return jnp.minimum(1.0, 1.0 / jnp.sqrt(total / number + EPSILON))


def kernel(cfg, pre_ref, delta_ref, weight_ref, ids_ref, head_out, rest_out, embed_out, stat_out,
           pre_v, delta_v, low, weight_v, part, pair_in, line_in, first_in, swap_in, head_v,
           small, small_in, mine, span_in, span_part, span_pair, span_all, embed_all, ids_all,
           stat, stat_in, stat_head_in,
           pre_sem, delta_sem, weight_sem, out_sem, pair_send, pair_recv, line_send, line_recv,
           first_send, first_recv, swap_sem, head_send, head_recv, span_send, span_recv, span_pair_sem,
           all_send, all_recv, embed_pair_sem, embed_send, embed_recv, ids_sem, ids_send, ids_recv,
           stat_send, stat_recv):
    n, heads, block, piece, spans, clients = cfg
    zs = n // 2
    q = 7
    sub = block // (q + 1)
    hq = block // piece
    rows, emit = low.shape
    me = lax.axis_index("client")
    my_head = lax.axis_index("head")
    z = me // 2
    x = me % 2
    relays = (zs - 1) * q

    barrier = pltpu.get_barrier_semaphore()
    for d in range(1, n):
        pl.semaphore_signal(barrier, inc=1, device_id={"client": lax.rem(me + d, n)}, device_id_type=MESH)
    for d in range(1, heads):
        pl.semaphore_signal(barrier, inc=1, device_id={"head": lax.rem(my_head + d, heads)}, device_id_type=MESH)

    after_first = (z + zs - 1) // zs
    before_last = (2 * zs - 2 - z) // zs
    middle = after_first * before_last
    upper = 2 * z // zs
    near = z + upper * (zs - 1 - 2 * z)

    def dest(k):
        both = (2 * near - k - 1 + zs) // zs
        odd = k % 2
        out = both * (odd * (k // 2) + (1 - odd) * (zs - 1 - k // 2)) + (1 - both) * (zs - 1 - k + near)
        return out + upper * (zs - 1 - 2 * out)

    def block_row(place, side):
        return (place * 2 + side) * block

    def piece_row(place, side, s):
        return pl.multiple_of(block_row(place, side) + (s + 1) * sub, sub)

    def landing(place):
        right = (place - z + zs) // zs
        target = z + 2 * right - 1
        gap = right * (place - target) + (1 - right) * (target - place)
        away = (gap + zs - 1) // zs
        slot = away * place + (1 - away) * (zs + 1 - right)
        return target * 2 + x, slot

    partner = z * 2 + 1 - x

    def unit_side(u):
        return (x + 1 - u % 2) % 2

    def unit_row(u):
        return pl.multiple_of(block_row(dest(u // 2), unit_side(u)), block)

    def pre_copy(u, h):
        columns = pl.ds(pl.multiple_of(unit_row(u) + h * piece, piece), piece)
        return pltpu.make_async_copy(
            pre_ref.at[:, columns], pre_v.at[u, :, pl.ds(pl.multiple_of(h * piece, piece), piece)],
            pre_sem.at[u * hq + h])

    chunk = math.gcd(rows, 256)
    delta_copies = [
        pltpu.make_async_copy(delta_ref.at[pl.ds(c * chunk, chunk), :], delta_v.at[pl.ds(c * chunk, chunk), :],
                              delta_sem.at[c])
        for c in range(rows // chunk)]
    weight_copy = pltpu.make_async_copy(weight_ref, weight_v, weight_sem)
    ids_copy = pltpu.make_async_copy(ids_ref, ids_all.at[me], ids_sem)
    pre_copy(0, 0).start()
    for copy in delta_copies:
        copy.start()
    ids_copy.start()
    def load(u, carry):
        @pl.when(u > 0)
        def _():
            pre_copy(u, 0).start()
        return carry
    lax.fori_loop(0, 2 * zs, load, 0)
    def load_rest(u, carry):
        for h in range(1, hq):
            pre_copy(u, h).start()
        return carry
    lax.fori_loop(0, 2 * zs, load_rest, 0)
    weight_copy.start()

    line_in[z * q] = jnp.zeros((sub, emit), BF16)
    first_in[z * 2] = jnp.zeros((sub, emit), BF16)

    step = 64
    bias = jnp.zeros((8, emit), F32)
    for c, copy in enumerate(delta_copies):
        copy.wait()
        def narrow(r, total):
            at = pl.ds(pl.multiple_of(c * chunk + r * step, step), step)
            value = delta_v[at, :]
            low[at, :] = value.astype(BF16)
            return total + jnp.sum(value.reshape(step // 8, 8, emit), axis=0)
        bias = lax.fori_loop(0, chunk // step, narrow, bias)
    bias = jnp.sum(bias, axis=0, keepdims=True)
    half = emit // 2
    pad = mine.shape[1] - spans
    tail = jnp.where(
        lax.broadcasted_iota(jnp.int32, (pad, emit), 0) == 0, jnp.broadcast_to(bias, (pad, emit)), 0.0
    ).astype(BF16)
    for h in range(2):
        mine[h, pl.ds(spans, pad), :] = tail[:, h * half:(h + 1) * half]

    pl.semaphore_wait(barrier, n - 1 + heads - 1)

    def product(u, h):
        p = pre_v[u, :, pl.ds(pl.multiple_of(h * piece, piece), piece)].astype(F32)
        hidden = (p * jax.nn.sigmoid(p)).astype(BF16)
        value = lax.dot_general(hidden, low[...], (((0,), (0,)), ((), ())), preferred_element_type=F32)
        part[pl.ds(pl.multiple_of(unit_row(u) + h * piece, piece), piece), :] = value.astype(BF16)

    def slope_sums(t):
        u = t // hq
        h = t % hq
        p = pre_v[u, :, pl.ds(pl.multiple_of(h * piece, piece), piece)].astype(F32)
        row = pl.multiple_of(unit_row(u) + h * piece, piece)
        value = lax.dot_general(
            low[...], weight_v[pl.ds(row, piece), :], (((1,), (1,)), ((), ())), preferred_element_type=F32)
        s = jax.nn.sigmoid(p)
        grad = value.astype(BF16).astype(F32) * (s * (1.0 + p * (1.0 - s)))
        grad = grad.reshape(clients, spans, piece)
        to = row // emit
        columns = pl.ds(pl.multiple_of(row % emit, piece), piece)
        small[to, pl.ds(0, spans), columns] = jnp.sum(grad, axis=0).astype(BF16)
        small[to, pl.ds(spans, clients), columns] = jnp.sum(grad, axis=1).astype(BF16)

    def pair_copy(i):
        return pltpu.make_async_remote_copy(
            src_ref=part.at[pl.ds(piece_row(dest(i // q), 1 - x, i % q), sub), :], dst_ref=pair_in.at[i],
            send_sem=pair_send.at[i], recv_sem=pair_recv.at[i],
            device_id={"client": partner}, device_id_type=MESH)

    def line_copy(i):
        place = dest(i // q)
        target, slot = landing(place)
        return pltpu.make_async_remote_copy(
            src_ref=part.at[pl.ds(piece_row(place, x, i % q), sub), :], dst_ref=line_in.at[slot * q + i % q],
            send_sem=line_send.at[i], recv_sem=line_recv.at[slot * q + i % q],
            device_id={"client": target}, device_id_type=MESH)

    def arrival(slot):
        return pltpu.make_async_remote_copy(
            src_ref=part.at[pl.ds(0, sub), :], dst_ref=line_in.at[slot], send_sem=line_send.at[0],
            recv_sem=line_recv.at[slot], device_id={"client": partner}, device_id_type=MESH)

    lead = q
    queue = 4
    slopes = 2 * zs * hq
    paced = slopes // 2 + 1
    step_rows = min(32, sub)

    def relay(i):
        place = dest(i // q)
        row = piece_row(place, x, i % q)
        pair_copy(i).wait_recv()
        @pl.when(middle == 1)
        def _():
            arrival(place * q + i % q).wait_recv()
        slot = middle * (place * q + i % q) + (1 - middle) * z * q
        def add(r, carry):
            at = pl.ds(pl.multiple_of(r * step_rows, step_rows), step_rows)
            mine_at = pl.ds(pl.multiple_of(row + r * step_rows, step_rows), step_rows)
            total = part[mine_at, :].astype(F32) + pair_in[i, at, :].astype(F32)
            part[mine_at, :] = (total + line_in[slot, at, :].astype(F32)).astype(BF16)
            return carry
        lax.fori_loop(0, sub // step_rows, add, 0)
        @pl.when(i >= paced)
        def _():
            line_copy(i - queue).wait_send()
        line_copy(i).start()
        @pl.when(i + lead < zs * q)
        def _():
            pair_copy(i + lead).start()

    def relay_range(start, stop):
        def body(i, carry):
            relay(i)
            return carry
        if stop > start:
            lax.fori_loop(start, stop, body, 0)

    def finish(s, square):
        i = relays + s
        row = piece_row(z, x, s)
        pair_copy(i).wait_recv()
        @pl.when(after_first == 1)
        def _():
            arrival(zs * q + s).wait_recv()
        @pl.when(before_last == 1)
        def _():
            arrival((zs + 1) * q + s).wait_recv()
        left = after_first * (zs * q + s) + (1 - after_first) * z * q
        right = before_last * ((zs + 1) * q + s) + (1 - before_last) * z * q
        def add(r, carry):
            at = pl.ds(pl.multiple_of(r * step_rows, step_rows), step_rows)
            mine_at = pl.ds(pl.multiple_of(row + r * step_rows, step_rows), step_rows)
            out_at = pl.ds(pl.multiple_of((s + 1) * sub + r * step_rows, step_rows), step_rows)
            total = part[mine_at, :].astype(F32) + pair_in[i, at, :].astype(F32)
            total = total + line_in[left, at, :].astype(F32) + line_in[right, at, :].astype(F32)
            head_v[out_at, :] = total
            return carry + jnp.sum((total * total).reshape(step_rows // 8, 8, emit), axis=0)
        square = lax.fori_loop(0, sub // step_rows, add, square)
        pltpu.make_async_copy(
            head_v.at[pl.ds(pl.multiple_of((s + 1) * sub, sub), sub), :],
            head_out.at[pl.ds(pl.multiple_of((s + 1) * sub, sub), sub), :], out_sem.at[s + 1]).start()
        return square

    def first_copy(j):
        place = dest(j // 2)
        side = unit_side(j)
        target, slot = landing(place)
        return pltpu.make_async_remote_copy(
            src_ref=part.at[pl.ds(pl.multiple_of(block_row(place, side), sub), sub), :],
            dst_ref=first_in.at[slot * 2 + side],
            send_sem=first_send.at[j], recv_sem=first_recv.at[slot * 2 + side],
            device_id={"client": target}, device_id_type=MESH)

    def first_arrival(slot):
        return pltpu.make_async_remote_copy(
            src_ref=part.at[pl.ds(0, sub), :], dst_ref=first_in.at[slot], send_sem=first_send.at[0],
            recv_sem=first_recv.at[slot], device_id={"client": partner}, device_id_type=MESH)

    def first_relay(j):
        @pl.when(middle == 1)
        def _():
            place = dest(j // 2)
            side = unit_side(j)
            row = pl.multiple_of(block_row(place, side), sub)
            first_arrival(place * 2 + side).wait_recv()
            def add(r, carry):
                at = pl.ds(pl.multiple_of(r * step_rows, step_rows), step_rows)
                mine_at = pl.ds(pl.multiple_of(row + r * step_rows, step_rows), step_rows)
                part[mine_at, :] = (
                    part[mine_at, :].astype(F32) + first_in[place * 2 + side, at, :].astype(F32)).astype(BF16)
                return carry
            lax.fori_loop(0, sub // step_rows, add, 0)
            first_copy(j).start()

    swap_copy = pltpu.make_async_remote_copy(
        src_ref=part.at[pl.ds(pl.multiple_of(block_row(z, 1 - x), sub), sub), :], dst_ref=swap_in,
        send_sem=swap_sem.at[0], recv_sem=swap_sem.at[1], device_id={"client": partner}, device_id_type=MESH)

    def first_wait(side):
        @pl.when(after_first == 1)
        def _():
            first_arrival(zs * 2 + side).wait_recv()
        @pl.when(before_last == 1)
        def _():
            first_arrival((zs + 1) * 2 + side).wait_recv()
        left = after_first * (zs * 2 + side) + (1 - after_first) * z * 2
        right = before_last * ((zs + 1) * 2 + side) + (1 - before_last) * z * 2
        return left, right

    def first_swap():
        row = block_row(z, 1 - x)
        left, right = first_wait(1 - x)
        def add(r, carry):
            at = pl.ds(pl.multiple_of(r * step_rows, step_rows), step_rows)
            mine_at = pl.ds(pl.multiple_of(row + r * step_rows, step_rows), step_rows)
            total = part[mine_at, :].astype(F32) + first_in[left, at, :].astype(F32)
            part[mine_at, :] = (total + first_in[right, at, :].astype(F32)).astype(BF16)
            return carry
        lax.fori_loop(0, sub // step_rows, add, 0)
        swap_copy.start()

    def first_finish(square):
        row = block_row(z, x)
        left, right = first_wait(x)
        swap_copy.wait_recv()
        def add(r, carry):
            at = pl.ds(pl.multiple_of(r * step_rows, step_rows), step_rows)
            mine_at = pl.ds(pl.multiple_of(row + r * step_rows, step_rows), step_rows)
            total = part[mine_at, :].astype(F32) + first_in[left, at, :].astype(F32)
            total = total + first_in[right, at, :].astype(F32) + swap_in[at, :].astype(F32)
            head_v[at, :] = total
            return carry + jnp.sum((total * total).reshape(step_rows // 8, 8, emit), axis=0)
        square = lax.fori_loop(0, sub // step_rows, add, square)
        pltpu.make_async_copy(head_v.at[pl.ds(0, sub), :], head_out.at[pl.ds(0, sub), :], out_sem.at[0]).start()
        return square

    ready = piece // sub - 1

    def opening(u, carry):
        pre_copy(u, 0).wait()
        product(u, 0)
        @pl.when(middle == 0)
        def _():
            first_copy(u).start()
        @pl.when(u == 0)
        def _():
            for i in range(ready):
                pair_copy(i).start()
        return carry
    lax.fori_loop(0, 2 * (zs - 1), opening, 0)
    if hq > 1:
        def second(t, carry):
            pre_copy(t // (hq - 1), 1 + t % (hq - 1)).wait()
            product(t // (hq - 1), 1 + t % (hq - 1))
            return carry
        lax.fori_loop(0, 3 * (hq - 1), second, 0)
    def more_pairs(i, carry):
        pair_copy(i).start()
        return carry
    lax.fori_loop(ready, lead, more_pairs, 0)
    first_relay(0)
    first_relay(1)
    def loaded(u, carry):
        @pl.when(u >= 2 * zs - 2)
        def _():
            pre_copy(u, 0).wait()
        for h in range(1, hq):
            pre_copy(u, h).wait()
        return carry
    lax.fori_loop(3 if hq > 1 else 2 * zs - 2, 2 * zs, loaded, 0)
    weight_copy.wait()

    ids_copy.wait()
    ids_copies = []
    for d in range(1, n):
        copy = pltpu.make_async_remote_copy(
            src_ref=ids_all.at[me], dst_ref=ids_all.at[me], send_sem=ids_send.at[d], recv_sem=ids_recv.at[me],
            device_id={"client": lax.rem(me + d, n)}, device_id_type=MESH)
        copy.start()
        ids_copies.append(copy)

    firsts = 2 * (zs - 1)
    def main(t, carry):
        slope_sums(t)
        @pl.when((t % 3 == 0) & (2 + t // 3 < firsts))
        def _():
            first_relay(2 + t // 3)
        @pl.when(t % 2 == 1)
        def _():
            relay(t // 2)
        return carry
    lax.fori_loop(0, slopes, main, 0)

    head_copies = []
    for d in range(1, heads):
        target = lax.rem(my_head + d, heads)
        copy = pltpu.make_async_remote_copy(
            src_ref=small.at[target], dst_ref=small_in.at[my_head],
            send_sem=head_send.at[d], recv_sem=head_recv.at[my_head],
            device_id={"head": target}, device_id_type=MESH)
        copy.start()
        head_copies.append(copy)

    done = 2 + (slopes + 2) // 3
    if done < firsts:
        def rest_first(j, carry):
            first_relay(j)
            return carry
        lax.fori_loop(done, firsts, rest_first, 0)

    at = slopes // 2
    if hq > 1:
        def third(t, carry):
            product(3 + t // (hq - 1), 1 + t % (hq - 1))
            return carry
        lax.fori_loop(0, (2 * zs - 5) * (hq - 1), third, 0)
    relay_range(at, at + 1)
    def fourth(t, carry):
        product(2 * zs - 2 + t // hq, t % hq)
        return carry
    lax.fori_loop(0, 2 * hq, fourth, 0)
    first_swap()
    relay_range(at + 1, at + 4)
    at = at + 4
    stop = [at + (relays - at) * k // 9 for k in (4, 8, 9)]

    for d in range(1, heads):
        source = lax.rem(my_head + d, heads)
        pltpu.make_async_remote_copy(
            src_ref=small.at[0], dst_ref=small_in.at[source], send_sem=head_send.at[d],
            recv_sem=head_recv.at[source], device_id={"head": source}, device_id_type=MESH).wait_recv()
    total = small[my_head].astype(F32)
    for d in range(1, heads):
        total = total + small_in[lax.rem(my_head + d, heads)].astype(F32)
    for h in range(2):
        mine[h, pl.ds(0, spans), :] = total[:spans, h * half:(h + 1) * half].astype(BF16)
    embed_all[z, x] = total[spans:].astype(BF16)

    embed_pair = pltpu.make_async_remote_copy(
        src_ref=embed_all.at[z, x], dst_ref=embed_all.at[z, x], send_sem=embed_pair_sem.at[0],
        recv_sem=embed_pair_sem.at[1], device_id={"client": partner}, device_id_type=MESH)
    embed_pair.start()
    roots = [zs // 2 - 1, zs // 2]
    def span_copy(h):
        return pltpu.make_async_remote_copy(
            src_ref=mine.at[h], dst_ref=span_in.at[z], send_sem=span_send.at[h], recv_sem=span_recv.at[z],
            device_id={"client": roots[h] * 2 + x}, device_id_type=MESH)
    for h in range(2):
        @pl.when(z != roots[h])
        def _():
            span_copy(h).start()

    relay_range(at, stop[0])

    embed_pair.wait_recv()
    embed_copies = []
    for d in range(1, zs):
        copy = pltpu.make_async_remote_copy(
            src_ref=embed_all.at[z], dst_ref=embed_all.at[z], send_sem=embed_send.at[d], recv_sem=embed_recv.at[z],
            device_id={"client": lax.rem(z + d, zs) * 2 + x}, device_id_type=MESH)
        copy.start()
        embed_copies.append(copy)
    span_pair_copy = pltpu.make_async_remote_copy(
        src_ref=span_part, dst_ref=span_pair, send_sem=span_pair_sem.at[0], recv_sem=span_pair_sem.at[1],
        device_id={"client": partner}, device_id_type=MESH)
    for h in range(2):
        @pl.when(z == roots[h])
        def _():
            total = mine[h].astype(F32)
            for d in range(1, zs):
                source = (roots[h] + d) % zs
                pltpu.make_async_remote_copy(
                    src_ref=mine.at[h], dst_ref=span_in.at[source], send_sem=span_send.at[h],
                    recv_sem=span_recv.at[source], device_id={"client": partner}, device_id_type=MESH).wait_recv()
                total = total + span_in[source].astype(F32)
            span_part[...] = total.astype(BF16)
            span_pair_copy.start()

    relay_range(stop[0], stop[1])

    def all_copy(h, d):
        return pltpu.make_async_remote_copy(
            src_ref=span_all.at[h], dst_ref=span_all.at[h], send_sem=all_send.at[d], recv_sem=all_recv.at[h],
            device_id={"client": lax.rem(z + d, zs) * 2 + x}, device_id_type=MESH)
    for h in range(2):
        @pl.when(z == roots[h])
        def _():
            span_pair_copy.wait_recv()
            span_all[h] = (span_part[...].astype(F32) + span_pair[...].astype(F32)).astype(BF16)
            for d in range(1, zs):
                all_copy(h, d).start()

    relay_range(stop[1], relays)
    square = jnp.zeros((8, emit), F32)
    square = first_finish(square)
    square = lax.fori_loop(0, 3, finish, square)

    for d in range(1, n):
        source = lax.rem(me + d, n)
        pltpu.make_async_remote_copy(
            src_ref=ids_all.at[me], dst_ref=ids_all.at[source], send_sem=ids_send.at[d],
            recv_sem=ids_recv.at[source], device_id={"client": source}, device_id_type=MESH).wait_recv()
    for d in range(1, zs):
        source = lax.rem(z + d, zs)
        pltpu.make_async_remote_copy(
            src_ref=embed_all.at[z], dst_ref=embed_all.at[source], send_sem=embed_send.at[d],
            recv_sem=embed_recv.at[source], device_id={"client": source * 2 + x}, device_id_type=MESH).wait_recv()
    wanted = lax.broadcasted_iota(jnp.int32, (clients, clients), 0) + me * clients
    embed_raw = jnp.zeros((clients, emit), F32)
    for c in range(n):
        chosen = (jnp.broadcast_to(ids_all[c], (clients, clients)) == wanted).astype(F32).astype(BF16)
        embed_raw = embed_raw + jnp.dot(chosen, embed_all[c // 2, c % 2], preferred_element_type=F32)
    embed_out[...] = embed_raw
    embed_square = jnp.sum(embed_raw * embed_raw)

    rest_square = jnp.zeros((), F32)
    for h in range(2):
        @pl.when(z != roots[h])
        def _():
            all_copy(h, 1).wait_recv()
        value = span_all[h].astype(F32)
        rest_out[:, pl.ds(h * half, half)] = value
        rest_square = rest_square + jnp.sum(value * value)

    square = lax.fori_loop(3, q, finish, square)
    head_total = jnp.sum(square)

    line = lax.broadcasted_iota(jnp.int32, (8, 128), 0)
    stat[0] = jnp.where(line == 0, head_total, jnp.where(line == 1, embed_square, rest_square / n))
    copies = []
    for d in range(1, n):
        copy = pltpu.make_async_remote_copy(
            src_ref=stat.at[0], dst_ref=stat_in.at[me], send_sem=stat_send.at[d - 1],
            recv_sem=stat_recv.at[me], device_id={"client": lax.rem(me + d, n)}, device_id_type=MESH)
        copy.start()
        copies.append(copy)
    stat_in[me] = stat[0]
    for d in range(1, n):
        source = lax.rem(me + d, n)
        pltpu.make_async_remote_copy(
            src_ref=stat.at[0], dst_ref=stat_in.at[source], send_sem=stat_send.at[d - 1],
            recv_sem=stat_recv.at[source], device_id={"client": source}, device_id_type=MESH).wait_recv()
    total = stat_in[0]
    for c in range(1, n):
        total = total + stat_in[c]
    stat[1] = total
    stat_head_in[my_head] = total
    more = []
    for d in range(1, heads):
        copy = pltpu.make_async_remote_copy(
            src_ref=stat.at[1], dst_ref=stat_head_in.at[my_head], send_sem=stat_send.at[n - 2 + d],
            recv_sem=stat_recv.at[n + my_head], device_id={"head": lax.rem(my_head + d, heads)}, device_id_type=MESH)
        copy.start()
        more.append(copy)
    for d in range(1, heads):
        source = lax.rem(my_head + d, heads)
        pltpu.make_async_remote_copy(
            src_ref=stat.at[1], dst_ref=stat_head_in.at[source], send_sem=stat_send.at[n - 2 + d],
            recv_sem=stat_recv.at[n + source], device_id={"head": source}, device_id_type=MESH).wait_recv()
    total = stat_head_in[0]
    for c in range(1, heads):
        total = total + stat_head_in[c]
    stat_out[...] = total

    def pair_sent(i, carry):
        pair_copy(i).wait_send()
        return carry
    lax.fori_loop(0, zs * q, pair_sent, 0)
    def line_sent(i, carry):
        line_copy(i).wait_send()
        return carry
    lax.fori_loop(0, paced - queue, line_sent, 0)
    lax.fori_loop(relays - queue, relays, line_sent, 0)
    def first_sent(j, carry):
        first_copy(j).wait_send()
        return carry
    lax.fori_loop(0, firsts, first_sent, 0)
    swap_copy.wait_send()
    embed_pair.wait_send()
    for copy in head_copies + embed_copies + ids_copies + copies + more:
        copy.wait_send()
    for h in range(2):
        @pl.when(z != roots[h])
        def _():
            span_copy(h).wait_send()
        @pl.when(z == roots[h])
        def _():
            span_pair_copy.wait_send()
            for d in range(1, zs):
                all_copy(h, d).wait_send()
    def written(s, carry):
        at = pl.multiple_of(s * sub, sub)
        pltpu.make_async_copy(
            head_v.at[pl.ds(at, sub), :], head_out.at[pl.ds(at, sub), :], out_sem.at[s]).wait()
        return carry
    lax.fori_loop(0, q + 1, written, 0)


def scale_kernel(sizes, spans, stat_ref, head_ref, rest_ref, embed_ref, head_out, bias_out, embed_out, span_out):
    head_size, embed_size, rest_size = sizes
    head_out[...] = clip_factor(stat_ref[0:1, 0:1], head_size) * head_ref[...]
    @pl.when(pl.program_id(0) == 0)
    def _():
        rest_factor = clip_factor(stat_ref[2:3, 0:1], rest_size)
        embed_out[...] = clip_factor(stat_ref[1:2, 0:1], embed_size) * embed_ref[...]
        bias_out[...] = rest_factor * rest_ref[spans:spans + 1, :]
        span_out[...] = rest_factor * rest_ref[:spans, :]


def per_device(n, heads, pre, delta, head_weight, client_ids):
    rows, hidden_width = pre.shape
    emit = delta.shape[1]
    clients = client_ids.shape[0]
    spans = rows // clients
    block = hidden_width // n
    piece = min(256, block)
    hq = block // piece
    zs = n // 2
    q = 7
    sub = block // (q + 1)
    padded = (spans + 16) // 16 * 16
    half = emit // 2
    cfg = (n, heads, block, piece, spans, clients)
    ids = client_ids.reshape(1, clients)
    hbm = pl.BlockSpec(memory_space=pl.ANY)
    vmem = pl.BlockSpec(memory_space=pltpu.VMEM)
    dma = pltpu.SemaphoreType.DMA
    chunk = math.gcd(rows, 256)
    head_raw, rest_raw, embed_raw, stats = pl.pallas_call(
        functools.partial(kernel, cfg),
        out_shape=(
            jax.ShapeDtypeStruct((block, emit), F32),
            jax.ShapeDtypeStruct((padded, emit), F32),
            jax.ShapeDtypeStruct((clients, emit), F32),
            jax.ShapeDtypeStruct((8, 128), F32),
        ),
        in_specs=[hbm, hbm, hbm, hbm],
        out_specs=(hbm, vmem, vmem, vmem),
        scratch_shapes=[
            pltpu.VMEM((n, rows, block), BF16),
            pltpu.VMEM((rows, emit), F32),
            pltpu.VMEM((rows, emit), BF16),
            pltpu.VMEM((hidden_width, emit), BF16),
            pltpu.VMEM((hidden_width, emit), BF16),
            pltpu.VMEM((zs * q, sub, emit), BF16),
            pltpu.VMEM(((zs + 2) * q, sub, emit), BF16),
            pltpu.VMEM(((zs + 2) * 2, sub, emit), BF16),
            pltpu.VMEM((sub, emit), BF16),
            pltpu.VMEM((block, emit), F32),
            pltpu.VMEM((heads, spans + clients, emit), BF16),
            pltpu.VMEM((heads, spans + clients, emit), BF16),
            pltpu.VMEM((2, padded, half), BF16),
            pltpu.VMEM((zs, padded, half), BF16),
            pltpu.VMEM((padded, half), BF16),
            pltpu.VMEM((padded, half), BF16),
            pltpu.VMEM((2, padded, half), BF16),
            pltpu.VMEM((zs, 2, clients, emit), BF16),
            pltpu.VMEM((n, 1, clients), jnp.int32),
            pltpu.VMEM((2, 8, 128), F32),
            pltpu.VMEM((n, 8, 128), F32),
            pltpu.VMEM((heads, 8, 128), F32),
            dma((n * hq,)), dma((rows // chunk,)), dma, dma((q + 1,)),
            dma((zs * q,)), dma((zs * q,)), dma(((zs - 1) * q,)), dma(((zs + 2) * q,)),
            dma((2 * (zs - 1),)), dma(((zs + 2) * 2,)), dma((2,)), dma((heads,)), dma((heads,)),
            dma((2,)), dma((zs,)), dma((2,)), dma((zs,)), dma((2,)), dma((2,)), dma((zs,)), dma((zs,)),
            dma, dma((n,)), dma((n,)), dma((n + heads - 2,)), dma((n + heads,)),
        ],
        compiler_params=pltpu.CompilerParams(
            collective_id=0, has_side_effects=True, vmem_limit_bytes=62 * 2**20
        ),
        name="clipped_grads",
    )(pre, delta, head_weight, ids)
    sizes = (hidden_width * emit * heads, clients * n * hidden_width, spans * hidden_width + emit * heads)
    steps = 4 if block % 32 == 0 else 1
    whole = lambda *shape: pl.BlockSpec(shape, lambda i: (0, 0))
    tile = pl.BlockSpec((block // steps, emit), lambda i: (i, 0))
    head_grad, bias_grad, embed_grad, span_grad = pl.pallas_call(
        functools.partial(scale_kernel, sizes, spans),
        grid=(steps,),
        out_shape=(
            jax.ShapeDtypeStruct((block, emit), F32),
            jax.ShapeDtypeStruct((1, emit), F32),
            jax.ShapeDtypeStruct((clients, emit), F32),
            jax.ShapeDtypeStruct((spans, emit), F32),
        ),
        in_specs=[whole(8, 128), tile, whole(padded, emit), whole(clients, emit)],
        out_specs=(tile, whole(1, emit), whole(clients, emit), whole(spans, emit)),
        name="scaled",
    )(stats, head_raw, rest_raw, embed_raw)
    return head_grad, bias_grad.reshape(emit), embed_grad, span_grad


def solution(mesh):
    placed = (P("client", None), P("client", "head"), P(None, "head"), P("client"))
    return jax.shard_map(
        functools.partial(per_device, mesh.shape["client"], mesh.shape["head"]),
        mesh=mesh,
        in_specs=placed,
        out_specs=(P("client", "head"), P("head"), P("client", "head"), P(None, "head")),
        check_vma=False,
    )
```

```python
import functools
import math

import jax
import jax.numpy as jnp
from jax import lax
from jax.experimental import pallas as pl
from jax.experimental.pallas import tpu as pltpu
from jax.sharding import PartitionSpec as P

EPSILON = 1e-06
MESH = pl.DeviceIdType.MESH
F32 = jnp.float32
BF16 = jnp.bfloat16


def clip_factor(total, number):
    return jnp.minimum(1.0, 1.0 / jnp.sqrt(total / number + EPSILON))


def kernel(cfg, pre_ref, delta_ref, weight_ref, ids_ref, head_out, rest_out, embed_out, stat_out,
           pre_v, delta_v, low, weight_v, part, pair_in, line_in, first_in, swap_in, head_v,
           small, small_in, mine, span_in, span_part, span_pair, span_all, embed_all, ids_all,
           embed_v, rest_v, stat_all,
           pre_sem, delta_sem, weight_sem, out_sem, pair_send, pair_recv, line_send, line_recv,
           first_send, first_recv, swap_sem, head_send, head_recv, span_send, span_recv, span_pair_sem,
           all_send, all_recv, write_sem, embed_pair_sem, embed_send, embed_recv, ids_sem, ids_send, ids_recv,
           stat_send, stat_recv):
    n, heads, block, piece, spans, clients = cfg
    zs = n // 2
    q = 7
    sub = block // (q + 1)
    hq = block // piece
    rows, emit = low.shape
    me = lax.axis_index("client")
    my_head = lax.axis_index("head")
    z = me // 2
    x = me % 2
    relays = (zs - 1) * q

    devices = n * heads
    flat = me * heads + my_head

    def device(d):
        other = lax.rem(flat + d, devices)
        return {"client": other // heads, "head": other % heads}

    barrier = pltpu.get_barrier_semaphore()
    def greet(d, carry):
        pl.semaphore_signal(barrier, inc=1, device_id=device(d), device_id_type=MESH)
        return carry
    lax.fori_loop(1, devices, greet, 0)

    after_first = (z + zs - 1) // zs
    before_last = (2 * zs - 2 - z) // zs
    middle = after_first * before_last
    upper = 2 * z // zs
    near = z + upper * (zs - 1 - 2 * z)

    def dest(k):
        both = (2 * near - k - 1 + zs) // zs
        odd = k % 2
        out = both * (odd * (k // 2) + (1 - odd) * (zs - 1 - k // 2)) + (1 - both) * (zs - 1 - k + near)
        return out + upper * (zs - 1 - 2 * out)

    def block_row(place, side):
        return (place * 2 + side) * block

    def piece_row(place, side, s):
        return pl.multiple_of(block_row(place, side) + (s + 1) * sub, sub)

    def landing(place):
        right = (place - z + zs) // zs
        target = z + 2 * right - 1
        gap = right * (place - target) + (1 - right) * (target - place)
        away = (gap + zs - 1) // zs
        slot = away * place + (1 - away) * (zs + 1 - right)
        return target * 2 + x, slot

    partner = z * 2 + 1 - x

    def unit_side(u):
        return (x + 1 - u % 2) % 2

    def unit_row(u):
        return pl.multiple_of(block_row(dest(u // 2), unit_side(u)), block)

    def pre_copy(u, h):
        columns = pl.ds(pl.multiple_of(unit_row(u) + h * piece, piece), piece)
        return pltpu.make_async_copy(
            pre_ref.at[:, columns], pre_v.at[u, :, pl.ds(pl.multiple_of(h * piece, piece), piece)],
            pre_sem.at[u * hq + h])

    chunk = math.gcd(rows, 256)
    delta_copies = [
        pltpu.make_async_copy(delta_ref.at[pl.ds(c * chunk, chunk), :], delta_v.at[pl.ds(c * chunk, chunk), :],
                              delta_sem.at[c])
        for c in range(rows // chunk)]
    weight_copy = pltpu.make_async_copy(weight_ref, weight_v, weight_sem)
    ids_copy = pltpu.make_async_copy(ids_ref, ids_all.at[me], ids_sem)
    pre_copy(0, 0).start()
    for copy in delta_copies:
        copy.start()
    ids_copy.start()
    def load(u, carry):
        @pl.when(u > 0)
        def _():
            pre_copy(u, 0).start()
        return carry
    lax.fori_loop(0, 2 * zs, load, 0)
    def load_rest(u, carry):
        for h in range(1, hq):
            pre_copy(u, h).start()
        return carry
    lax.fori_loop(0, 2 * zs, load_rest, 0)
    weight_copy.start()

    line_in[z * q] = jnp.zeros((sub, emit), BF16)
    first_in[z * 2] = jnp.zeros((sub, emit), BF16)

    step = 64
    for c, copy in enumerate(delta_copies):
        copy.wait()
        def narrow(r, carry):
            at = pl.ds(pl.multiple_of(c * chunk + r * step, step), step)
            low[at, :] = delta_v[at, :].astype(BF16)
            return carry
        lax.fori_loop(0, chunk // step, narrow, 0)

    pl.semaphore_wait(barrier, devices - 1)

    def product(u, h):
        p = pre_v[u, :, pl.ds(pl.multiple_of(h * piece, piece), piece)].astype(F32)
        hidden = (p * jax.nn.sigmoid(p)).astype(BF16)
        value = lax.dot_general(hidden, low[...], (((0,), (0,)), ((), ())), preferred_element_type=F32)
        part[pl.ds(pl.multiple_of(unit_row(u) + h * piece, piece), piece), :] = value.astype(BF16)

    def slope_sums(t):
        u = t // hq
        h = t % hq
        p = pre_v[u, :, pl.ds(pl.multiple_of(h * piece, piece), piece)].astype(F32)
        row = pl.multiple_of(unit_row(u) + h * piece, piece)
        value = lax.dot_general(
            low[...], weight_v[pl.ds(row, piece), :], (((1,), (1,)), ((), ())), preferred_element_type=F32)
        s = jax.nn.sigmoid(p)
        grad = value.astype(BF16).astype(F32) * (s * (1.0 + p * (1.0 - s)))
        grad = grad.reshape(clients, spans, piece)
        to = row // emit
        columns = pl.ds(pl.multiple_of(row % emit, piece), piece)
        small[to, pl.ds(0, spans), columns] = jnp.sum(grad, axis=0).astype(BF16)
        small[to, pl.ds(spans, clients), columns] = jnp.sum(grad, axis=1).astype(BF16)

    def pair_copy(i):
        return pltpu.make_async_remote_copy(
            src_ref=part.at[pl.ds(piece_row(dest(i // q), 1 - x, i % q), sub), :], dst_ref=pair_in.at[i],
            send_sem=pair_send.at[i], recv_sem=pair_recv.at[i],
            device_id={"client": partner}, device_id_type=MESH)

    def line_copy(i):
        place = dest(i // q)
        target, slot = landing(place)
        return pltpu.make_async_remote_copy(
            src_ref=part.at[pl.ds(piece_row(place, x, i % q), sub), :], dst_ref=line_in.at[slot * q + i % q],
            send_sem=line_send.at[i], recv_sem=line_recv.at[slot * q + i % q],
            device_id={"client": target}, device_id_type=MESH)

    def arrival(slot):
        return pltpu.make_async_remote_copy(
            src_ref=part.at[pl.ds(0, sub), :], dst_ref=line_in.at[slot], send_sem=line_send.at[0],
            recv_sem=line_recv.at[slot], device_id={"client": partner}, device_id_type=MESH)

    lead = q + 2
    queue = 4
    slopes = 2 * zs * hq
    paced = slopes // 2 + 1
    step_rows = min(32, sub)

    def relay(i):
        place = dest(i // q)
        row = piece_row(place, x, i % q)
        pair_copy(i).wait_recv()
        @pl.when(middle == 1)
        def _():
            arrival(place * q + i % q).wait_recv()
        slot = middle * (place * q + i % q) + (1 - middle) * z * q
        def add(r, carry):
            at = pl.ds(pl.multiple_of(r * step_rows, step_rows), step_rows)
            mine_at = pl.ds(pl.multiple_of(row + r * step_rows, step_rows), step_rows)
            total = part[mine_at, :].astype(F32) + pair_in[i, at, :].astype(F32)
            part[mine_at, :] = (total + line_in[slot, at, :].astype(F32)).astype(BF16)
            return carry
        lax.fori_loop(0, sub // step_rows, add, 0)
        @pl.when(i >= paced)
        def _():
            line_copy(i - queue).wait_send()
        line_copy(i).start()
        @pl.when(i + lead < zs * q)
        def _():
            pair_copy(i + lead).start()

    def relay_range(start, stop):
        def body(i, carry):
            relay(i)
            return carry
        if stop > start:
            lax.fori_loop(start, stop, body, 0)

    def finish(s, square):
        i = relays + s
        row = piece_row(z, x, s)
        pair_copy(i).wait_recv()
        @pl.when(after_first == 1)
        def _():
            arrival(zs * q + s).wait_recv()
        @pl.when(before_last == 1)
        def _():
            arrival((zs + 1) * q + s).wait_recv()
        left = after_first * (zs * q + s) + (1 - after_first) * z * q
        right = before_last * ((zs + 1) * q + s) + (1 - before_last) * z * q
        def add(r, carry):
            at = pl.ds(pl.multiple_of(r * step_rows, step_rows), step_rows)
            mine_at = pl.ds(pl.multiple_of(row + r * step_rows, step_rows), step_rows)
            out_at = pl.ds(pl.multiple_of((s + 1) * sub + r * step_rows, step_rows), step_rows)
            total = part[mine_at, :].astype(F32) + pair_in[i, at, :].astype(F32)
            total = total + line_in[left, at, :].astype(F32) + line_in[right, at, :].astype(F32)
            head_v[out_at, :] = total
            return carry + jnp.sum((total * total).reshape(step_rows // 8, 8, emit), axis=0)
        square = lax.fori_loop(0, sub // step_rows, add, square)
        pltpu.make_async_copy(
            head_v.at[pl.ds(pl.multiple_of((s + 1) * sub, sub), sub), :],
            head_out.at[pl.ds(pl.multiple_of((s + 1) * sub, sub), sub), :], out_sem.at[s + 1]).start()
        return square

    def first_copy(j):
        place = dest(j // 2)
        side = unit_side(j)
        target, slot = landing(place)
        return pltpu.make_async_remote_copy(
            src_ref=part.at[pl.ds(pl.multiple_of(block_row(place, side), sub), sub), :],
            dst_ref=first_in.at[slot * 2 + side],
            send_sem=first_send.at[j], recv_sem=first_recv.at[slot * 2 + side],
            device_id={"client": target}, device_id_type=MESH)

    def first_arrival(slot):
        return pltpu.make_async_remote_copy(
            src_ref=part.at[pl.ds(0, sub), :], dst_ref=first_in.at[slot], send_sem=first_send.at[0],
            recv_sem=first_recv.at[slot], device_id={"client": partner}, device_id_type=MESH)

    def first_relay(j):
        @pl.when(middle == 1)
        def _():
            place = dest(j // 2)
            side = unit_side(j)
            row = pl.multiple_of(block_row(place, side), sub)
            first_arrival(place * 2 + side).wait_recv()
            def add(r, carry):
                at = pl.ds(pl.multiple_of(r * step_rows, step_rows), step_rows)
                mine_at = pl.ds(pl.multiple_of(row + r * step_rows, step_rows), step_rows)
                part[mine_at, :] = (
                    part[mine_at, :].astype(F32) + first_in[place * 2 + side, at, :].astype(F32)).astype(BF16)
                return carry
            lax.fori_loop(0, sub // step_rows, add, 0)
            first_copy(j).start()

    swap_copy = pltpu.make_async_remote_copy(
        src_ref=part.at[pl.ds(pl.multiple_of(block_row(z, 1 - x), sub), sub), :], dst_ref=swap_in,
        send_sem=swap_sem.at[0], recv_sem=swap_sem.at[1], device_id={"client": partner}, device_id_type=MESH)

    def first_wait(side):
        @pl.when(after_first == 1)
        def _():
            first_arrival(zs * 2 + side).wait_recv()
        @pl.when(before_last == 1)
        def _():
            first_arrival((zs + 1) * 2 + side).wait_recv()
        left = after_first * (zs * 2 + side) + (1 - after_first) * z * 2
        right = before_last * ((zs + 1) * 2 + side) + (1 - before_last) * z * 2
        return left, right

    def first_swap():
        row = block_row(z, 1 - x)
        left, right = first_wait(1 - x)
        def add(r, carry):
            at = pl.ds(pl.multiple_of(r * step_rows, step_rows), step_rows)
            mine_at = pl.ds(pl.multiple_of(row + r * step_rows, step_rows), step_rows)
            total = part[mine_at, :].astype(F32) + first_in[left, at, :].astype(F32)
            part[mine_at, :] = (total + first_in[right, at, :].astype(F32)).astype(BF16)
            return carry
        lax.fori_loop(0, sub // step_rows, add, 0)
        swap_copy.start()

    def first_finish(square):
        row = block_row(z, x)
        left, right = first_wait(x)
        swap_copy.wait_recv()
        def add(r, carry):
            at = pl.ds(pl.multiple_of(r * step_rows, step_rows), step_rows)
            mine_at = pl.ds(pl.multiple_of(row + r * step_rows, step_rows), step_rows)
            total = part[mine_at, :].astype(F32) + first_in[left, at, :].astype(F32)
            total = total + first_in[right, at, :].astype(F32) + swap_in[at, :].astype(F32)
            head_v[at, :] = total
            return carry + jnp.sum((total * total).reshape(step_rows // 8, 8, emit), axis=0)
        square = lax.fori_loop(0, sub // step_rows, add, square)
        pltpu.make_async_copy(head_v.at[pl.ds(0, sub), :], head_out.at[pl.ds(0, sub), :], out_sem.at[0]).start()
        return square

    ready = piece // sub - 1

    def opening(u, carry):
        pre_copy(u, 0).wait()
        product(u, 0)
        @pl.when(middle == 0)
        def _():
            first_copy(u).start()
        @pl.when(u == 0)
        def _():
            for i in range(ready):
                pair_copy(i).start()
        return carry
    lax.fori_loop(0, 2 * (zs - 1), opening, 0)
    if hq > 1:
        def second(t, carry):
            pre_copy(t // (hq - 1), 1 + t % (hq - 1)).wait()
            product(t // (hq - 1), 1 + t % (hq - 1))
            return carry
        lax.fori_loop(0, 3 * (hq - 1), second, 0)
    def more_pairs(i, carry):
        pair_copy(i).start()
        return carry
    lax.fori_loop(ready, lead, more_pairs, 0)
    first_relay(0)
    first_relay(1)
    def loaded(u, carry):
        @pl.when(u >= 2 * zs - 2)
        def _():
            pre_copy(u, 0).wait()
        for h in range(1, hq):
            pre_copy(u, h).wait()
        return carry
    lax.fori_loop(3 if hq > 1 else 2 * zs - 2, 2 * zs, loaded, 0)
    weight_copy.wait()

    ids_copy.wait()
    ids_copies = []
    for d in range(1, n):
        copy = pltpu.make_async_remote_copy(
            src_ref=ids_all.at[me], dst_ref=ids_all.at[me], send_sem=ids_send.at[d], recv_sem=ids_recv.at[me],
            device_id={"client": lax.rem(me + d, n)}, device_id_type=MESH)
        copy.start()
        ids_copies.append(copy)

    firsts = 2 * (zs - 1)
    def main(t, carry):
        slope_sums(t)
        @pl.when((t % 3 == 0) & (2 + t // 3 < firsts))
        def _():
            first_relay(2 + t // 3)
        @pl.when(t % 2 == 1)
        def _():
            relay(t // 2)
        return carry
    lax.fori_loop(0, slopes, main, 0)

    head_copies = []
    for d in range(1, heads):
        target = lax.rem(my_head + d, heads)
        copy = pltpu.make_async_remote_copy(
            src_ref=small.at[target], dst_ref=small_in.at[my_head],
            send_sem=head_send.at[d], recv_sem=head_recv.at[my_head],
            device_id={"head": target}, device_id_type=MESH)
        copy.start()
        head_copies.append(copy)

    done = 2 + (slopes + 2) // 3
    if done < firsts:
        def rest_first(j, carry):
            first_relay(j)
            return carry
        lax.fori_loop(done, firsts, rest_first, 0)

    def add_rows(r, total):
        value = delta_v[pl.ds(pl.multiple_of(r * step, step), step), :]
        return total + jnp.sum(value.reshape(step // 8, 8, emit), axis=0)
    bias = lax.fori_loop(0, rows // step, add_rows, jnp.zeros((8, emit), F32))
    bias = jnp.sum(bias, axis=0, keepdims=True)
    half = emit // 2
    pad = mine.shape[1] - spans
    tail = jnp.where(
        lax.broadcasted_iota(jnp.int32, (pad, emit), 0) == 0, jnp.broadcast_to(bias, (pad, emit)), 0.0
    ).astype(BF16)
    for h in range(2):
        mine[h, pl.ds(spans, pad), :] = tail[:, h * half:(h + 1) * half]

    at = slopes // 2
    if hq > 1:
        def third(t, carry):
            product(3 + t // (hq - 1), 1 + t % (hq - 1))
            return carry
        lax.fori_loop(0, (2 * zs - 5) * (hq - 1), third, 0)
    relay_range(at, at + 1)
    def fourth(t, carry):
        product(2 * zs - 2 + t // hq, t % hq)
        return carry
    lax.fori_loop(0, 2 * hq, fourth, 0)
    first_swap()
    relay_range(at + 1, at + 4)
    at = at + 4
    stop = [at + (relays - at) * k // 9 for k in (4, 8, 9)]

    for d in range(1, heads):
        source = lax.rem(my_head + d, heads)
        pltpu.make_async_remote_copy(
            src_ref=small.at[0], dst_ref=small_in.at[source], send_sem=head_send.at[d],
            recv_sem=head_recv.at[source], device_id={"head": source}, device_id_type=MESH).wait_recv()
    total = small[my_head].astype(F32)
    for d in range(1, heads):
        total = total + small_in[lax.rem(my_head + d, heads)].astype(F32)
    for h in range(2):
        mine[h, pl.ds(0, spans), :] = total[:spans, h * half:(h + 1) * half].astype(BF16)
    embed_all[z, x] = total[spans:].astype(BF16)

    embed_pair = pltpu.make_async_remote_copy(
        src_ref=embed_all.at[z, x], dst_ref=embed_all.at[z, x], send_sem=embed_pair_sem.at[0],
        recv_sem=embed_pair_sem.at[1], device_id={"client": partner}, device_id_type=MESH)
    embed_pair.start()
    roots = [zs // 2 - 1, zs // 2]
    def span_copy(h):
        return pltpu.make_async_remote_copy(
            src_ref=mine.at[h], dst_ref=span_in.at[z], send_sem=span_send.at[h], recv_sem=span_recv.at[z],
            device_id={"client": roots[h] * 2 + x}, device_id_type=MESH)
    for h in range(2):
        @pl.when(z != roots[h])
        def _():
            span_copy(h).start()

    relay_range(at, stop[0])

    embed_pair.wait_recv()
    embed_copies = []
    for d in range(1, zs):
        copy = pltpu.make_async_remote_copy(
            src_ref=embed_all.at[z], dst_ref=embed_all.at[z], send_sem=embed_send.at[d], recv_sem=embed_recv.at[z],
            device_id={"client": lax.rem(z + d, zs) * 2 + x}, device_id_type=MESH)
        copy.start()
        embed_copies.append(copy)
    span_pair_copy = pltpu.make_async_remote_copy(
        src_ref=span_part, dst_ref=span_pair, send_sem=span_pair_sem.at[0], recv_sem=span_pair_sem.at[1],
        device_id={"client": partner}, device_id_type=MESH)
    for h in range(2):
        @pl.when(z == roots[h])
        def _():
            total = mine[h].astype(F32)
            for d in range(1, zs):
                source = (roots[h] + d) % zs
                pltpu.make_async_remote_copy(
                    src_ref=mine.at[h], dst_ref=span_in.at[source], send_sem=span_send.at[h],
                    recv_sem=span_recv.at[source], device_id={"client": partner}, device_id_type=MESH).wait_recv()
                total = total + span_in[source].astype(F32)
            span_part[...] = total.astype(BF16)
            span_pair_copy.start()

    relay_range(stop[0], stop[1])

    def all_copy(h, d):
        return pltpu.make_async_remote_copy(
            src_ref=span_all.at[h], dst_ref=span_all.at[h], send_sem=all_send.at[d], recv_sem=all_recv.at[h],
            device_id={"client": lax.rem(z + d, zs) * 2 + x}, device_id_type=MESH)
    for h in range(2):
        @pl.when(z == roots[h])
        def _():
            span_pair_copy.wait_recv()
            span_all[h] = (span_part[...].astype(F32) + span_pair[...].astype(F32)).astype(BF16)
            for d in range(1, zs):
                all_copy(h, d).start()

    relay_range(stop[1], relays)
    square = jnp.zeros((8, emit), F32)
    square = first_finish(square)
    square = lax.fori_loop(0, 3, finish, square)

    for d in range(1, n):
        source = lax.rem(me + d, n)
        pltpu.make_async_remote_copy(
            src_ref=ids_all.at[me], dst_ref=ids_all.at[source], send_sem=ids_send.at[d],
            recv_sem=ids_recv.at[source], device_id={"client": source}, device_id_type=MESH).wait_recv()
    for d in range(1, zs):
        source = lax.rem(z + d, zs)
        pltpu.make_async_remote_copy(
            src_ref=embed_all.at[z], dst_ref=embed_all.at[source], send_sem=embed_send.at[d],
            recv_sem=embed_recv.at[source], device_id={"client": source * 2 + x}, device_id_type=MESH).wait_recv()
    wanted = lax.broadcasted_iota(jnp.int32, (clients, clients), 0) + me * clients
    embed_raw = jnp.zeros((clients, emit), F32)
    for c in range(n):
        chosen = (jnp.broadcast_to(ids_all[c], (clients, clients)) == wanted).astype(F32).astype(BF16)
        embed_raw = embed_raw + jnp.dot(chosen, embed_all[c // 2, c % 2], preferred_element_type=F32)
    embed_v[...] = embed_raw
    embed_write = pltpu.make_async_copy(embed_v, embed_out, write_sem.at[0])
    embed_write.start()
    embed_square = jnp.sum(embed_raw * embed_raw)

    rest_square = jnp.zeros((), F32)
    for h in range(2):
        @pl.when(z != roots[h])
        def _():
            all_copy(h, 1).wait_recv()
        value = span_all[h].astype(F32)
        rest_v[:, pl.ds(h * half, half)] = value
        rest_square = rest_square + jnp.sum(value * value)

    rest_write = pltpu.make_async_copy(rest_v, rest_out, write_sem.at[1])
    rest_write.start()

    square = lax.fori_loop(3, q, finish, square)
    head_total = jnp.sum(square)

    lane = lax.broadcasted_iota(jnp.int32, (1, 128), 1)
    stat_all[flat] = jnp.where(lane == 0, head_total, jnp.where(lane == 1, embed_square, rest_square / n))
    def stat_copy(d):
        return pltpu.make_async_remote_copy(
            src_ref=stat_all.at[flat], dst_ref=stat_all.at[flat], send_sem=stat_send.at[d],
            recv_sem=stat_recv.at[flat], device_id=device(d), device_id_type=MESH)
    def tell(d, carry):
        stat_copy(d).start()
        return carry
    lax.fori_loop(1, devices, tell, 0)
    def hear(d, carry):
        source = lax.rem(flat + d, devices)
        pltpu.make_async_remote_copy(
            src_ref=stat_all.at[flat], dst_ref=stat_all.at[source], send_sem=stat_send.at[d],
            recv_sem=stat_recv.at[source], device_id=device(d), device_id_type=MESH).wait_recv()
        return carry
    lax.fori_loop(1, devices, hear, 0)
    stat_out[...] = jnp.sum(stat_all[...], axis=0)

    def told(d, carry):
        stat_copy(d).wait_send()
        return carry
    lax.fori_loop(1, devices, told, 0)
    def pair_sent(i, carry):
        pair_copy(i).wait_send()
        return carry
    lax.fori_loop(0, zs * q, pair_sent, 0)
    def line_sent(i, carry):
        line_copy(i).wait_send()
        return carry
    lax.fori_loop(0, paced - queue, line_sent, 0)
    lax.fori_loop(relays - queue, relays, line_sent, 0)
    def first_sent(j, carry):
        first_copy(j).wait_send()
        return carry
    lax.fori_loop(0, firsts, first_sent, 0)
    swap_copy.wait_send()
    embed_pair.wait_send()
    embed_write.wait()
    rest_write.wait()
    for copy in head_copies + embed_copies + ids_copies:
        copy.wait_send()
    for h in range(2):
        @pl.when(z != roots[h])
        def _():
            span_copy(h).wait_send()
        @pl.when(z == roots[h])
        def _():
            span_pair_copy.wait_send()
            for d in range(1, zs):
                all_copy(h, d).wait_send()
    def written(s, carry):
        at = pl.multiple_of(s * sub, sub)
        pltpu.make_async_copy(
            head_v.at[pl.ds(at, sub), :], head_out.at[pl.ds(at, sub), :], out_sem.at[s]).wait()
        return carry
    lax.fori_loop(0, q + 1, written, 0)


def scale_kernel(sizes, stat_ref, head_ref, rest_ref, embed_ref, head_out, bias_out, embed_out, span_out,
                 stat, head, rest, embed, in_sem, out_sem):
    head_size, embed_size, rest_size = sizes
    spans = span_out.shape[0]
    steps = in_sem.shape[0] - 3
    rows = head.shape[0] // steps
    stat_in = pltpu.make_async_copy(stat_ref, stat, in_sem.at[steps])
    rest_in = pltpu.make_async_copy(rest_ref, rest, in_sem.at[steps + 1])
    embed_in = pltpu.make_async_copy(embed_ref, embed, in_sem.at[steps + 2])
    def part(ref, i):
        return ref.at[pl.ds(i * rows, rows), :]
    stat_in.start()
    heads_in = [pltpu.make_async_copy(part(head_ref, i), part(head, i), in_sem.at[i]) for i in range(steps)]
    heads_out = [pltpu.make_async_copy(part(head, i), part(head_out, i), out_sem.at[i]) for i in range(steps)]
    for copy in heads_in:
        copy.start()
    rest_in.start()
    embed_in.start()
    stat_in.wait()
    factor = clip_factor(stat[0:1, 0:1], head_size)
    embed_factor = clip_factor(stat[0:1, 1:2], embed_size)
    rest_factor = clip_factor(stat[0:1, 2:3], rest_size)
    for i in range(steps):
        heads_in[i].wait()
        head[pl.ds(i * rows, rows), :] = factor * head[pl.ds(i * rows, rows), :]
        heads_out[i].start()
    rest_in.wait()
    rest[...] = rest_factor * rest[...]
    bias_copy = pltpu.make_async_copy(rest.at[pl.ds(spans, 1), :], bias_out, out_sem.at[steps])
    span_copy = pltpu.make_async_copy(rest.at[pl.ds(0, spans), :], span_out, out_sem.at[steps + 1])
    bias_copy.start()
    span_copy.start()
    embed_in.wait()
    embed[...] = embed_factor * embed[...]
    embed_copy = pltpu.make_async_copy(embed, embed_out, out_sem.at[steps + 2])
    embed_copy.start()
    for copy in heads_out + [bias_copy, span_copy, embed_copy]:
        copy.wait()


def per_device(n, heads, pre, delta, head_weight, client_ids):
    rows, hidden_width = pre.shape
    emit = delta.shape[1]
    clients = client_ids.shape[0]
    spans = rows // clients
    block = hidden_width // n
    piece = min(256, block)
    hq = block // piece
    zs = n // 2
    q = 7
    sub = block // (q + 1)
    padded = (spans + 16) // 16 * 16
    half = emit // 2
    cfg = (n, heads, block, piece, spans, clients)
    ids = client_ids.reshape(1, clients)
    hbm = pl.BlockSpec(memory_space=pl.ANY)
    vmem = pl.BlockSpec(memory_space=pltpu.VMEM)
    dma = pltpu.SemaphoreType.DMA
    chunk = math.gcd(rows, 256)
    head_raw, rest_raw, embed_raw, stats = pl.pallas_call(
        functools.partial(kernel, cfg),
        out_shape=(
            jax.ShapeDtypeStruct((block, emit), F32),
            jax.ShapeDtypeStruct((padded, emit), F32),
            jax.ShapeDtypeStruct((clients, emit), F32),
            jax.ShapeDtypeStruct((1, 128), F32),
        ),
        in_specs=[hbm, hbm, hbm, hbm],
        out_specs=(hbm, hbm, hbm, vmem),
        scratch_shapes=[
            pltpu.VMEM((n, rows, block), BF16),
            pltpu.VMEM((rows, emit), F32),
            pltpu.VMEM((rows, emit), BF16),
            pltpu.VMEM((hidden_width, emit), BF16),
            pltpu.VMEM((hidden_width, emit), BF16),
            pltpu.VMEM((zs * q, sub, emit), BF16),
            pltpu.VMEM(((zs + 2) * q, sub, emit), BF16),
            pltpu.VMEM(((zs + 2) * 2, sub, emit), BF16),
            pltpu.VMEM((sub, emit), BF16),
            pltpu.VMEM((block, emit), F32),
            pltpu.VMEM((heads, spans + clients, emit), BF16),
            pltpu.VMEM((heads, spans + clients, emit), BF16),
            pltpu.VMEM((2, padded, half), BF16),
            pltpu.VMEM((zs, padded, half), BF16),
            pltpu.VMEM((padded, half), BF16),
            pltpu.VMEM((padded, half), BF16),
            pltpu.VMEM((2, padded, half), BF16),
            pltpu.VMEM((zs, 2, clients, emit), BF16),
            pltpu.VMEM((n, 1, clients), jnp.int32),
            pltpu.VMEM((clients, emit), F32),
            pltpu.VMEM((padded, emit), F32),
            pltpu.VMEM((n * heads, 1, 128), F32),
            dma((n * hq,)), dma((rows // chunk,)), dma, dma((q + 1,)),
            dma((zs * q,)), dma((zs * q,)), dma(((zs - 1) * q,)), dma(((zs + 2) * q,)),
            dma((2 * (zs - 1),)), dma(((zs + 2) * 2,)), dma((2,)), dma((heads,)), dma((heads,)),
            dma((2,)), dma((zs,)), dma((2,)), dma((zs,)), dma((2,)), dma((2,)), dma((2,)), dma((zs,)), dma((zs,)),
            dma, dma((n,)), dma((n,)), dma((n * heads,)), dma((n * heads,)),
        ],
        compiler_params=pltpu.CompilerParams(
            collective_id=0, has_side_effects=True, vmem_limit_bytes=62 * 2**20
        ),
        name="clipped_grads",
    )(pre, delta, head_weight, ids)
    sizes = (hidden_width * emit * heads, clients * n * hidden_width, spans * hidden_width + emit * heads)
    steps = 4
    head_grad, bias_grad, embed_grad, span_grad = pl.pallas_call(
        functools.partial(scale_kernel, sizes),
        out_shape=(
            jax.ShapeDtypeStruct((block, emit), F32),
            jax.ShapeDtypeStruct((1, emit), F32),
            jax.ShapeDtypeStruct((clients, emit), F32),
            jax.ShapeDtypeStruct((spans, emit), F32),
        ),
        in_specs=[hbm] * 4,
        out_specs=(hbm,) * 4,
        scratch_shapes=[
            pltpu.VMEM((1, 128), F32),
            pltpu.VMEM((block, emit), F32),
            pltpu.VMEM((padded, emit), F32),
            pltpu.VMEM((clients, emit), F32),
            dma((steps + 3,)), dma((steps + 3,)),
        ],
        name="scaled",
    )(stats, head_raw, rest_raw, embed_raw)
    return head_grad, bias_grad.reshape(emit), embed_grad, span_grad


def solution(mesh):
    placed = (P("client", None), P("client", "head"), P(None, "head"), P("client"))
    return jax.shard_map(
        functools.partial(per_device, mesh.shape["client"], mesh.shape["head"]),
        mesh=mesh,
        in_specs=placed,
        out_specs=(P("client", "head"), P("head"), P("client", "head"), P(None, "head")),
        check_vma=False,
    )
```

```python
import functools
import math

import jax
import jax.numpy as jnp
from jax import lax
from jax.experimental import pallas as pl
from jax.experimental.pallas import tpu as pltpu
from jax.sharding import PartitionSpec as P

EPSILON = 1e-06
MESH = pl.DeviceIdType.MESH
F32 = jnp.float32
BF16 = jnp.bfloat16


def clip_factor(total, number):
    return jnp.minimum(1.0, 1.0 / jnp.sqrt(total / number + EPSILON))


def kernel(cfg, pre_ref, delta_ref, weight_ref, ids_ref, head_out, rest_out, embed_out, stat_out,
           pre_v, delta_v, low, weight_v, part, pair_in, line_in, first_in, swap_in, head_v,
           small, small_in, mine, span_in, span_part, span_pair, span_all, embed_all, ids_all,
           embed_v, rest_v, stat_all,
           pre_sem, delta_sem, weight_sem, out_sem, pair_send, pair_recv, line_send, line_recv,
           first_send, first_recv, swap_sem, head_send, head_recv, span_send, span_recv, span_pair_sem,
           all_send, all_recv, write_sem, embed_pair_sem, embed_send, embed_recv, ids_sem, ids_send, ids_recv,
           stat_send, stat_recv):
    n, heads, block, piece, spans, clients = cfg
    zs = n // 2
    q = 7
    sub = block // (q + 1)
    hq = block // piece
    rows, emit = low.shape
    half = emit // 2
    me = lax.axis_index("client")
    my_head = lax.axis_index("head")
    z = me // 2
    x = me % 2
    relays = (zs - 1) * q
    firsts = 2 * (zs - 1)
    slopes = 2 * zs * hq
    devices = n * heads
    flat = me * heads + my_head

    after_first = (z + zs - 1) // zs
    before_last = (2 * zs - 2 - z) // zs
    middle = after_first * before_last
    upper = 2 * z // zs
    near = z + upper * (zs - 1 - 2 * z)
    partner = z * 2 + 1 - x

    def wait_all(ref, sem):
        pltpu.make_async_copy(ref, ref, sem).wait()

    def send(src, dst, send_sem, recv_sem, client):
        return pltpu.make_async_remote_copy(
            src_ref=src, dst_ref=dst, send_sem=send_sem, recv_sem=recv_sem,
            device_id={"client": client}, device_id_type=MESH)

    def dest(k):
        both = (2 * near - k - 1 + zs) // zs
        odd = k % 2
        out = both * (odd * (k // 2) + (1 - odd) * (zs - 1 - k // 2)) + (1 - both) * (zs - 1 - k + near)
        return out + upper * (zs - 1 - 2 * out)

    def block_row(place, side):
        return (place * 2 + side) * block

    def piece_row(place, side, s):
        return pl.multiple_of(block_row(place, side) + (s + 1) * sub, sub)

    def landing(place):
        right = (place - z + zs) // zs
        target = z + 2 * right - 1
        gap = right * (place - target) + (1 - right) * (target - place)
        away = (gap + zs - 1) // zs
        slot = away * place + (1 - away) * (zs + 1 - right)
        sem = away * place + (1 - away) * (right * zs + (1 - right) * place)
        return target * 2 + x, slot, sem

    def unit_side(u):
        return (x + 1 - u % 2) % 2

    def unit_row(u):
        return pl.multiple_of(block_row(dest(u // 2), unit_side(u)), block)

    def pre_copy(u, h, sem):
        columns = pl.ds(pl.multiple_of(unit_row(u) + h * piece, piece), piece)
        return pltpu.make_async_copy(
            pre_ref.at[:, columns], pre_v.at[u, :, pl.ds(pl.multiple_of(h * piece, piece), piece)], pre_sem.at[sem])

    chunk = math.gcd(rows, 256)
    delta_copies = [
        pltpu.make_async_copy(delta_ref.at[pl.ds(c * chunk, chunk), :], delta_v.at[pl.ds(c * chunk, chunk), :],
                              delta_sem.at[c])
        for c in range(rows // chunk)]
    weight_copy = pltpu.make_async_copy(weight_ref, weight_v, weight_sem)
    ids_copy = pltpu.make_async_copy(ids_ref, ids_all.at[me], ids_sem)
    pre_copy(0, 0, 0).start()
    for copy in delta_copies:
        copy.start()

    def device(d):
        other = lax.rem(flat + d, devices)
        return {"client": other // heads, "head": other % heads}

    barrier = pltpu.get_barrier_semaphore()
    def greet(d, carry):
        pl.semaphore_signal(barrier, inc=1, device_id=device(d), device_id_type=MESH)
        return carry
    lax.fori_loop(1, devices, greet, 0)

    def load(u, carry):
        pre_copy(u, 0, 1).start()
        return carry
    lax.fori_loop(1, firsts, load, 0)
    def load_rest(u, carry):
        @pl.when(u >= firsts)
        def _():
            pre_copy(u, 0, 2).start()
        for h in range(1, hq):
            pre_copy(u, h, 2).start()
        return carry
    lax.fori_loop(0 if hq > 1 else firsts, 2 * zs, load_rest, 0)
    weight_copy.start()
    ids_copy.start()

    def product(u, h):
        p = pre_v[u, :, pl.ds(pl.multiple_of(h * piece, piece), piece)].astype(F32)
        hidden = (p * jax.nn.sigmoid(p)).astype(BF16)
        value = lax.dot_general(hidden, low[...], (((0,), (0,)), ((), ())), preferred_element_type=F32)
        part[pl.ds(pl.multiple_of(unit_row(u) + h * piece, piece), piece), :] = value.astype(BF16)

    def slope_sums(t):
        u = t // hq
        h = t % hq
        p = pre_v[u, :, pl.ds(pl.multiple_of(h * piece, piece), piece)].astype(F32)
        row = pl.multiple_of(unit_row(u) + h * piece, piece)
        value = lax.dot_general(
            low[...], weight_v[pl.ds(row, piece), :], (((1,), (1,)), ((), ())), preferred_element_type=F32)
        s = jax.nn.sigmoid(p)
        grad = value.astype(BF16).astype(F32) * (s * (1.0 + p * (1.0 - s)))
        grad = grad.reshape(clients, spans, piece)
        to = row // emit
        columns = pl.ds(pl.multiple_of(row % emit, piece), piece)
        small[to, pl.ds(0, spans), columns] = jnp.sum(grad, axis=0).astype(BF16)
        small[to, pl.ds(spans, clients), columns] = jnp.sum(grad, axis=1).astype(BF16)

    def pair_copy(i):
        return send(part.at[pl.ds(piece_row(dest(i // q), 1 - x, i % q), sub), :], pair_in.at[i],
                    pair_send, pair_recv.at[i], partner)

    queue = 3

    def line_copy(i):
        place = dest(i // q)
        target, slot, sem = landing(place)
        return send(part.at[pl.ds(piece_row(place, x, i % q), sub), :], line_in.at[slot * q + i % q],
                    line_send.at[i % queue], line_recv.at[sem * q + i % q], target)

    lead = q + 4 * middle
    step_rows = min(32, sub)

    def relay(i):
        place = dest(i // q)
        row = piece_row(place, x, i % q)
        pair_copy(i).wait_recv()
        @pl.when(middle == 1)
        def _():
            wait_all(line_in.at[place * q + i % q], line_recv.at[place * q + i % q])
        slot = middle * (place * q + i % q) + (1 - middle) * z * q
        def add(r, carry):
            at = pl.ds(pl.multiple_of(r * step_rows, step_rows), step_rows)
            mine_at = pl.ds(pl.multiple_of(row + r * step_rows, step_rows), step_rows)
            total = part[mine_at, :].astype(F32) + pair_in[i, at, :].astype(F32)
            part[mine_at, :] = (total + line_in[slot, at, :].astype(F32)).astype(BF16)
            return carry
        lax.fori_loop(0, sub // step_rows, add, 0)
        @pl.when(i >= queue)
        def _():
            line_copy(i - queue).wait_send()
        line_copy(i).start()
        @pl.when(i + lead < zs * q)
        def _():
            pair_copy(i + lead).start()

    def relay_range(start, stop):
        def body(i, carry):
            relay(i)
            return carry
        lax.fori_loop(start, stop, body, 0)

    def finish(s, square):
        i = relays + s
        row = piece_row(z, x, s)
        pair_copy(i).wait_recv()
        @pl.when(after_first == 1)
        def _():
            wait_all(line_in.at[zs * q + s], line_recv.at[zs * q + s])
        @pl.when(before_last == 1)
        def _():
            wait_all(line_in.at[(zs + 1) * q + s], line_recv.at[z * q + s])
        left = after_first * (zs * q + s) + (1 - after_first) * z * q
        right = before_last * ((zs + 1) * q + s) + (1 - before_last) * z * q
        def add(r, carry):
            at = pl.ds(pl.multiple_of(r * step_rows, step_rows), step_rows)
            mine_at = pl.ds(pl.multiple_of(row + r * step_rows, step_rows), step_rows)
            out_at = pl.ds(pl.multiple_of((s + 1) * sub + r * step_rows, step_rows), step_rows)
            total = part[mine_at, :].astype(F32) + pair_in[i, at, :].astype(F32)
            total = total + line_in[left, at, :].astype(F32) + line_in[right, at, :].astype(F32)
            head_v[out_at, :] = total
            return carry + jnp.sum((total * total).reshape(step_rows // 8, 8, emit), axis=0)
        square = lax.fori_loop(0, sub // step_rows, add, square)
        at = pl.ds(pl.multiple_of((s + 1) * sub, sub), sub)
        pltpu.make_async_copy(head_v.at[at, :], head_out.at[at, :], out_sem).start()
        return square

    def first_copy(j):
        place = dest(j // 2)
        side = unit_side(j)
        target, slot, sem = landing(place)
        return send(part.at[pl.ds(pl.multiple_of(block_row(place, side), sub), sub), :],
                    first_in.at[slot * 2 + side], first_send, first_recv.at[sem * 2 + side], target)

    def first_relay(j):
        @pl.when(middle == 1)
        def _():
            place = dest(j // 2)
            side = unit_side(j)
            row = pl.multiple_of(block_row(place, side), sub)
            wait_all(first_in.at[place * 2 + side], first_recv.at[place * 2 + side])
            def add(r, carry):
                at = pl.ds(pl.multiple_of(r * step_rows, step_rows), step_rows)
                mine_at = pl.ds(pl.multiple_of(row + r * step_rows, step_rows), step_rows)
                part[mine_at, :] = (
                    part[mine_at, :].astype(F32) + first_in[place * 2 + side, at, :].astype(F32)).astype(BF16)
                return carry
            lax.fori_loop(0, sub // step_rows, add, 0)
            first_copy(j).start()

    swap_copy = send(part.at[pl.ds(pl.multiple_of(block_row(z, 1 - x), sub), sub), :], swap_in,
                     swap_sem.at[0], swap_sem.at[1], partner)

    def first_wait(side):
        @pl.when(after_first == 1)
        def _():
            wait_all(first_in.at[zs * 2 + side], first_recv.at[zs * 2 + side])
        @pl.when(before_last == 1)
        def _():
            wait_all(first_in.at[(zs + 1) * 2 + side], first_recv.at[z * 2 + side])
        left = after_first * (zs * 2 + side) + (1 - after_first) * z * 2
        right = before_last * ((zs + 1) * 2 + side) + (1 - before_last) * z * 2
        return left, right

    def first_swap():
        row = block_row(z, 1 - x)
        left, right = first_wait(1 - x)
        def add(r, carry):
            at = pl.ds(pl.multiple_of(r * step_rows, step_rows), step_rows)
            mine_at = pl.ds(pl.multiple_of(row + r * step_rows, step_rows), step_rows)
            total = part[mine_at, :].astype(F32) + first_in[left, at, :].astype(F32)
            part[mine_at, :] = (total + first_in[right, at, :].astype(F32)).astype(BF16)
            return carry
        lax.fori_loop(0, sub // step_rows, add, 0)
        swap_copy.start()

    def first_finish(square):
        row = block_row(z, x)
        left, right = first_wait(x)
        swap_copy.wait_recv()
        def add(r, carry):
            at = pl.ds(pl.multiple_of(r * step_rows, step_rows), step_rows)
            mine_at = pl.ds(pl.multiple_of(row + r * step_rows, step_rows), step_rows)
            total = part[mine_at, :].astype(F32) + first_in[left, at, :].astype(F32)
            total = total + first_in[right, at, :].astype(F32) + swap_in[at, :].astype(F32)
            head_v[at, :] = total
            return carry + jnp.sum((total * total).reshape(step_rows // 8, 8, emit), axis=0)
        square = lax.fori_loop(0, sub // step_rows, add, square)
        pltpu.make_async_copy(head_v.at[pl.ds(0, sub), :], head_out.at[pl.ds(0, sub), :], out_sem).start()
        return square

    pre_copy(0, 0, 0).wait()
    step = 64
    for c, copy in enumerate(delta_copies):
        copy.wait()
        def narrow(r, carry):
            at = pl.ds(pl.multiple_of(c * chunk + r * step, step), step)
            low[at, :] = delta_v[at, :].astype(BF16)
            return carry
        lax.fori_loop(0, chunk // step, narrow, 0)
        at = pl.ds(c * chunk, chunk)
        p = pre_v[0, at, pl.ds(0, piece)].astype(F32)
        hidden = (p * jax.nn.sigmoid(p)).astype(BF16)
        value = lax.dot_general(hidden, low[at, :], (((0,), (0,)), ((), ())), preferred_element_type=F32)
        if c > 0:
            value = value + head_v[pl.ds(0, piece), :]
        if c < len(delta_copies) - 1:
            head_v[pl.ds(0, piece), :] = value
        else:
            part[pl.ds(pl.multiple_of(unit_row(0), piece), piece), :] = value.astype(BF16)

    pl.semaphore_wait(barrier, devices - 1)

    ready = piece // sub - 1
    @pl.when(middle == 0)
    def _():
        first_copy(0).start()
    for i in range(min(ready, q)):
        pair_copy(i).start()
    line_in[z * q] = jnp.zeros((sub, emit), BF16)
    first_in[z * 2] = jnp.zeros((sub, emit), BF16)

    wait_all(pre_v.at[pl.ds(0, firsts - 1), :, pl.ds(0, piece)], pre_sem.at[1])
    def opening(u, carry):
        product(u, 0)
        @pl.when(middle == 0)
        def _():
            first_copy(u).start()
        return carry
    lax.fori_loop(1, firsts, opening, 0)
    wait_all(pre_v.at[pl.ds(0, (2 * zs * hq - firsts) // hq)], pre_sem.at[2])
    if hq > 1:
        def second(t, carry):
            product(t // (hq - 1), 1 + t % (hq - 1))
            return carry
        lax.fori_loop(0, 3 * (hq - 1), second, 0)
    def more_pairs(i, carry):
        pair_copy(i).start()
        return carry
    lax.fori_loop(min(ready, q), lead, more_pairs, 0)
    first_relay(0)
    first_relay(1)
    weight_copy.wait()

    ids_copy.wait()
    for d in range(1, n):
        send(ids_all.at[me], ids_all.at[me], ids_send, ids_recv, lax.rem(me + d, n)).start()

    base = 3 + middle * (slopes - 8)
    stride = 3 - middle
    def main(t, carry):
        slope_sums(t)
        @pl.when((t >= 4) & (t % 2 == 0) & (t // 2 < firsts))
        def _():
            first_relay(t // 2)
        @pl.when((t >= base) & ((t - base) % stride == 0))
        def _():
            relay((t - base) // stride)
        return carry
    lax.fori_loop(0, slopes, main, 0)

    for d in range(1, heads):
        target = lax.rem(my_head + d, heads)
        pltpu.make_async_remote_copy(
            src_ref=small.at[target], dst_ref=small_in.at[lax.rem(my_head - target + heads, heads) - 1],
            send_sem=head_send, recv_sem=head_recv, device_id={"head": target}, device_id_type=MESH).start()

    done = slopes // 2
    if done < firsts:
        def rest_first(j, carry):
            first_relay(j)
            return carry
        lax.fori_loop(done, firsts, rest_first, 0)

    def add_rows(r, total):
        value = delta_v[pl.ds(pl.multiple_of(r * step, step), step), :]
        return total + jnp.sum(value.reshape(step // 8, 8, emit), axis=0)
    bias = lax.fori_loop(0, rows // step, add_rows, jnp.zeros((8, emit), F32))
    bias = jnp.sum(bias, axis=0, keepdims=True)
    pad = mine.shape[1] - spans
    tail = jnp.where(
        lax.broadcasted_iota(jnp.int32, (pad, emit), 0) == 0, jnp.broadcast_to(bias, (pad, emit)), 0.0
    ).astype(BF16)
    for h in range(2):
        mine[h, pl.ds(spans, pad), :] = tail[:, h * half:(h + 1) * half]

    ends = [(slopes - 4) // 3 + 1] + [(slopes - 4) // 3 + 1 + k for k in (2, 4, 5, 9, 11, 14)]
    inner = [3] + [3 + k for k in (1, 2, 4, 7, 9, 12)]
    stops = [(1 - middle) * e + middle * i for e, i in zip(ends, inner)] + [relays]

    if hq > 1:
        def third(t, carry):
            product(3 + t // (hq - 1), 1 + t % (hq - 1))
            return carry
        lax.fori_loop(0, (2 * zs - 5) * (hq - 1), third, 0)
    relay_range(stops[0], stops[1])
    def fourth(t, carry):
        product(2 * zs - 2 + t // hq, t % hq)
        return carry
    lax.fori_loop(0, 2 * hq, fourth, 0)
    first_swap()
    relay_range(stops[1], stops[2])
    relay_range(stops[2], stops[3])

    wait_all(small_in, head_recv)
    total = small[my_head].astype(F32)
    for d in range(heads - 1):
        total = total + small_in[d].astype(F32)
    for h in range(2):
        mine[h, pl.ds(0, spans), :] = total[:spans, h * half:(h + 1) * half].astype(BF16)
    embed_all[z, x] = total[spans:].astype(BF16)

    embed_pair = send(embed_all.at[z, x], embed_all.at[z, x], embed_pair_sem.at[0], embed_pair_sem.at[1], partner)
    embed_pair.start()

    roots = [zs // 2 - 1, zs // 2]
    def span_copy(h, right):
        return send(mine.at[h], span_in.at[h, 1 - right], span_send.at[h], span_recv.at[2 * h + 1 - right],
                    (z + 2 * right - 1) * 2 + x)
    def span_arrival(h, side):
        wait_all(span_in.at[h, side], span_recv.at[2 * h + side])
    for h in range(2):
        @pl.when(z == 0)
        def _():
            if roots[h] != 0:
                span_copy(h, 1).start()
        @pl.when(z == zs - 1)
        def _():
            if roots[h] != zs - 1:
                span_copy(h, 0).start()

    relay_range(stops[3], stops[4])

    def embed_copy(j, right):
        source = z + j - 2 * right * j
        return send(embed_all.at[source], embed_all.at[source], embed_send.at[right], embed_recv.at[source],
                    (z + 2 * right - 1) * 2 + x)

    def embed_step(j):
        if j > 0:
            @pl.when((z - (j - 1) >= 0) & (z < zs - 1))
            def _():
                embed_copy(j - 1, 1).wait_send()
            @pl.when((z + j - 1 <= zs - 1) & (z > 0))
            def _():
                embed_copy(j - 1, 0).wait_send()
            @pl.when(z - j >= 0)
            def _():
                wait_all(embed_all.at[z - j], embed_recv.at[z - j])
            @pl.when(z + j <= zs - 1)
            def _():
                wait_all(embed_all.at[z + j], embed_recv.at[z + j])
        if j < zs - 1:
            @pl.when((z - j >= 0) & (z < zs - 1))
            def _():
                embed_copy(j, 1).start()
            @pl.when((z + j <= zs - 1) & (z > 0))
            def _():
                embed_copy(j, 0).start()

    embed_pair.wait_recv()
    for h in range(2):
        for right, between in ((1, (z > 0) & (z < roots[h])), (0, (z < zs - 1) & (z > roots[h]))):
            @pl.when(between)
            def _():
                span_arrival(h, 1 - right)
                mine[h] = (mine[h].astype(F32) + span_in[h, 1 - right].astype(F32)).astype(BF16)
                span_copy(h, right).start()
    embed_step(0)

    relay_range(stops[4], stops[5])

    span_pair_copy = send(span_part, span_pair, span_pair_sem.at[0], span_pair_sem.at[1], partner)
    for h in range(2):
        @pl.when(z == roots[h])
        def _():
            total = mine[h].astype(F32)
            for side, there in ((0, roots[h] > 0), (1, roots[h] < zs - 1)):
                if there:
                    span_arrival(h, side)
                    total = total + span_in[h, side].astype(F32)
            span_part[...] = total.astype(BF16)
            span_pair_copy.start()
    embed_step(1)

    relay_range(stops[5], stops[6])

    def all_copy(h, d):
        return send(span_all.at[h], span_all.at[h], all_send, all_recv.at[h], lax.rem(z + d, zs) * 2 + x)
    for h in range(2):
        @pl.when(z == roots[h])
        def _():
            span_pair_copy.wait_recv()
            span_all[h] = (span_part[...].astype(F32) + span_pair[...].astype(F32)).astype(BF16)
            for d in range(1, zs):
                all_copy(h, d).start()
    for j in range(2, zs):
        embed_step(j)

    relay_range(stops[6], stops[7])
    square = jnp.zeros((8, emit), F32)
    square = first_finish(square)
    square = lax.fori_loop(0, 3, finish, square)

    wait_all(ids_all.at[pl.ds(0, n - 1)], ids_recv)
    wanted = lax.broadcasted_iota(jnp.int32, (clients, clients), 0) + me * clients
    embed_raw = jnp.zeros((clients, emit), F32)
    for c in range(n):
        chosen = (jnp.broadcast_to(ids_all[c], (clients, clients)) == wanted).astype(F32).astype(BF16)
        embed_raw = embed_raw + jnp.dot(chosen, embed_all[c // 2, c % 2], preferred_element_type=F32)
    embed_v[...] = embed_raw
    embed_write = pltpu.make_async_copy(embed_v, embed_out, write_sem.at[0])
    embed_write.start()
    embed_square = jnp.sum(embed_raw * embed_raw)

    rest_square = jnp.zeros((), F32)
    for h in range(2):
        @pl.when(z != roots[h])
        def _():
            wait_all(span_all.at[h], all_recv.at[h])
        value = span_all[h].astype(F32)
        rest_v[:, pl.ds(h * half, half)] = value
        rest_square = rest_square + jnp.sum(value * value)
    rest_write = pltpu.make_async_copy(rest_v, rest_out, write_sem.at[1])
    rest_write.start()

    square = lax.fori_loop(3, q, finish, square)
    head_total = jnp.sum(square)

    lane = lax.broadcasted_iota(jnp.int32, (1, 128), 1)
    stat_all[flat] = jnp.where(lane == 0, head_total, jnp.where(lane == 1, embed_square, rest_square / n))
    def tell(d, carry):
        pltpu.make_async_remote_copy(
            src_ref=stat_all.at[flat], dst_ref=stat_all.at[flat], send_sem=stat_send,
            recv_sem=stat_recv, device_id=device(d), device_id_type=MESH).start()
        return carry
    lax.fori_loop(1, devices, tell, 0)

    wait_all(part.at[pl.ds(0, zs * q * sub)], pair_send)
    for i in range(relays - queue, relays):
        line_copy(i).wait_send()
    wait_all(part.at[pl.ds(0, firsts * sub)], first_send)
    swap_copy.wait_send()
    embed_pair.wait_send()
    wait_all(small.at[pl.ds(0, heads - 1)], head_send)
    wait_all(ids_all.at[pl.ds(0, n - 1)], ids_send)
    for h in range(2):
        @pl.when(z < roots[h])
        def _():
            span_copy(h, 1).wait_send()
        @pl.when(z > roots[h])
        def _():
            span_copy(h, 0).wait_send()
        @pl.when(z == roots[h])
        def _():
            span_pair_copy.wait_send()
            wait_all(part.at[pl.ds(0, (zs - 1) * mine.shape[1] // 2)], all_send)
    embed_write.wait()
    rest_write.wait()
    pltpu.make_async_copy(head_v, head_out, out_sem).wait()

    wait_all(stat_all.at[pl.ds(0, devices - 1)], stat_recv)
    stat_out[...] = jnp.sum(stat_all[...], axis=0)
    wait_all(stat_all.at[pl.ds(0, devices - 1)], stat_send)


def scale_kernel(sizes, stat_ref, head_ref, rest_ref, embed_ref, head_out, bias_out, embed_out, span_out,
                 stat, head, rest, embed, in_sem, out_sem):
    head_size, embed_size, rest_size = sizes
    spans = span_out.shape[0]
    steps = in_sem.shape[0] - 3
    rows = head.shape[0] // steps
    stat_in = pltpu.make_async_copy(stat_ref, stat, in_sem.at[steps])
    rest_in = pltpu.make_async_copy(rest_ref, rest, in_sem.at[steps + 1])
    embed_in = pltpu.make_async_copy(embed_ref, embed, in_sem.at[steps + 2])
    def part(ref, i):
        return ref.at[pl.ds(i * rows, rows), :]
    stat_in.start()
    heads_in = [pltpu.make_async_copy(part(head_ref, i), part(head, i), in_sem.at[i]) for i in range(steps)]
    heads_out = [pltpu.make_async_copy(part(head, i), part(head_out, i), out_sem.at[i]) for i in range(steps)]
    for copy in heads_in:
        copy.start()
    rest_in.start()
    embed_in.start()
    stat_in.wait()
    factor = clip_factor(stat[0:1, 0:1], head_size)
    embed_factor = clip_factor(stat[0:1, 1:2], embed_size)
    rest_factor = clip_factor(stat[0:1, 2:3], rest_size)
    for i in range(steps):
        heads_in[i].wait()
        head[pl.ds(i * rows, rows), :] = factor * head[pl.ds(i * rows, rows), :]
        heads_out[i].start()
    rest_in.wait()
    rest[...] = rest_factor * rest[...]
    bias_copy = pltpu.make_async_copy(rest.at[pl.ds(spans, 1), :], bias_out, out_sem.at[steps])
    span_copy = pltpu.make_async_copy(rest.at[pl.ds(0, spans), :], span_out, out_sem.at[steps + 1])
    bias_copy.start()
    span_copy.start()
    embed_in.wait()
    embed[...] = embed_factor * embed[...]
    embed_copy = pltpu.make_async_copy(embed, embed_out, out_sem.at[steps + 2])
    embed_copy.start()
    for copy in heads_out + [bias_copy, span_copy, embed_copy]:
        copy.wait()


def per_device(n, heads, pre, delta, head_weight, client_ids):
    rows, hidden_width = pre.shape
    emit = delta.shape[1]
    clients = client_ids.shape[0]
    spans = rows // clients
    block = hidden_width // n
    piece = min(256, block)
    hq = block // piece
    zs = n // 2
    q = 7
    sub = block // (q + 1)
    padded = (spans + 16) // 16 * 16
    half = emit // 2
    cfg = (n, heads, block, piece, spans, clients)
    ids = client_ids.reshape(1, clients)
    hbm = pl.BlockSpec(memory_space=pl.ANY)
    vmem = pl.BlockSpec(memory_space=pltpu.VMEM)
    dma = pltpu.SemaphoreType.DMA
    chunk = math.gcd(rows, 256)
    head_raw, rest_raw, embed_raw, stats = pl.pallas_call(
        functools.partial(kernel, cfg),
        out_shape=(
            jax.ShapeDtypeStruct((block, emit), F32),
            jax.ShapeDtypeStruct((padded, emit), F32),
            jax.ShapeDtypeStruct((clients, emit), F32),
            jax.ShapeDtypeStruct((1, 128), F32),
        ),
        in_specs=[hbm, hbm, hbm, hbm],
        out_specs=(hbm, hbm, hbm, vmem),
        scratch_shapes=[
            pltpu.VMEM((n, rows, block), BF16),
            pltpu.VMEM((rows, emit), F32),
            pltpu.VMEM((rows, emit), BF16),
            pltpu.VMEM((hidden_width, emit), BF16),
            pltpu.VMEM((hidden_width, emit), BF16),
            pltpu.VMEM((zs * q, sub, emit), BF16),
            pltpu.VMEM(((zs + 2) * q, sub, emit), BF16),
            pltpu.VMEM(((zs + 2) * 2, sub, emit), BF16),
            pltpu.VMEM((sub, emit), BF16),
            pltpu.VMEM((block, emit), F32),
            pltpu.VMEM((heads, spans + clients, emit), BF16),
            pltpu.VMEM((heads - 1, spans + clients, emit), BF16),
            pltpu.VMEM((2, padded, half), BF16),
            pltpu.VMEM((2, 2, padded, half), BF16),
            pltpu.VMEM((padded, half), BF16),
            pltpu.VMEM((padded, half), BF16),
            pltpu.VMEM((2, padded, half), BF16),
            pltpu.VMEM((zs, 2, clients, emit), BF16),
            pltpu.VMEM((n, 1, clients), jnp.int32),
            pltpu.VMEM((clients, emit), F32),
            pltpu.VMEM((padded, emit), F32),
            pltpu.VMEM((n * heads, 1, 128), F32),
            dma((3,)), dma((rows // chunk,)), dma, dma,
            dma, dma((zs * q,)), dma((3,)), dma(((zs + 1) * q,)),
            dma, dma(((zs + 1) * 2,)), dma((2,)), dma, dma,
            dma((2,)), dma((4,)), dma((2,)), dma, dma((2,)), dma((2,)), dma((2,)), dma((2,)), dma((zs,)),
            dma, dma, dma, dma, dma,
        ],
        compiler_params=pltpu.CompilerParams(
            collective_id=0, has_side_effects=True, vmem_limit_bytes=62 * 2**20
        ),
        name="clipped_grads",
    )(pre, delta, head_weight, ids)
    sizes = (hidden_width * emit * heads, clients * n * hidden_width, spans * hidden_width + emit * heads)
    steps = 4
    head_grad, bias_grad, embed_grad, span_grad = pl.pallas_call(
        functools.partial(scale_kernel, sizes),
        out_shape=(
            jax.ShapeDtypeStruct((block, emit), F32),
            jax.ShapeDtypeStruct((1, emit), F32),
            jax.ShapeDtypeStruct((clients, emit), F32),
            jax.ShapeDtypeStruct((spans, emit), F32),
        ),
        in_specs=[hbm] * 4,
        out_specs=(hbm,) * 4,
        scratch_shapes=[
            pltpu.VMEM((1, 128), F32),
            pltpu.VMEM((block, emit), F32),
            pltpu.VMEM((padded, emit), F32),
            pltpu.VMEM((clients, emit), F32),
            dma((steps + 3,)), dma((steps + 3,)),
        ],
        name="scaled",
    )(stats, head_raw, rest_raw, embed_raw)
    return head_grad, bias_grad.reshape(emit), embed_grad, span_grad


def solution(mesh):
    placed = (P("client", None), P("client", "head"), P(None, "head"), P("client"))
    return jax.shard_map(
        functools.partial(per_device, mesh.shape["client"], mesh.shape["head"]),
        mesh=mesh,
        in_specs=placed,
        out_specs=(P("client", "head"), P("head"), P("client", "head"), P(None, "head")),
        check_vma=False,
    )
```

```python
import functools
import math

import jax
import jax.numpy as jnp
from jax import lax
from jax.experimental import pallas as pl
from jax.experimental.pallas import tpu as pltpu
from jax.sharding import PartitionSpec as P

EPSILON = 1e-06
MESH = pl.DeviceIdType.MESH
F32 = jnp.float32
BF16 = jnp.bfloat16


def clip_factor(total, number):
    return jnp.minimum(1.0, 1.0 / jnp.sqrt(total / number + EPSILON))


def kernel(cfg, pre_ref, delta_ref, weight_ref, ids_ref, head_out, rest_out, embed_out, stat_out,
           pre_v, delta_v, low, weight_v, part, pair_in, line_in, first_in, swap_in, head_v,
           small, small_in, mine, span_in, span_part, span_pair, span_all, embed_all, ids_all,
           embed_v, rest_v, stat_all,
           pre_sem, delta_sem, weight_sem, out_sem, pair_send, pair_recv, line_send, line_recv,
           first_send, first_recv, swap_sem, head_send, head_recv, span_send, span_recv, span_pair_sem,
           all_send, all_recv, write_sem, embed_pair_sem, embed_send, embed_recv, ids_sem, ids_send, ids_recv,
           stat_send, stat_recv):
    n, heads, block, piece, spans, clients = cfg
    zs = n // 2
    q = 7
    sub = block // (q + 1)
    hq = block // piece
    rows, emit = low.shape
    half = emit // 2
    me = lax.axis_index("client")
    my_head = lax.axis_index("head")
    z = me // 2
    x = me % 2
    relays = (zs - 1) * q
    firsts = 2 * (zs - 1)
    slopes = 2 * zs * hq
    devices = n * heads
    flat = me * heads + my_head

    after_first = (z + zs - 1) // zs
    before_last = (2 * zs - 2 - z) // zs
    middle = after_first * before_last
    upper = 2 * z // zs
    near = z + upper * (zs - 1 - 2 * z)
    partner = z * 2 + 1 - x

    def wait_all(ref, sem):
        pltpu.make_async_copy(ref, ref, sem).wait()

    def send(src, dst, send_sem, recv_sem, client):
        return pltpu.make_async_remote_copy(
            src_ref=src, dst_ref=dst, send_sem=send_sem, recv_sem=recv_sem,
            device_id={"client": client}, device_id_type=MESH)

    def dest(k):
        both = (2 * near - k - 1 + zs) // zs
        odd = k % 2
        out = both * (odd * (k // 2) + (1 - odd) * (zs - 1 - k // 2)) + (1 - both) * (zs - 1 - k + near)
        return out + upper * (zs - 1 - 2 * out)

    def block_row(place, side):
        return (place * 2 + side) * block

    def piece_row(place, side, s):
        return pl.multiple_of(block_row(place, side) + (s + 1) * sub, sub)

    def landing(place):
        right = (place - z + zs) // zs
        target = z + 2 * right - 1
        gap = right * (place - target) + (1 - right) * (target - place)
        away = (gap + zs - 1) // zs
        slot = away * place + (1 - away) * (zs + 1 - right)
        sem = away * place + (1 - away) * (right * zs + (1 - right) * place)
        return target * 2 + x, slot, sem

    def unit_side(u):
        return (x + 1 - u % 2) % 2

    def unit_row(u):
        return pl.multiple_of(block_row(dest(u // 2), unit_side(u)), block)

    def pre_copy(u, h, sem):
        columns = pl.ds(pl.multiple_of(unit_row(u) + h * piece, piece), piece)
        return pltpu.make_async_copy(
            pre_ref.at[:, columns], pre_v.at[u, :, pl.ds(pl.multiple_of(h * piece, piece), piece)], pre_sem.at[sem])

    chunk = math.gcd(rows, 256)
    delta_copies = [
        pltpu.make_async_copy(delta_ref.at[pl.ds(c * chunk, chunk), :], delta_v.at[pl.ds(c * chunk, chunk), :],
                              delta_sem.at[c])
        for c in range(rows // chunk)]
    weight_copy = pltpu.make_async_copy(weight_ref, weight_v, weight_sem)
    ids_copy = pltpu.make_async_copy(ids_ref, ids_all.at[me], ids_sem)
    pre_copy(0, 0, 0).start()
    for copy in delta_copies:
        copy.start()

    def device(d):
        other = lax.rem(flat + d, devices)
        return {"client": other // heads, "head": other % heads}

    barrier = pltpu.get_barrier_semaphore()
    def greet(d, carry):
        pl.semaphore_signal(barrier, inc=1, device_id=device(d), device_id_type=MESH)
        return carry
    lax.fori_loop(1, devices, greet, 0)

    def load(u, carry):
        pre_copy(u, 0, 1).start()
        return carry
    lax.fori_loop(1, firsts, load, 0)
    def load_rest(u, carry):
        @pl.when(u >= firsts)
        def _():
            pre_copy(u, 0, 2).start()
        for h in range(1, hq):
            pre_copy(u, h, 2).start()
        return carry
    lax.fori_loop(0 if hq > 1 else firsts, 2 * zs, load_rest, 0)
    weight_copy.start()
    ids_copy.start()

    def product(u, h):
        p = pre_v[u, :, pl.ds(pl.multiple_of(h * piece, piece), piece)].astype(F32)
        hidden = (p * jax.nn.sigmoid(p)).astype(BF16)
        value = lax.dot_general(hidden, low[...], (((0,), (0,)), ((), ())), preferred_element_type=F32)
        part[pl.ds(pl.multiple_of(unit_row(u) + h * piece, piece), piece), :] = value.astype(BF16)

    def slope_sums(t):
        u = t // hq
        h = t % hq
        p = pre_v[u, :, pl.ds(pl.multiple_of(h * piece, piece), piece)].astype(F32)
        row = pl.multiple_of(unit_row(u) + h * piece, piece)
        value = lax.dot_general(
            low[...], weight_v[pl.ds(row, piece), :], (((1,), (1,)), ((), ())), preferred_element_type=F32)
        s = jax.nn.sigmoid(p)
        grad = value.astype(BF16).astype(F32) * (s * (1.0 + p * (1.0 - s)))
        grad = grad.reshape(clients, spans, piece)
        to = row // emit
        columns = pl.ds(pl.multiple_of(row % emit, piece), piece)
        small[to, pl.ds(0, spans), columns] = jnp.sum(grad, axis=0).astype(BF16)
        small[to, pl.ds(spans, clients), columns] = jnp.sum(grad, axis=1).astype(BF16)

    def pair_copy(i):
        return send(part.at[pl.ds(piece_row(dest(i // q), 1 - x, i % q), sub), :], pair_in.at[i],
                    pair_send, pair_recv.at[i], partner)

    queue = 3

    def line_copy(i):
        place = dest(i // q)
        target, slot, sem = landing(place)
        return send(part.at[pl.ds(piece_row(place, x, i % q), sub), :], line_in.at[slot * q + i % q],
                    line_send.at[i % queue], line_recv.at[sem * q + i % q], target)

    lead = q + 2 * middle
    step_rows = min(32, sub)

    def relay(i, ahead):
        place = dest(i // q)
        row = piece_row(place, x, i % q)
        pair_copy(i).wait_recv()
        @pl.when(middle == 1)
        def _():
            wait_all(line_in.at[place * q + i % q], line_recv.at[place * q + i % q])
        slot = middle * (place * q + i % q) + (1 - middle) * z * q
        def add(r, carry):
            at = pl.ds(pl.multiple_of(r * step_rows, step_rows), step_rows)
            mine_at = pl.ds(pl.multiple_of(row + r * step_rows, step_rows), step_rows)
            total = part[mine_at, :].astype(F32) + pair_in[i, at, :].astype(F32)
            part[mine_at, :] = (total + line_in[slot, at, :].astype(F32)).astype(BF16)
            return carry
        lax.fori_loop(0, sub // step_rows, add, 0)
        @pl.when(i >= queue)
        def _():
            line_copy(i - queue).wait_send()
        line_copy(i).start()
        @pl.when(i + ahead < zs * q)
        def _():
            pair_copy(i + ahead).start()

    def relay_range(start, stop, ahead):
        def body(i, carry):
            relay(i, ahead)
            return carry
        lax.fori_loop(start, stop, body, 0)

    def finish(s, square):
        i = relays + s
        row = piece_row(z, x, s)
        pair_copy(i).wait_recv()
        @pl.when(after_first == 1)
        def _():
            wait_all(line_in.at[zs * q + s], line_recv.at[zs * q + s])
        @pl.when(before_last == 1)
        def _():
            wait_all(line_in.at[(zs + 1) * q + s], line_recv.at[z * q + s])
        left = after_first * (zs * q + s) + (1 - after_first) * z * q
        right = before_last * ((zs + 1) * q + s) + (1 - before_last) * z * q
        def add(r, carry):
            at = pl.ds(pl.multiple_of(r * step_rows, step_rows), step_rows)
            mine_at = pl.ds(pl.multiple_of(row + r * step_rows, step_rows), step_rows)
            out_at = pl.ds(pl.multiple_of((s + 1) * sub + r * step_rows, step_rows), step_rows)
            total = part[mine_at, :].astype(F32) + pair_in[i, at, :].astype(F32)
            total = total + line_in[left, at, :].astype(F32) + line_in[right, at, :].astype(F32)
            head_v[out_at, :] = total
            return carry + jnp.sum((total * total).reshape(step_rows // 8, 8, emit), axis=0)
        square = lax.fori_loop(0, sub // step_rows, add, square)
        at = pl.ds(pl.multiple_of((s + 1) * sub, sub), sub)
        pltpu.make_async_copy(head_v.at[at, :], head_out.at[at, :], out_sem).start()
        return square

    def first_copy(j):
        place = dest(j // 2)
        side = unit_side(j)
        target, slot, sem = landing(place)
        return send(part.at[pl.ds(pl.multiple_of(block_row(place, side), sub), sub), :],
                    first_in.at[slot * 2 + side], first_send, first_recv.at[sem * 2 + side], target)

    def first_relay(j):
        @pl.when(middle == 1)
        def _():
            place = dest(j // 2)
            side = unit_side(j)
            row = pl.multiple_of(block_row(place, side), sub)
            wait_all(first_in.at[place * 2 + side], first_recv.at[place * 2 + side])
            def add(r, carry):
                at = pl.ds(pl.multiple_of(r * step_rows, step_rows), step_rows)
                mine_at = pl.ds(pl.multiple_of(row + r * step_rows, step_rows), step_rows)
                part[mine_at, :] = (
                    part[mine_at, :].astype(F32) + first_in[place * 2 + side, at, :].astype(F32)).astype(BF16)
                return carry
            lax.fori_loop(0, sub // step_rows, add, 0)
            first_copy(j).start()

    swap_copy = send(part.at[pl.ds(pl.multiple_of(block_row(z, 1 - x), sub), sub), :], swap_in,
                     swap_sem.at[0], swap_sem.at[1], partner)

    def first_wait(side):
        @pl.when(after_first == 1)
        def _():
            wait_all(first_in.at[zs * 2 + side], first_recv.at[zs * 2 + side])
        @pl.when(before_last == 1)
        def _():
            wait_all(first_in.at[(zs + 1) * 2 + side], first_recv.at[z * 2 + side])
        left = after_first * (zs * 2 + side) + (1 - after_first) * z * 2
        right = before_last * ((zs + 1) * 2 + side) + (1 - before_last) * z * 2
        return left, right

    def first_swap():
        row = block_row(z, 1 - x)
        left, right = first_wait(1 - x)
        def add(r, carry):
            at = pl.ds(pl.multiple_of(r * step_rows, step_rows), step_rows)
            mine_at = pl.ds(pl.multiple_of(row + r * step_rows, step_rows), step_rows)
            total = part[mine_at, :].astype(F32) + first_in[left, at, :].astype(F32)
            part[mine_at, :] = (total + first_in[right, at, :].astype(F32)).astype(BF16)
            return carry
        lax.fori_loop(0, sub // step_rows, add, 0)
        swap_copy.start()

    def first_finish(square):
        row = block_row(z, x)
        left, right = first_wait(x)
        swap_copy.wait_recv()
        def add(r, carry):
            at = pl.ds(pl.multiple_of(r * step_rows, step_rows), step_rows)
            mine_at = pl.ds(pl.multiple_of(row + r * step_rows, step_rows), step_rows)
            total = part[mine_at, :].astype(F32) + first_in[left, at, :].astype(F32)
            total = total + first_in[right, at, :].astype(F32) + swap_in[at, :].astype(F32)
            head_v[at, :] = total
            return carry + jnp.sum((total * total).reshape(step_rows // 8, 8, emit), axis=0)
        square = lax.fori_loop(0, sub // step_rows, add, square)
        pltpu.make_async_copy(head_v.at[pl.ds(0, sub), :], head_out.at[pl.ds(0, sub), :], out_sem).start()
        return square

    pre_copy(0, 0, 0).wait()
    step = 64
    for c, copy in enumerate(delta_copies):
        copy.wait()
        def narrow(r, carry):
            at = pl.ds(pl.multiple_of(c * chunk + r * step, step), step)
            low[at, :] = delta_v[at, :].astype(BF16)
            return carry
        lax.fori_loop(0, chunk // step, narrow, 0)
        at = pl.ds(c * chunk, chunk)
        p = pre_v[0, at, pl.ds(0, piece)].astype(F32)
        hidden = (p * jax.nn.sigmoid(p)).astype(BF16)
        value = lax.dot_general(hidden, low[at, :], (((0,), (0,)), ((), ())), preferred_element_type=F32)
        if c > 0:
            value = value + head_v[pl.ds(0, piece), :]
        if c < len(delta_copies) - 1:
            head_v[pl.ds(0, piece), :] = value
        else:
            part[pl.ds(pl.multiple_of(unit_row(0), piece), piece), :] = value.astype(BF16)

    pl.semaphore_wait(barrier, devices - 1)

    ready = piece // sub - 1
    @pl.when(middle == 0)
    def _():
        first_copy(0).start()
    for i in range(min(ready, q)):
        pair_copy(i).start()
    line_in[z * q] = jnp.zeros((sub, emit), BF16)
    first_in[z * 2] = jnp.zeros((sub, emit), BF16)

    wait_all(pre_v.at[pl.ds(0, firsts - 1), :, pl.ds(0, piece)], pre_sem.at[1])
    def opening(u, carry):
        product(u, 0)
        @pl.when(middle == 0)
        def _():
            first_copy(u).start()
        return carry
    lax.fori_loop(1, firsts, opening, 0)
    wait_all(pre_v.at[pl.ds(0, (2 * zs * hq - firsts) // hq)], pre_sem.at[2])
    if hq > 1:
        def second(t, carry):
            product(t // (hq - 1), 1 + t % (hq - 1))
            return carry
        lax.fori_loop(0, 3 * (hq - 1), second, 0)
    def more_pairs(i, carry):
        pair_copy(i).start()
        return carry
    lax.fori_loop(min(ready, q), lead, more_pairs, 0)
    first_relay(0)
    first_relay(1)
    weight_copy.wait()

    ids_copy.wait()
    for d in range(1, n):
        send(ids_all.at[me], ids_all.at[me], ids_send, ids_recv, lax.rem(me + d, n)).start()

    base = 3 + middle * (slopes - 8)
    stride = 3 - middle
    def main(t, carry):
        slope_sums(t)
        @pl.when((t >= 4) & (t % 2 == 0) & (t // 2 < firsts))
        def _():
            first_relay(t // 2)
        @pl.when((t >= base) & ((t - base) % stride == 0))
        def _():
            relay((t - base) // stride, lead)
        return carry
    lax.fori_loop(0, slopes, main, 0)

    for d in range(1, heads):
        target = lax.rem(my_head + d, heads)
        pltpu.make_async_remote_copy(
            src_ref=small.at[target], dst_ref=small_in.at[lax.rem(my_head - target + heads, heads) - 1],
            send_sem=head_send, recv_sem=head_recv, device_id={"head": target}, device_id_type=MESH).start()

    done = slopes // 2
    if done < firsts:
        def rest_first(j, carry):
            first_relay(j)
            return carry
        lax.fori_loop(done, firsts, rest_first, 0)

    def add_rows(r, total):
        value = delta_v[pl.ds(pl.multiple_of(r * step, step), step), :]
        return total + jnp.sum(value.reshape(step // 8, 8, emit), axis=0)
    bias = lax.fori_loop(0, rows // step, add_rows, jnp.zeros((8, emit), F32))
    bias = jnp.sum(bias, axis=0, keepdims=True)
    pad = mine.shape[1] - spans
    tail = jnp.where(
        lax.broadcasted_iota(jnp.int32, (pad, emit), 0) == 0, jnp.broadcast_to(bias, (pad, emit)), 0.0
    ).astype(BF16)
    for h in range(2):
        mine[h, pl.ds(spans, pad), :] = tail[:, h * half:(h + 1) * half]

    ends = [(slopes - 4) // 3 + 1] + [(slopes - 4) // 3 + 1 + k for k in (2, 4, 4, 8, 13, 16)]
    inner = [3] + [3 + k for k in (1, 2, 3, 7, 11, 15)]
    stops = [(1 - middle) * e + middle * i for e, i in zip(ends, inner)] + [relays]

    if hq > 1:
        def third(t, carry):
            product(3 + t // (hq - 1), 1 + t % (hq - 1))
            return carry
        lax.fori_loop(0, (2 * zs - 5) * (hq - 1), third, 0)
    relay_range(stops[0], stops[1], lead)
    def fourth(t, carry):
        product(2 * zs - 2 + t // hq, t % hq)
        return carry
    lax.fori_loop(0, 2 * hq, fourth, 0)
    relay_range(stops[1], stops[2], lead)
    relay_range(stops[2], stops[3], lead)

    wait_all(small_in, head_recv)
    total = small[my_head].astype(F32)
    for d in range(heads - 1):
        total = total + small_in[d].astype(F32)
    for h in range(2):
        mine[h, pl.ds(0, spans), :] = total[:spans, h * half:(h + 1) * half].astype(BF16)
    embed_all[z, x] = total[spans:].astype(BF16)

    embed_pair = send(embed_all.at[z, x], embed_all.at[z, x], embed_pair_sem.at[0], embed_pair_sem.at[1], partner)
    embed_pair.start()
    @pl.when(middle == 1)
    def _():
        pair_copy(stops[3] + lead).start()
    lead = lead + middle

    roots = [zs // 2 - 1, zs // 2]
    def span_copy(h, right):
        return send(mine.at[h], span_in.at[h, 1 - right], span_send.at[h], span_recv.at[2 * h + 1 - right],
                    (z + 2 * right - 1) * 2 + x)
    def span_arrival(h, side):
        wait_all(span_in.at[h, side], span_recv.at[2 * h + side])
    for h in range(2):
        @pl.when(z == 0)
        def _():
            if roots[h] != 0:
                span_copy(h, 1).start()
        @pl.when(z == zs - 1)
        def _():
            if roots[h] != zs - 1:
                span_copy(h, 0).start()

    relay_range(stops[3], stops[4], lead)

    def embed_copy(j, right):
        source = z + j - 2 * right * j
        return send(embed_all.at[source], embed_all.at[source], embed_send.at[right], embed_recv.at[source],
                    (z + 2 * right - 1) * 2 + x)

    def embed_step(j):
        for right, near_end, there in ((1, before_last, z - j >= 0), (0, after_first, z + j <= zs - 1)):
            @pl.when((near_end == 1) & there)
            def _():
                if j > 0:
                    source = z + j - 2 * right * j
                    wait_all(embed_all.at[source], embed_recv.at[source])
                    embed_copy(j - 1, right).wait_send()
                embed_copy(j, right).start()

    embed_pair.wait_recv()
    for h in range(2):
        for right, between in ((1, (z > 0) & (z < roots[h])), (0, (z < zs - 1) & (z > roots[h]))):
            @pl.when(between)
            def _():
                span_arrival(h, 1 - right)
                mine[h] = (mine[h].astype(F32) + span_in[h, 1 - right].astype(F32)).astype(BF16)
                span_copy(h, right).start()
    embed_step(0)

    relay_range(stops[4], stops[5], lead)

    span_pair_copy = send(span_part, span_pair, span_pair_sem.at[0], span_pair_sem.at[1], partner)
    for h in range(2):
        @pl.when(z == roots[h])
        def _():
            total = mine[h].astype(F32)
            for side, there in ((0, roots[h] > 0), (1, roots[h] < zs - 1)):
                if there:
                    span_arrival(h, side)
                    total = total + span_in[h, side].astype(F32)
            span_part[...] = total.astype(BF16)
            span_pair_copy.start()
    first_swap()
    embed_step(1)

    relay_range(stops[5], stops[6], lead)

    def all_copy(h, d):
        return send(span_all.at[h], span_all.at[h], all_send, all_recv.at[h], lax.rem(z + d, zs) * 2 + x)
    for h in range(2):
        @pl.when(z == roots[h])
        def _():
            span_pair_copy.wait_recv()
            span_all[h] = (span_part[...].astype(F32) + span_pair[...].astype(F32)).astype(BF16)
            for d in range(1, zs):
                all_copy(h, d).start()
    for j in range(2, zs - 1):
        embed_step(j)

    relay_range(stops[6], stops[7], lead)
    square = jnp.zeros((8, emit), F32)
    square = first_finish(square)
    square = lax.fori_loop(0, 5, finish, square)

    for j in range(1, zs):
        for right, near_end, there in ((1, before_last, z - j >= 0), (0, after_first, z + j <= zs - 1)):
            source = z + j - 2 * right * j
            @pl.when(there if j == zs - 1 else (near_end == 0) & there)
            def _():
                wait_all(embed_all.at[source], embed_recv.at[source])
    for right, near_end, last in ((1, before_last, z), (0, after_first, zs - 1 - z)):
        for j in range(zs - 1):
            @pl.when((near_end == 1) & (last == j))
            def _():
                embed_copy(j, right).wait_send()
    wait_all(ids_all.at[pl.ds(0, n - 1)], ids_recv)
    wanted = lax.broadcasted_iota(jnp.int32, (clients, clients), 0) + me * clients
    embed_raw = jnp.zeros((clients, emit), F32)
    for c in range(n):
        chosen = (jnp.broadcast_to(ids_all[c], (clients, clients)) == wanted).astype(F32).astype(BF16)
        embed_raw = embed_raw + jnp.dot(chosen, embed_all[c // 2, c % 2], preferred_element_type=F32)
    embed_v[...] = embed_raw
    embed_write = pltpu.make_async_copy(embed_v, embed_out, write_sem.at[0])
    embed_write.start()
    embed_square = jnp.sum(embed_raw * embed_raw)

    rest_square = jnp.zeros((), F32)
    for h in range(2):
        @pl.when(z != roots[h])
        def _():
            wait_all(span_all.at[h], all_recv.at[h])
        value = span_all[h].astype(F32)
        rest_v[:, pl.ds(h * half, half)] = value
        rest_square = rest_square + jnp.sum(value * value)
    rest_write = pltpu.make_async_copy(rest_v, rest_out, write_sem.at[1])
    rest_write.start()

    square = lax.fori_loop(5, q, finish, square)
    head_total = jnp.sum(square)

    lane = lax.broadcasted_iota(jnp.int32, (1, 128), 1)
    stat_all[flat] = jnp.where(lane == 0, head_total, jnp.where(lane == 1, embed_square, rest_square / n))
    def tell(d, carry):
        pltpu.make_async_remote_copy(
            src_ref=stat_all.at[flat], dst_ref=stat_all.at[flat], send_sem=stat_send,
            recv_sem=stat_recv, device_id=device(d), device_id_type=MESH).start()
        return carry
    lax.fori_loop(1, devices, tell, 0)

    wait_all(part.at[pl.ds(0, zs * q * sub)], pair_send)
    for i in range(relays - queue, relays):
        line_copy(i).wait_send()
    wait_all(part.at[pl.ds(0, firsts * sub)], first_send)
    swap_copy.wait_send()
    embed_pair.wait_send()
    wait_all(small.at[pl.ds(0, heads - 1)], head_send)
    wait_all(ids_all.at[pl.ds(0, n - 1)], ids_send)
    for h in range(2):
        @pl.when(z < roots[h])
        def _():
            span_copy(h, 1).wait_send()
        @pl.when(z > roots[h])
        def _():
            span_copy(h, 0).wait_send()
        @pl.when(z == roots[h])
        def _():
            span_pair_copy.wait_send()
            wait_all(part.at[pl.ds(0, (zs - 1) * mine.shape[1] // 2)], all_send)
    embed_write.wait()
    rest_write.wait()
    pltpu.make_async_copy(head_v, head_out, out_sem).wait()

    wait_all(stat_all.at[pl.ds(0, devices - 1)], stat_recv)
    stat_out[...] = jnp.sum(stat_all[...], axis=0)
    wait_all(stat_all.at[pl.ds(0, devices - 1)], stat_send)


def scale_kernel(sizes, stat_ref, head_ref, rest_ref, embed_ref, head_out, bias_out, embed_out, span_out,
                 stat, head, rest, embed, in_sem, out_sem):
    head_size, embed_size, rest_size = sizes
    spans = span_out.shape[0]
    steps = in_sem.shape[0] - 3
    rows = head.shape[0] // steps
    stat_in = pltpu.make_async_copy(stat_ref, stat, in_sem.at[steps])
    rest_in = pltpu.make_async_copy(rest_ref, rest, in_sem.at[steps + 1])
    embed_in = pltpu.make_async_copy(embed_ref, embed, in_sem.at[steps + 2])
    def part(ref, i):
        return ref.at[pl.ds(i * rows, rows), :]
    stat_in.start()
    heads_in = [pltpu.make_async_copy(part(head_ref, i), part(head, i), in_sem.at[i]) for i in range(steps)]
    heads_out = [pltpu.make_async_copy(part(head, i), part(head_out, i), out_sem.at[i]) for i in range(steps)]
    for copy in heads_in:
        copy.start()
    rest_in.start()
    embed_in.start()
    stat_in.wait()
    factor = clip_factor(stat[0:1, 0:1], head_size)
    embed_factor = clip_factor(stat[0:1, 1:2], embed_size)
    rest_factor = clip_factor(stat[0:1, 2:3], rest_size)
    for i in range(steps):
        heads_in[i].wait()
        head[pl.ds(i * rows, rows), :] = factor * head[pl.ds(i * rows, rows), :]
        heads_out[i].start()
    rest_in.wait()
    rest[...] = rest_factor * rest[...]
    bias_copy = pltpu.make_async_copy(rest.at[pl.ds(spans, 1), :], bias_out, out_sem.at[steps])
    span_copy = pltpu.make_async_copy(rest.at[pl.ds(0, spans), :], span_out, out_sem.at[steps + 1])
    bias_copy.start()
    span_copy.start()
    embed_in.wait()
    embed[...] = embed_factor * embed[...]
    embed_copy = pltpu.make_async_copy(embed, embed_out, out_sem.at[steps + 2])
    embed_copy.start()
    for copy in heads_out + [bias_copy, span_copy, embed_copy]:
        copy.wait()


def per_device(n, heads, pre, delta, head_weight, client_ids):
    rows, hidden_width = pre.shape
    emit = delta.shape[1]
    clients = client_ids.shape[0]
    spans = rows // clients
    block = hidden_width // n
    piece = min(256, block)
    hq = block // piece
    zs = n // 2
    q = 7
    sub = block // (q + 1)
    padded = (spans + 16) // 16 * 16
    half = emit // 2
    cfg = (n, heads, block, piece, spans, clients)
    ids = client_ids.reshape(1, clients)
    hbm = pl.BlockSpec(memory_space=pl.ANY)
    vmem = pl.BlockSpec(memory_space=pltpu.VMEM)
    dma = pltpu.SemaphoreType.DMA
    chunk = math.gcd(rows, 256)
    head_raw, rest_raw, embed_raw, stats = pl.pallas_call(
        functools.partial(kernel, cfg),
        out_shape=(
            jax.ShapeDtypeStruct((block, emit), F32),
            jax.ShapeDtypeStruct((padded, emit), F32),
            jax.ShapeDtypeStruct((clients, emit), F32),
            jax.ShapeDtypeStruct((1, 128), F32),
        ),
        in_specs=[hbm, hbm, hbm, hbm],
        out_specs=(hbm, hbm, hbm, vmem),
        scratch_shapes=[
            pltpu.VMEM((n, rows, block), BF16),
            pltpu.VMEM((rows, emit), F32),
            pltpu.VMEM((rows, emit), BF16),
            pltpu.VMEM((hidden_width, emit), BF16),
            pltpu.VMEM((hidden_width, emit), BF16),
            pltpu.VMEM((zs * q, sub, emit), BF16),
            pltpu.VMEM(((zs + 2) * q, sub, emit), BF16),
            pltpu.VMEM(((zs + 2) * 2, sub, emit), BF16),
            pltpu.VMEM((sub, emit), BF16),
            pltpu.VMEM((block, emit), F32),
            pltpu.VMEM((heads, spans + clients, emit), BF16),
            pltpu.VMEM((heads - 1, spans + clients, emit), BF16),
            pltpu.VMEM((2, padded, half), BF16),
            pltpu.VMEM((2, 2, padded, half), BF16),
            pltpu.VMEM((padded, half), BF16),
            pltpu.VMEM((padded, half), BF16),
            pltpu.VMEM((2, padded, half), BF16),
            pltpu.VMEM((zs, 2, clients, emit), BF16),
            pltpu.VMEM((n, 1, clients), jnp.int32),
            pltpu.VMEM((clients, emit), F32),
            pltpu.VMEM((padded, emit), F32),
            pltpu.VMEM((n * heads, 1, 128), F32),
            dma((3,)), dma((rows // chunk,)), dma, dma,
            dma, dma((zs * q,)), dma((3,)), dma(((zs + 1) * q,)),
            dma, dma(((zs + 1) * 2,)), dma((2,)), dma, dma,
            dma((2,)), dma((4,)), dma((2,)), dma, dma((2,)), dma((2,)), dma((2,)), dma((2,)), dma((zs,)),
            dma, dma, dma, dma, dma,
        ],
        compiler_params=pltpu.CompilerParams(
            collective_id=0, has_side_effects=True, vmem_limit_bytes=62 * 2**20
        ),
        name="clipped_grads",
    )(pre, delta, head_weight, ids)
    sizes = (hidden_width * emit * heads, clients * n * hidden_width, spans * hidden_width + emit * heads)
    steps = 4
    head_grad, bias_grad, embed_grad, span_grad = pl.pallas_call(
        functools.partial(scale_kernel, sizes),
        out_shape=(
            jax.ShapeDtypeStruct((block, emit), F32),
            jax.ShapeDtypeStruct((1, emit), F32),
            jax.ShapeDtypeStruct((clients, emit), F32),
            jax.ShapeDtypeStruct((spans, emit), F32),
        ),
        in_specs=[hbm] * 4,
        out_specs=(hbm,) * 4,
        scratch_shapes=[
            pltpu.VMEM((1, 128), F32),
            pltpu.VMEM((block, emit), F32),
            pltpu.VMEM((padded, emit), F32),
            pltpu.VMEM((clients, emit), F32),
            dma((steps + 3,)), dma((steps + 3,)),
        ],
        name="scaled",
    )(stats, head_raw, rest_raw, embed_raw)
    return head_grad, bias_grad.reshape(emit), embed_grad, span_grad


def solution(mesh):
    placed = (P("client", None), P("client", "head"), P(None, "head"), P("client"))
    return jax.shard_map(
        functools.partial(per_device, mesh.shape["client"], mesh.shape["head"]),
        mesh=mesh,
        in_specs=placed,
        out_specs=(P("client", "head"), P("head"), P("client", "head"), P(None, "head")),
        check_vma=False,
    )
```

```python
import functools
import math

import jax
import jax.numpy as jnp
from jax import lax
from jax.experimental import pallas as pl
from jax.experimental.pallas import tpu as pltpu
from jax.sharding import PartitionSpec as P

EPSILON = 1e-06
MESH = pl.DeviceIdType.MESH
F32 = jnp.float32
BF16 = jnp.bfloat16


def clip_factor(total, number):
    return jnp.minimum(1.0, 1.0 / jnp.sqrt(total / number + EPSILON))


def kernel(cfg, pre_ref, delta_ref, weight_ref, ids_ref, head_out, rest_out, embed_out, stat_out,
           pre_v, delta_v, low, weight_v, part, pair_in, line_in, first_in, swap_in, head_v,
           small, small_in, mine, span_in, span_part, span_pair, span_all, embed_all, ids_all,
           embed_v, rest_v, stat_all,
           pre_sem, first_pre_sem, delta_sem, weight_sem, out_sem, pair_send, pair_recv, line_send, line_recv,
           first_send, first_recv, swap_sem, head_send, head_recv, span_send, span_recv, span_pair_sem,
           all_send, all_recv, write_sem, embed_pair_sem, embed_send, embed_recv, ids_sem, ids_send, ids_recv,
           stat_send, stat_recv):
    n, heads, block, piece, spans, clients = cfg
    zs = n // 2
    q = 7
    sub = block // (q + 1)
    hq = block // piece
    rows, emit = low.shape
    half = emit // 2
    me = lax.axis_index("client")
    my_head = lax.axis_index("head")
    z = me // 2
    x = me % 2
    relays = (zs - 1) * q
    firsts = 2 * (zs - 1)
    slopes = 2 * zs * hq
    devices = n * heads
    flat = me * heads + my_head

    after_first = (z + zs - 1) // zs
    before_last = (2 * zs - 2 - z) // zs
    middle = after_first * before_last
    upper = 2 * z // zs
    near = z + upper * (zs - 1 - 2 * z)
    partner = z * 2 + 1 - x

    def wait_all(ref, sem):
        pltpu.make_async_copy(ref, ref, sem).wait()

    def send(src, dst, send_sem, recv_sem, client):
        return pltpu.make_async_remote_copy(
            src_ref=src, dst_ref=dst, send_sem=send_sem, recv_sem=recv_sem,
            device_id={"client": client}, device_id_type=MESH)

    def dest(k):
        both = (2 * near - k - 1 + zs) // zs
        odd = k % 2
        out = both * (odd * (k // 2) + (1 - odd) * (zs - 1 - k // 2)) + (1 - both) * (zs - 1 - k + near)
        return out + upper * (zs - 1 - 2 * out)

    def block_row(place, side):
        return (place * 2 + side) * block

    def piece_row(place, side, s):
        return pl.multiple_of(block_row(place, side) + (s + 1) * sub, sub)

    def landing(place):
        right = (place - z + zs) // zs
        target = z + 2 * right - 1
        gap = right * (place - target) + (1 - right) * (target - place)
        away = (gap + zs - 1) // zs
        slot = away * place + (1 - away) * (zs + 1 - right)
        sem = away * place + (1 - away) * (right * zs + (1 - right) * place)
        return target * 2 + x, slot, sem

    def unit_side(u):
        return (x + 1 - u % 2) % 2

    def unit_row(u):
        return pl.multiple_of(block_row(dest(u // 2), unit_side(u)), block)

    def pre_copy(u, h, sem):
        columns = pl.ds(pl.multiple_of(unit_row(u) + h * piece, piece), piece)
        return pltpu.make_async_copy(
            pre_ref.at[:, columns], pre_v.at[u, :, pl.ds(pl.multiple_of(h * piece, piece), piece)], pre_sem.at[sem])

    chunk = math.gcd(rows, 256)
    delta_copies = [
        pltpu.make_async_copy(delta_ref.at[pl.ds(c * chunk, chunk), :], delta_v.at[pl.ds(c * chunk, chunk), :],
                              delta_sem.at[c])
        for c in range(rows // chunk)]
    weight_copy = pltpu.make_async_copy(weight_ref, weight_v, weight_sem)
    ids_copy = pltpu.make_async_copy(ids_ref, ids_all.at[me], ids_sem)
    first_column = pl.multiple_of(unit_row(0), piece)
    first_copies = [
        pltpu.make_async_copy(pre_ref.at[pl.ds(c * chunk, chunk), pl.ds(first_column, piece)],
                              pre_v.at[0, pl.ds(c * chunk, chunk), pl.ds(0, piece)], first_pre_sem.at[c])
        for c in range(rows // chunk)]
    for c in range(rows // chunk):
        first_copies[c].start()
        delta_copies[c].start()

    def each_other(action):
        columns = [lax.rem(my_head + d, heads) for d in range(heads)]
        for column in columns[1:]:
            action(me, column)
        def body(d, carry):
            client = lax.rem(me + d, n)
            for column in columns:
                action(client, column)
            return carry
        lax.fori_loop(1, n, body, 0)

    barrier = pltpu.get_barrier_semaphore()
    def greet(client, head):
        pl.semaphore_signal(barrier, inc=1, device_id={"client": client, "head": head}, device_id_type=MESH)
    each_other(greet)

    def load(u, carry):
        pre_copy(u, 0, 0).start()
        return carry
    def load_rest(u, carry):
        @pl.when(u >= firsts)
        def _():
            pre_copy(u, 0, 1).start()
        for h in range(1, hq):
            pre_copy(u, h, 1).start()
        return carry

    def product(u, h):
        p = pre_v[u, :, pl.ds(pl.multiple_of(h * piece, piece), piece)].astype(F32)
        hidden = (p * jax.nn.sigmoid(p)).astype(BF16)
        value = lax.dot_general(hidden, low[...], (((0,), (0,)), ((), ())), preferred_element_type=F32)
        part[pl.ds(pl.multiple_of(unit_row(u) + h * piece, piece), piece), :] = value.astype(BF16)

    def slope_sums(t):
        u = t // hq
        h = t % hq
        p = pre_v[u, :, pl.ds(pl.multiple_of(h * piece, piece), piece)].astype(F32)
        row = pl.multiple_of(unit_row(u) + h * piece, piece)
        value = lax.dot_general(
            low[...], weight_v[pl.ds(row, piece), :], (((1,), (1,)), ((), ())), preferred_element_type=F32)
        s = jax.nn.sigmoid(p)
        grad = value.astype(BF16).astype(F32) * (s * (1.0 + p * (1.0 - s)))
        grad = grad.reshape(clients, spans, piece)
        to = row // emit
        columns = pl.ds(pl.multiple_of(row % emit, piece), piece)
        small[to, pl.ds(0, spans), columns] = jnp.sum(grad, axis=0).astype(BF16)
        small[to, pl.ds(spans, clients), columns] = jnp.sum(grad, axis=1).astype(BF16)

    def pair_copy(i):
        return send(part.at[pl.ds(piece_row(dest(i // q), 1 - x, i % q), sub), :], pair_in.at[i],
                    pair_send, pair_recv.at[i], partner)

    queue = 3 + middle
    swaps = 1 if zs == 4 else 0

    def order(r):
        m = r - q
        late = swaps * middle * ((m + relays) // relays)
        return late * (q + m % 2 * q + m // 2) + (1 - late) * r

    def pairs_sent(r):
        late = swaps * middle * ((r - q + relays) // relays)
        return late * (2 * q + 2 + (r - q) // 2) + (1 - late) * (r + q + 2 * middle)

    def line_copy(r):
        i = order(r)
        place = dest(i // q)
        target, slot, sem = landing(place)
        return send(part.at[pl.ds(piece_row(place, x, i % q), sub), :], line_in.at[slot * q + i % q],
                    line_send.at[r % queue], line_recv.at[sem * q + i % q], target)

    step_rows = min(32, sub)

    def start_pairs(start, stop):
        def body(i, carry):
            @pl.when(i < zs * q)
            def _():
                pair_copy(i).start()
            return carry
        lax.fori_loop(start, stop, body, 0)

    def relay(r, extra):
        i = order(r)
        place = dest(i // q)
        row = piece_row(place, x, i % q)
        pair_copy(i).wait_recv()
        @pl.when(middle == 1)
        def _():
            wait_all(line_in.at[place * q + i % q], line_recv.at[place * q + i % q])
        slot = middle * (place * q + i % q) + (1 - middle) * z * q
        def add(r, carry):
            at = pl.ds(pl.multiple_of(r * step_rows, step_rows), step_rows)
            mine_at = pl.ds(pl.multiple_of(row + r * step_rows, step_rows), step_rows)
            total = part[mine_at, :].astype(F32) + pair_in[i, at, :].astype(F32)
            part[mine_at, :] = (total + line_in[slot, at, :].astype(F32)).astype(BF16)
            return carry
        lax.fori_loop(0, sub // step_rows, add, 0)
        @pl.when(r >= queue)
        def _():
            line_copy(r - queue).wait_send()
        line_copy(r).start()
        start_pairs(pairs_sent(r) + extra, pairs_sent(r + 1) + extra)

    def relay_range(start, stop, extra):
        def body(r, carry):
            relay(r, extra)
            return carry
        lax.fori_loop(start, stop, body, 0)

    def finish(s, square):
        i = relays + s
        row = piece_row(z, x, s)
        pair_copy(i).wait_recv()
        @pl.when(after_first == 1)
        def _():
            wait_all(line_in.at[zs * q + s], line_recv.at[zs * q + s])
        @pl.when(before_last == 1)
        def _():
            wait_all(line_in.at[(zs + 1) * q + s], line_recv.at[z * q + s])
        left = after_first * (zs * q + s) + (1 - after_first) * z * q
        right = before_last * ((zs + 1) * q + s) + (1 - before_last) * z * q
        def add(r, carry):
            at = pl.ds(pl.multiple_of(r * step_rows, step_rows), step_rows)
            mine_at = pl.ds(pl.multiple_of(row + r * step_rows, step_rows), step_rows)
            out_at = pl.ds(pl.multiple_of((s + 1) * sub + r * step_rows, step_rows), step_rows)
            total = part[mine_at, :].astype(F32) + pair_in[i, at, :].astype(F32)
            total = total + line_in[left, at, :].astype(F32) + line_in[right, at, :].astype(F32)
            head_v[out_at, :] = total
            return carry + jnp.sum((total * total).reshape(step_rows // 8, 8, emit), axis=0)
        square = lax.fori_loop(0, sub // step_rows, add, square)
        at = pl.ds(pl.multiple_of((s + 1) * sub, sub), sub)
        pltpu.make_async_copy(head_v.at[at, :], head_out.at[at, :], out_sem).start()
        return square

    def first_copy(j):
        place = dest(j // 2)
        side = unit_side(j)
        target, slot, sem = landing(place)
        return send(part.at[pl.ds(pl.multiple_of(block_row(place, side), sub), sub), :],
                    first_in.at[slot * 2 + side], first_send, first_recv.at[sem * 2 + side], target)

    def first_relay(j):
        @pl.when(middle == 1)
        def _():
            place = dest(j // 2)
            side = unit_side(j)
            row = pl.multiple_of(block_row(place, side), sub)
            wait_all(first_in.at[place * 2 + side], first_recv.at[place * 2 + side])
            def add(r, carry):
                at = pl.ds(pl.multiple_of(r * step_rows, step_rows), step_rows)
                mine_at = pl.ds(pl.multiple_of(row + r * step_rows, step_rows), step_rows)
                part[mine_at, :] = (
                    part[mine_at, :].astype(F32) + first_in[place * 2 + side, at, :].astype(F32)).astype(BF16)
                return carry
            lax.fori_loop(0, sub // step_rows, add, 0)
            first_copy(j).start()

    swap_copy = send(part.at[pl.ds(pl.multiple_of(block_row(z, 1 - x), sub), sub), :], swap_in,
                     swap_sem.at[0], swap_sem.at[1], partner)

    def first_wait(side):
        @pl.when(after_first == 1)
        def _():
            wait_all(first_in.at[zs * 2 + side], first_recv.at[zs * 2 + side])
        @pl.when(before_last == 1)
        def _():
            wait_all(first_in.at[(zs + 1) * 2 + side], first_recv.at[z * 2 + side])
        left = after_first * (zs * 2 + side) + (1 - after_first) * z * 2
        right = before_last * ((zs + 1) * 2 + side) + (1 - before_last) * z * 2
        return left, right

    def first_swap():
        row = block_row(z, 1 - x)
        left, right = first_wait(1 - x)
        def add(r, carry):
            at = pl.ds(pl.multiple_of(r * step_rows, step_rows), step_rows)
            mine_at = pl.ds(pl.multiple_of(row + r * step_rows, step_rows), step_rows)
            total = part[mine_at, :].astype(F32) + first_in[left, at, :].astype(F32)
            part[mine_at, :] = (total + first_in[right, at, :].astype(F32)).astype(BF16)
            return carry
        lax.fori_loop(0, sub // step_rows, add, 0)
        swap_copy.start()

    def first_finish(square):
        row = block_row(z, x)
        left, right = first_wait(x)
        swap_copy.wait_recv()
        def add(r, carry):
            at = pl.ds(pl.multiple_of(r * step_rows, step_rows), step_rows)
            mine_at = pl.ds(pl.multiple_of(row + r * step_rows, step_rows), step_rows)
            total = part[mine_at, :].astype(F32) + first_in[left, at, :].astype(F32)
            total = total + first_in[right, at, :].astype(F32) + swap_in[at, :].astype(F32)
            head_v[at, :] = total
            return carry + jnp.sum((total * total).reshape(step_rows // 8, 8, emit), axis=0)
        square = lax.fori_loop(0, sub // step_rows, add, square)
        pltpu.make_async_copy(head_v.at[pl.ds(0, sub), :], head_out.at[pl.ds(0, sub), :], out_sem).start()
        return square

    lax.fori_loop(1, firsts, load, 0)
    step = 64
    for c in range(rows // chunk):
        first_copies[c].wait()
        delta_copies[c].wait()
        def narrow(r, carry):
            at = pl.ds(pl.multiple_of(c * chunk + r * step, step), step)
            low[at, :] = delta_v[at, :].astype(BF16)
            return carry
        lax.fori_loop(0, chunk // step, narrow, 0)
        at = pl.ds(c * chunk, chunk)
        p = pre_v[0, at, pl.ds(0, piece)].astype(F32)
        hidden = (p * jax.nn.sigmoid(p)).astype(BF16)
        value = lax.dot_general(hidden, low[at, :], (((0,), (0,)), ((), ())), preferred_element_type=F32)
        if c > 0:
            value = value + head_v[pl.ds(0, piece), :]
        if c < len(delta_copies) - 1:
            head_v[pl.ds(0, piece), :] = value
        else:
            part[pl.ds(pl.multiple_of(unit_row(0), piece), piece), :] = value.astype(BF16)

    pl.semaphore_wait(barrier, devices - 1)

    ready = piece // sub - 1
    @pl.when(middle == 0)
    def _():
        first_copy(0).start()
    for i in range(min(ready, q)):
        pair_copy(i).start()
    lax.fori_loop(0 if hq > 1 else firsts, 2 * zs, load_rest, 0)
    weight_copy.start()
    ids_copy.start()
    line_in[z * q] = jnp.zeros((sub, emit), BF16)
    first_in[z * 2] = jnp.zeros((sub, emit), BF16)

    wait_all(pre_v.at[pl.ds(0, firsts - 1), :, pl.ds(0, piece)], pre_sem.at[0])
    def opening(u, carry):
        product(u, 0)
        @pl.when(middle == 0)
        def _():
            first_copy(u).start()
        return carry
    lax.fori_loop(1, firsts, opening, 0)
    wait_all(pre_v.at[pl.ds(0, (2 * zs * hq - firsts) // hq)], pre_sem.at[1])
    if hq > 1:
        def second(t, carry):
            product(t // (hq - 1), 1 + t % (hq - 1))
            return carry
        lax.fori_loop(0, 3 * (hq - 1), second, 0)
    start_pairs(min(ready, q), pairs_sent(0))
    first_relay(0)
    first_relay(1)
    weight_copy.wait()

    ids_copy.wait()
    for d in range(1, n):
        send(ids_all.at[me], ids_all.at[me], ids_send, ids_recv, lax.rem(me + d, n)).start()

    base = 3 + middle * (slopes - 8)
    stride = 3 - middle
    def main(t, carry):
        slope_sums(t)
        @pl.when((t >= 4) & (t % 2 == 0) & (t // 2 < firsts))
        def _():
            first_relay(t // 2)
        @pl.when((t >= base) & ((t - base) % stride == 0))
        def _():
            relay((t - base) // stride, 0)
        return carry
    lax.fori_loop(0, slopes, main, 0)

    for d in range(1, heads):
        target = lax.rem(my_head + d, heads)
        pltpu.make_async_remote_copy(
            src_ref=small.at[target], dst_ref=small_in.at[lax.rem(my_head - target + heads, heads) - 1],
            send_sem=head_send, recv_sem=head_recv, device_id={"head": target}, device_id_type=MESH).start()

    done = slopes // 2
    if done < firsts:
        def rest_first(j, carry):
            first_relay(j)
            return carry
        lax.fori_loop(done, firsts, rest_first, 0)

    def add_rows(r, total):
        value = delta_v[pl.ds(pl.multiple_of(r * step, step), step), :]
        return total + jnp.sum(value.reshape(step // 8, 8, emit), axis=0)
    bias = lax.fori_loop(0, rows // step, add_rows, jnp.zeros((8, emit), F32))
    bias = jnp.sum(bias, axis=0, keepdims=True)
    pad = mine.shape[1] - spans
    tail = jnp.where(
        lax.broadcasted_iota(jnp.int32, (pad, emit), 0) == 0, jnp.broadcast_to(bias, (pad, emit)), 0.0
    ).astype(BF16)
    for h in range(2):
        mine[h, pl.ds(spans, pad), :] = tail[:, h * half:(h + 1) * half]

    ends = [(slopes - 4) // 3 + 1] + [(slopes - 4) // 3 + 1 + k for k in (2, 4, 4, 8, 13, 16)]
    inner = [3] + [3 + k for k in (1, 2, 3, 8, 15, 18)]
    stops = [(1 - middle) * e + middle * i for e, i in zip(ends, inner)] + [relays]

    if hq > 1:
        def third(t, carry):
            product(3 + t // (hq - 1), 1 + t % (hq - 1))
            return carry
        lax.fori_loop(0, (2 * zs - 5) * (hq - 1), third, 0)
    relay_range(stops[0], stops[1], 0)
    def fourth(t, carry):
        product(2 * zs - 2 + t // hq, t % hq)
        return carry
    lax.fori_loop(0, 2 * hq, fourth, 0)
    relay_range(stops[1], stops[2], 0)
    relay_range(stops[2], stops[3], 0)

    wait_all(small_in, head_recv)
    total = small[my_head].astype(F32)
    for d in range(heads - 1):
        total = total + small_in[d].astype(F32)
    for h in range(2):
        mine[h, pl.ds(0, spans), :] = total[:spans, h * half:(h + 1) * half].astype(BF16)
    embed_all[z, x] = total[spans:].astype(BF16)

    embed_pair = send(embed_all.at[z, x], embed_all.at[z, x], embed_pair_sem.at[0], embed_pair_sem.at[1], partner)
    embed_pair.start()

    roots = [zs // 2 - 1, zs // 2]
    def span_copy(h, right):
        return send(mine.at[h], span_in.at[h, 1 - right], span_send.at[h], span_recv.at[2 * h + 1 - right],
                    (z + 2 * right - 1) * 2 + x)
    def span_arrival(h, side):
        wait_all(span_in.at[h, side], span_recv.at[2 * h + side])
    for h in range(2):
        @pl.when(z == 0)
        def _():
            if roots[h] != 0:
                span_copy(h, 1).start()
        @pl.when(z == zs - 1)
        def _():
            if roots[h] != zs - 1:
                span_copy(h, 0).start()

    start_pairs(pairs_sent(stops[3]), pairs_sent(stops[3]) + middle)
    relay_range(stops[3], stops[4], middle)

    def embed_copy(j, right):
        source = z + j - 2 * right * j
        return send(embed_all.at[source], embed_all.at[source], embed_send.at[right], embed_recv.at[source],
                    (z + 2 * right - 1) * 2 + x)

    def embed_step(j):
        for right, near_end, there in ((1, before_last, z - j >= 0), (0, after_first, z + j <= zs - 1)):
            @pl.when((near_end == 1) & there)
            def _():
                if j > 0:
                    source = z + j - 2 * right * j
                    wait_all(embed_all.at[source], embed_recv.at[source])
                    embed_copy(j - 1, right).wait_send()
                embed_copy(j, right).start()

    embed_pair.wait_recv()
    for h in range(2):
        for right, between in ((1, (z > 0) & (z < roots[h])), (0, (z < zs - 1) & (z > roots[h]))):
            @pl.when(between)
            def _():
                span_arrival(h, 1 - right)
                mine[h] = (mine[h].astype(F32) + span_in[h, 1 - right].astype(F32)).astype(BF16)
                span_copy(h, right).start()
    embed_step(0)

    relay_range(stops[4], stops[5], middle)

    span_pair_copy = send(span_part, span_pair, span_pair_sem.at[0], span_pair_sem.at[1], partner)
    for h in range(2):
        @pl.when(z == roots[h])
        def _():
            total = mine[h].astype(F32)
            for side, there in ((0, roots[h] > 0), (1, roots[h] < zs - 1)):
                if there:
                    span_arrival(h, side)
                    total = total + span_in[h, side].astype(F32)
            span_part[...] = total.astype(BF16)
            span_pair_copy.start()
    first_swap()
    embed_step(1)

    start_pairs(pairs_sent(stops[5]) + middle, pairs_sent(stops[5]) + 3 * middle)
    relay_range(stops[5], stops[6], 3 * middle)

    def all_copy(h, d):
        return send(span_all.at[h], span_all.at[h], all_send, all_recv.at[h], lax.rem(z + d, zs) * 2 + x)
    for h in range(2):
        @pl.when(z == roots[h])
        def _():
            span_pair_copy.wait_recv()
            span_all[h] = (span_part[...].astype(F32) + span_pair[...].astype(F32)).astype(BF16)
            for d in range(1, zs):
                all_copy(h, d).start()
    for j in range(2, zs - 1):
        embed_step(j)

    relay_range(stops[6], stops[7], 3 * middle)
    start_pairs(pairs_sent(relays) + 3 * middle, zs * q)
    square = jnp.zeros((8, emit), F32)
    square = first_finish(square)
    square = lax.fori_loop(0, 5, finish, square)

    for j in range(1, zs):
        for right, near_end, there in ((1, before_last, z - j >= 0), (0, after_first, z + j <= zs - 1)):
            source = z + j - 2 * right * j
            @pl.when(there if j == zs - 1 else (near_end == 0) & there)
            def _():
                wait_all(embed_all.at[source], embed_recv.at[source])
    for right, near_end, last in ((1, before_last, z), (0, after_first, zs - 1 - z)):
        for j in range(zs - 1):
            @pl.when((near_end == 1) & (last == j))
            def _():
                embed_copy(j, right).wait_send()
    wait_all(ids_all.at[pl.ds(0, n - 1)], ids_recv)
    wanted = lax.broadcasted_iota(jnp.int32, (clients, clients), 0) + me * clients
    embed_raw = jnp.zeros((clients, emit), F32)
    for c in range(n):
        chosen = (jnp.broadcast_to(ids_all[c], (clients, clients)) == wanted).astype(F32).astype(BF16)
        embed_raw = embed_raw + jnp.dot(chosen, embed_all[c // 2, c % 2], preferred_element_type=F32)
    embed_v[...] = embed_raw
    embed_write = pltpu.make_async_copy(embed_v, embed_out, write_sem.at[0])
    embed_write.start()
    embed_square = jnp.sum(embed_raw * embed_raw)

    rest_square = jnp.zeros((), F32)
    for h in range(2):
        @pl.when(z != roots[h])
        def _():
            wait_all(span_all.at[h], all_recv.at[h])
        value = span_all[h].astype(F32)
        rest_v[:, pl.ds(h * half, half)] = value
        rest_square = rest_square + jnp.sum(value * value)
    rest_write = pltpu.make_async_copy(rest_v, rest_out, write_sem.at[1])
    rest_write.start()

    square = lax.fori_loop(5, q, finish, square)
    head_total = jnp.sum(square)

    lane = lax.broadcasted_iota(jnp.int32, (1, 128), 1)
    stat_all[flat] = jnp.where(lane == 0, head_total, jnp.where(lane == 1, embed_square, rest_square / n))
    def tell(client, head):
        pltpu.make_async_remote_copy(
            src_ref=stat_all.at[flat], dst_ref=stat_all.at[flat], send_sem=stat_send, recv_sem=stat_recv,
            device_id={"client": client, "head": head}, device_id_type=MESH).start()
    each_other(tell)

    wait_all(part.at[pl.ds(0, zs * q * sub)], pair_send)
    def line_sent(r, carry):
        line_copy(r).wait_send()
        return carry
    lax.fori_loop(relays - queue, relays, line_sent, 0)
    wait_all(part.at[pl.ds(0, firsts * sub)], first_send)
    swap_copy.wait_send()
    embed_pair.wait_send()
    wait_all(small.at[pl.ds(0, heads - 1)], head_send)
    wait_all(ids_all.at[pl.ds(0, n - 1)], ids_send)
    for h in range(2):
        @pl.when(z < roots[h])
        def _():
            span_copy(h, 1).wait_send()
        @pl.when(z > roots[h])
        def _():
            span_copy(h, 0).wait_send()
        @pl.when(z == roots[h])
        def _():
            span_pair_copy.wait_send()
            wait_all(part.at[pl.ds(0, (zs - 1) * mine.shape[1] // 2)], all_send)
    embed_write.wait()
    rest_write.wait()
    pltpu.make_async_copy(head_v, head_out, out_sem).wait()

    wait_all(stat_all.at[pl.ds(0, devices - 1)], stat_recv)
    stat_out[...] = jnp.sum(stat_all[...], axis=0)
    wait_all(stat_all.at[pl.ds(0, devices - 1)], stat_send)


def scale_kernel(sizes, stat_ref, head_ref, rest_ref, embed_ref, head_out, bias_out, embed_out, span_out,
                 stat, head, rest, embed, in_sem, out_sem):
    head_size, embed_size, rest_size = sizes
    spans = span_out.shape[0]
    steps = in_sem.shape[0] - 3
    rows = head.shape[0] // steps
    stat_in = pltpu.make_async_copy(stat_ref, stat, in_sem.at[steps])
    rest_in = pltpu.make_async_copy(rest_ref, rest, in_sem.at[steps + 1])
    embed_in = pltpu.make_async_copy(embed_ref, embed, in_sem.at[steps + 2])
    def part(ref, i):
        return ref.at[pl.ds(i * rows, rows), :]
    stat_in.start()
    heads_in = [pltpu.make_async_copy(part(head_ref, i), part(head, i), in_sem.at[i]) for i in range(steps)]
    heads_out = [pltpu.make_async_copy(part(head, i), part(head_out, i), out_sem.at[i]) for i in range(steps)]
    for copy in heads_in:
        copy.start()
    rest_in.start()
    embed_in.start()
    stat_in.wait()
    factor = clip_factor(stat[0:1, 0:1], head_size)
    embed_factor = clip_factor(stat[0:1, 1:2], embed_size)
    rest_factor = clip_factor(stat[0:1, 2:3], rest_size)
    for i in range(steps):
        heads_in[i].wait()
        head[pl.ds(i * rows, rows), :] = factor * head[pl.ds(i * rows, rows), :]
        heads_out[i].start()
    rest_in.wait()
    rest[...] = rest_factor * rest[...]
    bias_copy = pltpu.make_async_copy(rest.at[pl.ds(spans, 1), :], bias_out, out_sem.at[steps])
    span_copy = pltpu.make_async_copy(rest.at[pl.ds(0, spans), :], span_out, out_sem.at[steps + 1])
    bias_copy.start()
    span_copy.start()
    embed_in.wait()
    embed[...] = embed_factor * embed[...]
    embed_copy = pltpu.make_async_copy(embed, embed_out, out_sem.at[steps + 2])
    embed_copy.start()
    for copy in heads_out + [bias_copy, span_copy, embed_copy]:
        copy.wait()


def per_device(n, heads, pre, delta, head_weight, client_ids):
    rows, hidden_width = pre.shape
    emit = delta.shape[1]
    clients = client_ids.shape[0]
    spans = rows // clients
    block = hidden_width // n
    piece = min(256, block)
    hq = block // piece
    zs = n // 2
    q = 7
    sub = block // (q + 1)
    padded = (spans + 16) // 16 * 16
    half = emit // 2
    cfg = (n, heads, block, piece, spans, clients)
    ids = client_ids.reshape(1, clients)
    hbm = pl.BlockSpec(memory_space=pl.ANY)
    vmem = pl.BlockSpec(memory_space=pltpu.VMEM)
    dma = pltpu.SemaphoreType.DMA
    chunk = math.gcd(rows, 256)
    head_raw, rest_raw, embed_raw, stats = pl.pallas_call(
        functools.partial(kernel, cfg),
        out_shape=(
            jax.ShapeDtypeStruct((block, emit), F32),
            jax.ShapeDtypeStruct((padded, emit), F32),
            jax.ShapeDtypeStruct((clients, emit), F32),
            jax.ShapeDtypeStruct((1, 128), F32),
        ),
        in_specs=[hbm, hbm, hbm, hbm],
        out_specs=(hbm, hbm, hbm, vmem),
        scratch_shapes=[
            pltpu.VMEM((n, rows, block), BF16),
            pltpu.VMEM((rows, emit), F32),
            pltpu.VMEM((rows, emit), BF16),
            pltpu.VMEM((hidden_width, emit), BF16),
            pltpu.VMEM((hidden_width, emit), BF16),
            pltpu.VMEM((zs * q, sub, emit), BF16),
            pltpu.VMEM(((zs + 2) * q, sub, emit), BF16),
            pltpu.VMEM(((zs + 2) * 2, sub, emit), BF16),
            pltpu.VMEM((sub, emit), BF16),
            pltpu.VMEM((block, emit), F32),
            pltpu.VMEM((heads, spans + clients, emit), BF16),
            pltpu.VMEM((heads - 1, spans + clients, emit), BF16),
            pltpu.VMEM((2, padded, half), BF16),
            pltpu.VMEM((2, 2, padded, half), BF16),
            pltpu.VMEM((padded, half), BF16),
            pltpu.VMEM((padded, half), BF16),
            pltpu.VMEM((2, padded, half), BF16),
            pltpu.VMEM((zs, 2, clients, emit), BF16),
            pltpu.VMEM((n, 1, clients), jnp.int32),
            pltpu.VMEM((clients, emit), F32),
            pltpu.VMEM((padded, emit), F32),
            pltpu.VMEM((n * heads, 1, 128), F32),
            dma((2,)), dma((rows // chunk,)), dma((rows // chunk,)), dma, dma,
            dma, dma((zs * q,)), dma((4,)), dma(((zs + 1) * q,)),
            dma, dma(((zs + 1) * 2,)), dma((2,)), dma, dma,
            dma((2,)), dma((4,)), dma((2,)), dma, dma((2,)), dma((2,)), dma((2,)), dma((2,)), dma((zs,)),
            dma, dma, dma, dma, dma,
        ],
        compiler_params=pltpu.CompilerParams(
            collective_id=0, has_side_effects=True, vmem_limit_bytes=62 * 2**20
        ),
        name="clipped_grads",
    )(pre, delta, head_weight, ids)
    sizes = (hidden_width * emit * heads, clients * n * hidden_width, spans * hidden_width + emit * heads)
    steps = 4
    head_grad, bias_grad, embed_grad, span_grad = pl.pallas_call(
        functools.partial(scale_kernel, sizes),
        out_shape=(
            jax.ShapeDtypeStruct((block, emit), F32),
            jax.ShapeDtypeStruct((1, emit), F32),
            jax.ShapeDtypeStruct((clients, emit), F32),
            jax.ShapeDtypeStruct((spans, emit), F32),
        ),
        in_specs=[hbm] * 4,
        out_specs=(hbm,) * 4,
        scratch_shapes=[
            pltpu.VMEM((1, 128), F32),
            pltpu.VMEM((block, emit), F32),
            pltpu.VMEM((padded, emit), F32),
            pltpu.VMEM((clients, emit), F32),
            dma((steps + 3,)), dma((steps + 3,)),
        ],
        name="scaled",
    )(stats, head_raw, rest_raw, embed_raw)
    return head_grad, bias_grad.reshape(emit), embed_grad, span_grad


def solution(mesh):
    placed = (P("client", None), P("client", "head"), P(None, "head"), P("client"))
    return jax.shard_map(
        functools.partial(per_device, mesh.shape["client"], mesh.shape["head"]),
        mesh=mesh,
        in_specs=placed,
        out_specs=(P("client", "head"), P("head"), P("client", "head"), P(None, "head")),
        check_vma=False,
    )
```

```python
import functools
import math

import jax
import jax.numpy as jnp
from jax import lax
from jax.experimental import pallas as pl
from jax.experimental.pallas import tpu as pltpu
from jax.sharding import PartitionSpec as P

EPSILON = 1e-06
MESH = pl.DeviceIdType.MESH
F32 = jnp.float32
BF16 = jnp.bfloat16


def clip_factor(total, number):
    return jnp.minimum(1.0, 1.0 / jnp.sqrt(total / number + EPSILON))


def kernel(cfg, pre_ref, delta_ref, weight_ref, ids_ref, head_out, rest_out, embed_out, stat_out,
           pre_v, delta_v, low, weight_v, part, pair_in, line_in, first_in, swap_in, cross_in, head_v,
           small, small_in, mine, span_in, span_part, span_pair, span_all, embed_all, ids_all,
           embed_v, rest_v, stat_all,
           pre_sem, first_pre_sem, delta_sem, weight_sem, out_sem, pair_send, pair_recv, line_send, line_recv,
           first_send, first_recv, swap_sem, cross_sem, head_send, head_recv, span_send, span_recv, span_pair_sem,
           all_send, all_recv, write_sem, embed_pair_sem, embed_send, embed_recv, ids_sem, ids_send, ids_recv,
           stat_send, stat_recv):
    n, heads, block, piece, spans, clients = cfg
    zs = n // 2
    q = 7
    sub = block // (q + 1)
    hq = block // piece
    rows, emit = low.shape
    half = emit // 2
    me = lax.axis_index("client")
    my_head = lax.axis_index("head")
    z = me // 2
    x = me % 2
    relays = (zs - 1) * q
    firsts = 2 * (zs - 1)
    slopes = 2 * zs * hq
    devices = n * heads
    flat = me * heads + my_head

    after_first = (z + zs - 1) // zs
    before_last = (2 * zs - 2 - z) // zs
    middle = after_first * before_last
    upper = 2 * z // zs
    near = z + upper * (zs - 1 - 2 * z)
    partner = z * 2 + 1 - x

    def wait_all(ref, sem):
        pltpu.make_async_copy(ref, ref, sem).wait()

    def send(src, dst, send_sem, recv_sem, client):
        return pltpu.make_async_remote_copy(
            src_ref=src, dst_ref=dst, send_sem=send_sem, recv_sem=recv_sem,
            device_id={"client": client}, device_id_type=MESH)

    def dest(k):
        both = (2 * near - k - 1 + zs) // zs
        odd = k % 2
        out = both * (odd * (k // 2) + (1 - odd) * (zs - 1 - k // 2)) + (1 - both) * (zs - 1 - k + near)
        return out + upper * (zs - 1 - 2 * out)

    def block_row(place, side):
        return (place * 2 + side) * block

    def piece_row(place, side, s):
        return pl.multiple_of(block_row(place, side) + (s + 1) * sub, sub)

    def landing(place):
        right = (place - z + zs) // zs
        target = z + 2 * right - 1
        gap = right * (place - target) + (1 - right) * (target - place)
        away = (gap + zs - 1) // zs
        slot = away * place + (1 - away) * (zs + 1 - right)
        sem = away * place + (1 - away) * (right * zs + (1 - right) * place)
        return target * 2 + x, slot, sem

    def unit_side(u):
        return (x + 1 - u % 2) % 2

    def unit_row(u):
        return pl.multiple_of(block_row(dest(u // 2), unit_side(u)), block)

    def pre_copy(u, h, sem):
        columns = pl.ds(pl.multiple_of(unit_row(u) + h * piece, piece), piece)
        return pltpu.make_async_copy(
            pre_ref.at[:, columns], pre_v.at[u, :, pl.ds(pl.multiple_of(h * piece, piece), piece)], pre_sem.at[sem])

    chunk = math.gcd(rows, 256)
    delta_copies = [
        pltpu.make_async_copy(delta_ref.at[pl.ds(c * chunk, chunk), :], delta_v.at[pl.ds(c * chunk, chunk), :],
                              delta_sem.at[c])
        for c in range(rows // chunk)]
    weight_copy = pltpu.make_async_copy(weight_ref, weight_v, weight_sem)
    ids_copy = pltpu.make_async_copy(ids_ref, ids_all.at[me], ids_sem)
    first_column = pl.multiple_of(unit_row(0), piece)
    first_copies = [
        pltpu.make_async_copy(pre_ref.at[pl.ds(c * chunk, chunk), pl.ds(first_column, piece)],
                              pre_v.at[0, pl.ds(c * chunk, chunk), pl.ds(0, piece)], first_pre_sem.at[c])
        for c in range(rows // chunk)]
    for c in range(rows // chunk):
        first_copies[c].start()
        delta_copies[c].start()

    def each_other(action):
        columns = [lax.rem(my_head + d, heads) for d in range(heads)]
        for column in columns[1:]:
            action(me, column)
        def body(d, carry):
            client = lax.rem(me + d, n)
            for column in columns:
                action(client, column)
            return carry
        lax.fori_loop(1, n, body, 0)

    barrier = pltpu.get_barrier_semaphore()
    def greet(client, head):
        pl.semaphore_signal(barrier, inc=1, device_id={"client": client, "head": head}, device_id_type=MESH)
    each_other(greet)

    def load(u, carry):
        pre_copy(u, 0, 0).start()
        return carry
    def load_rest(u, carry):
        @pl.when(u >= firsts)
        def _():
            pre_copy(u, 0, 1).start()
        for h in range(1, hq):
            pre_copy(u, h, 1).start()
        return carry

    def product(u, h):
        p = pre_v[u, :, pl.ds(pl.multiple_of(h * piece, piece), piece)].astype(F32)
        hidden = (p * jax.nn.sigmoid(p)).astype(BF16)
        value = lax.dot_general(hidden, low[...], (((0,), (0,)), ((), ())), preferred_element_type=F32)
        part[pl.ds(pl.multiple_of(unit_row(u) + h * piece, piece), piece), :] = value.astype(BF16)

    def slope_sums(t):
        u = t // hq
        h = t % hq
        p = pre_v[u, :, pl.ds(pl.multiple_of(h * piece, piece), piece)].astype(F32)
        row = pl.multiple_of(unit_row(u) + h * piece, piece)
        value = lax.dot_general(
            low[...], weight_v[pl.ds(row, piece), :], (((1,), (1,)), ((), ())), preferred_element_type=F32)
        s = jax.nn.sigmoid(p)
        grad = value.astype(BF16).astype(F32) * (s * (1.0 + p * (1.0 - s)))
        grad = grad.reshape(clients, spans, piece)
        to = row // emit
        columns = pl.ds(pl.multiple_of(row % emit, piece), piece)
        small[to, pl.ds(0, spans), columns] = jnp.sum(grad, axis=0).astype(BF16)
        small[to, pl.ds(spans, clients), columns] = jnp.sum(grad, axis=1).astype(BF16)

    def pair_copy(i):
        return send(part.at[pl.ds(piece_row(dest(i // q), 1 - x, i % q), sub), :], pair_in.at[i],
                    pair_send, pair_recv.at[i], partner)

    queue = 3 + middle
    cross = zs == 4
    swaps = 1 if cross else 0
    skip = q - 1

    def order(r):
        m = r - q
        late = swaps * middle * ((m + relays) // relays)
        return late * (q + m % 2 * q + m // 2) + (1 - late) * r

    def pairs_sent(r):
        late = swaps * middle * ((r - q + relays) // relays)
        return late * (2 * q + 3 + (r - q) // 2) + (1 - late) * (r + q + (2 + swaps) * middle)

    def line_copy(r):
        i = order(r)
        place = dest(i // q)
        target, slot, sem = landing(place)
        return send(part.at[pl.ds(piece_row(place, x, i % q), sub), :], line_in.at[slot * q + i % q],
                    line_send.at[r % queue], line_recv.at[sem * q + i % q], target)

    step_rows = min(32, sub)

    def start_pairs(start, stop):
        def body(i, carry):
            @pl.when((i < zs * q) & (swaps * middle * (skip + 1) != i + 1))
            def _():
                pair_copy(i).start()
            return carry
        lax.fori_loop(start, stop, body, 0)

    cross_copy = send(part.at[pl.ds(piece_row(dest(0), 1 - x, skip), sub), :], cross_in,
                      cross_sem.at[0], cross_sem.at[1], landing(dest(0))[0])

    def cross_add():
        row = piece_row(dest(1), 1 - x, skip)
        cross_copy.wait_recv()
        def add(r, carry):
            at = pl.ds(pl.multiple_of(r * step_rows, step_rows), step_rows)
            mine_at = pl.ds(pl.multiple_of(row + r * step_rows, step_rows), step_rows)
            part[mine_at, :] = (part[mine_at, :].astype(F32) + cross_in[at, :].astype(F32)).astype(BF16)
            return carry
        lax.fori_loop(0, sub // step_rows, add, 0)

    def relay(r, extra):
        i = order(r)
        place = dest(i // q)
        row = piece_row(place, x, i % q)
        @pl.when(swaps * middle * (skip + 1) != i + 1)
        def _():
            pair_copy(i).wait_recv()
        @pl.when(middle == 1)
        def _():
            wait_all(line_in.at[place * q + i % q], line_recv.at[place * q + i % q])
        slot = middle * (place * q + i % q) + (1 - middle) * z * q
        def add(r, carry):
            at = pl.ds(pl.multiple_of(r * step_rows, step_rows), step_rows)
            mine_at = pl.ds(pl.multiple_of(row + r * step_rows, step_rows), step_rows)
            total = part[mine_at, :].astype(F32) + pair_in[i, at, :].astype(F32)
            part[mine_at, :] = (total + line_in[slot, at, :].astype(F32)).astype(BF16)
            return carry
        lax.fori_loop(0, sub // step_rows, add, 0)
        @pl.when(r >= queue)
        def _():
            line_copy(r - queue).wait_send()
        line_copy(r).start()
        start_pairs(pairs_sent(r) + extra, pairs_sent(r + 1) + extra)

    def relay_range(start, stop, extra):
        def body(r, carry):
            relay(r, extra)
            return carry
        lax.fori_loop(start, stop, body, 0)

    def finish(s, square):
        i = relays + s
        row = piece_row(z, x, s)
        pair_copy(i).wait_recv()
        @pl.when(after_first == 1)
        def _():
            wait_all(line_in.at[zs * q + s], line_recv.at[zs * q + s])
        @pl.when(before_last == 1)
        def _():
            wait_all(line_in.at[(zs + 1) * q + s], line_recv.at[z * q + s])
        left = after_first * (zs * q + s) + (1 - after_first) * z * q
        right = before_last * ((zs + 1) * q + s) + (1 - before_last) * z * q
        def add(r, carry):
            at = pl.ds(pl.multiple_of(r * step_rows, step_rows), step_rows)
            mine_at = pl.ds(pl.multiple_of(row + r * step_rows, step_rows), step_rows)
            out_at = pl.ds(pl.multiple_of((s + 1) * sub + r * step_rows, step_rows), step_rows)
            total = part[mine_at, :].astype(F32) + pair_in[i, at, :].astype(F32)
            total = total + line_in[left, at, :].astype(F32) + line_in[right, at, :].astype(F32)
            head_v[out_at, :] = total
            return carry + jnp.sum((total * total).reshape(step_rows // 8, 8, emit), axis=0)
        square = lax.fori_loop(0, sub // step_rows, add, square)
        at = pl.ds(pl.multiple_of((s + 1) * sub, sub), sub)
        pltpu.make_async_copy(head_v.at[at, :], head_out.at[at, :], out_sem).start()
        return square

    def first_copy(j):
        place = dest(j // 2)
        side = unit_side(j)
        target, slot, sem = landing(place)
        return send(part.at[pl.ds(pl.multiple_of(block_row(place, side), sub), sub), :],
                    first_in.at[slot * 2 + side], first_send, first_recv.at[sem * 2 + side], target)

    def first_relay(j):
        @pl.when(middle == 1)
        def _():
            place = dest(j // 2)
            side = unit_side(j)
            row = pl.multiple_of(block_row(place, side), sub)
            wait_all(first_in.at[place * 2 + side], first_recv.at[place * 2 + side])
            def add(r, carry):
                at = pl.ds(pl.multiple_of(r * step_rows, step_rows), step_rows)
                mine_at = pl.ds(pl.multiple_of(row + r * step_rows, step_rows), step_rows)
                part[mine_at, :] = (
                    part[mine_at, :].astype(F32) + first_in[place * 2 + side, at, :].astype(F32)).astype(BF16)
                return carry
            lax.fori_loop(0, sub // step_rows, add, 0)
            first_copy(j).start()

    swap_copy = send(part.at[pl.ds(pl.multiple_of(block_row(z, 1 - x), sub), sub), :], swap_in,
                     swap_sem.at[0], swap_sem.at[1], partner)

    def first_wait(side):
        @pl.when(after_first == 1)
        def _():
            wait_all(first_in.at[zs * 2 + side], first_recv.at[zs * 2 + side])
        @pl.when(before_last == 1)
        def _():
            wait_all(first_in.at[(zs + 1) * 2 + side], first_recv.at[z * 2 + side])
        left = after_first * (zs * 2 + side) + (1 - after_first) * z * 2
        right = before_last * ((zs + 1) * 2 + side) + (1 - before_last) * z * 2
        return left, right

    def first_swap():
        row = block_row(z, 1 - x)
        left, right = first_wait(1 - x)
        def add(r, carry):
            at = pl.ds(pl.multiple_of(r * step_rows, step_rows), step_rows)
            mine_at = pl.ds(pl.multiple_of(row + r * step_rows, step_rows), step_rows)
            total = part[mine_at, :].astype(F32) + first_in[left, at, :].astype(F32)
            part[mine_at, :] = (total + first_in[right, at, :].astype(F32)).astype(BF16)
            return carry
        lax.fori_loop(0, sub // step_rows, add, 0)
        swap_copy.start()

    def first_finish(square):
        row = block_row(z, x)
        left, right = first_wait(x)
        swap_copy.wait_recv()
        def add(r, carry):
            at = pl.ds(pl.multiple_of(r * step_rows, step_rows), step_rows)
            mine_at = pl.ds(pl.multiple_of(row + r * step_rows, step_rows), step_rows)
            total = part[mine_at, :].astype(F32) + first_in[left, at, :].astype(F32)
            total = total + first_in[right, at, :].astype(F32) + swap_in[at, :].astype(F32)
            head_v[at, :] = total
            return carry + jnp.sum((total * total).reshape(step_rows // 8, 8, emit), axis=0)
        square = lax.fori_loop(0, sub // step_rows, add, square)
        pltpu.make_async_copy(head_v.at[pl.ds(0, sub), :], head_out.at[pl.ds(0, sub), :], out_sem).start()
        return square

    opened = min(128, piece)
    lax.fori_loop(1, firsts, load, 0)
    step = 64
    for c in range(rows // chunk):
        first_copies[c].wait()
        delta_copies[c].wait()
        def narrow(r, carry):
            at = pl.ds(pl.multiple_of(c * chunk + r * step, step), step)
            low[at, :] = delta_v[at, :].astype(BF16)
            return carry
        lax.fori_loop(0, chunk // step, narrow, 0)
        at = pl.ds(c * chunk, chunk)
        p = pre_v[0, at, pl.ds(0, opened)].astype(F32)
        hidden = (p * jax.nn.sigmoid(p)).astype(BF16)
        value = lax.dot_general(hidden, low[at, :], (((0,), (0,)), ((), ())), preferred_element_type=F32)
        if c > 0:
            value = value + head_v[pl.ds(0, opened), :]
        if c < len(delta_copies) - 1:
            head_v[pl.ds(0, opened), :] = value
        else:
            part[pl.ds(pl.multiple_of(unit_row(0), opened), opened), :] = value.astype(BF16)

    pl.semaphore_wait(barrier, devices - 1)

    ready = min(piece // sub - 1, q)
    soon = min(opened // sub - 1, q)
    @pl.when(middle == 0)
    def _():
        first_copy(0).start()
    for i in range(soon):
        pair_copy(i).start()
    if opened < piece:
        rest = piece - opened
        p = pre_v[0, :, pl.ds(opened, rest)].astype(F32)
        hidden = (p * jax.nn.sigmoid(p)).astype(BF16)
        value = lax.dot_general(hidden, low[...], (((0,), (0,)), ((), ())), preferred_element_type=F32)
        part[pl.ds(pl.multiple_of(unit_row(0) + opened, opened), rest), :] = value.astype(BF16)
    for i in range(soon, ready):
        pair_copy(i).start()
    lax.fori_loop(0 if hq > 1 else firsts, 2 * zs, load_rest, 0)
    weight_copy.start()
    ids_copy.start()
    line_in[z * q] = jnp.zeros((sub, emit), BF16)
    first_in[z * 2] = jnp.zeros((sub, emit), BF16)

    wait_all(pre_v.at[pl.ds(0, firsts - 1), :, pl.ds(0, piece)], pre_sem.at[0])
    def opening(u, carry):
        product(u, 0)
        @pl.when(middle == 0)
        def _():
            first_copy(u).start()
        return carry
    lax.fori_loop(1, firsts, opening, 0)
    wait_all(pre_v.at[pl.ds(0, (2 * zs * hq - firsts) // hq)], pre_sem.at[1])
    if hq > 1:
        def second(t, carry):
            product(t // (hq - 1), 1 + t % (hq - 1))
            return carry
        lax.fori_loop(0, 3 * (hq - 1), second, 0)
    if cross:
        @pl.when(middle == 1)
        def _():
            pair_in[skip] = jnp.zeros((sub, emit), BF16)
            cross_copy.start()
    start_pairs(ready, pairs_sent(0))
    first_relay(0)
    first_relay(1)
    weight_copy.wait()

    ids_copy.wait()
    for d in range(1, n):
        send(ids_all.at[me], ids_all.at[me], ids_send, ids_recv, lax.rem(me + d, n)).start()

    base = 3 + middle * (slopes - 8)
    stride = 3 - middle
    def main(t, carry):
        slope_sums(t)
        @pl.when((t >= 4) & (t % 2 == 0) & (t // 2 < firsts))
        def _():
            first_relay(t // 2)
        @pl.when((t >= base) & ((t - base) % stride == 0))
        def _():
            relay((t - base) // stride, 0)
        return carry
    lax.fori_loop(0, slopes, main, 0)

    for d in range(1, heads):
        target = lax.rem(my_head + d, heads)
        pltpu.make_async_remote_copy(
            src_ref=small.at[target], dst_ref=small_in.at[lax.rem(my_head - target + heads, heads) - 1],
            send_sem=head_send, recv_sem=head_recv, device_id={"head": target}, device_id_type=MESH).start()

    if cross:
        @pl.when(middle == 1)
        def _():
            cross_add()

    done = slopes // 2
    if done < firsts:
        def rest_first(j, carry):
            first_relay(j)
            return carry
        lax.fori_loop(done, firsts, rest_first, 0)

    def add_rows(r, total):
        value = delta_v[pl.ds(pl.multiple_of(r * step, step), step), :]
        return total + jnp.sum(value.reshape(step // 8, 8, emit), axis=0)
    bias = lax.fori_loop(0, rows // step, add_rows, jnp.zeros((8, emit), F32))
    bias = jnp.sum(bias, axis=0, keepdims=True)
    pad = mine.shape[1] - spans
    tail = jnp.where(
        lax.broadcasted_iota(jnp.int32, (pad, emit), 0) == 0, jnp.broadcast_to(bias, (pad, emit)), 0.0
    ).astype(BF16)
    for h in range(2):
        mine[h, pl.ds(spans, pad), :] = tail[:, h * half:(h + 1) * half]

    ends = [(slopes - 4) // 3 + 1] + [(slopes - 4) // 3 + 1 + k for k in (2, 4, 4, 8, 13, 16)]
    inner = [3] + [3 + k for k in (1, 2, 3, 8, 15, 18)]
    stops = [(1 - middle) * e + middle * i for e, i in zip(ends, inner)] + [relays]

    if hq > 1:
        def third(t, carry):
            product(3 + t // (hq - 1), 1 + t % (hq - 1))
            return carry
        lax.fori_loop(0, (2 * zs - 5) * (hq - 1), third, 0)
    relay_range(stops[0], stops[1], 0)
    def fourth(t, carry):
        product(2 * zs - 2 + t // hq, t % hq)
        return carry
    lax.fori_loop(0, 2 * hq, fourth, 0)
    relay_range(stops[1], stops[2], 0)
    relay_range(stops[2], stops[3], 0)

    wait_all(small_in, head_recv)
    total = small[my_head].astype(F32)
    for d in range(heads - 1):
        total = total + small_in[d].astype(F32)
    for h in range(2):
        mine[h, pl.ds(0, spans), :] = total[:spans, h * half:(h + 1) * half].astype(BF16)
    embed_all[z, x] = total[spans:].astype(BF16)

    embed_pair = send(embed_all.at[z, x], embed_all.at[z, x], embed_pair_sem.at[0], embed_pair_sem.at[1], partner)
    embed_pair.start()

    roots = [zs // 2 - 1, zs // 2]
    def span_copy(h, right):
        return send(mine.at[h], span_in.at[h, 1 - right], span_send.at[h], span_recv.at[2 * h + 1 - right],
                    (z + 2 * right - 1) * 2 + x)
    def span_arrival(h, side):
        wait_all(span_in.at[h, side], span_recv.at[2 * h + side])
    for h in range(2):
        @pl.when(z == 0)
        def _():
            if roots[h] != 0:
                span_copy(h, 1).start()
        @pl.when(z == zs - 1)
        def _():
            if roots[h] != zs - 1:
                span_copy(h, 0).start()

    start_pairs(pairs_sent(stops[3]), pairs_sent(stops[3]) + middle)
    relay_range(stops[3], stops[4], middle)

    def embed_copy(j, right):
        source = z + j - 2 * right * j
        return send(embed_all.at[source], embed_all.at[source], embed_send.at[right], embed_recv.at[source],
                    (z + 2 * right - 1) * 2 + x)

    def embed_step(j):
        for right, near_end, there in ((1, before_last, z - j >= 0), (0, after_first, z + j <= zs - 1)):
            @pl.when((near_end == 1) & there)
            def _():
                if j > 0:
                    source = z + j - 2 * right * j
                    wait_all(embed_all.at[source], embed_recv.at[source])
                    embed_copy(j - 1, right).wait_send()
                embed_copy(j, right).start()

    embed_pair.wait_recv()
    for h in range(2):
        for right, between in ((1, (z > 0) & (z < roots[h])), (0, (z < zs - 1) & (z > roots[h]))):
            @pl.when(between)
            def _():
                span_arrival(h, 1 - right)
                mine[h] = (mine[h].astype(F32) + span_in[h, 1 - right].astype(F32)).astype(BF16)
                span_copy(h, right).start()
    embed_step(0)

    relay_range(stops[4], stops[5], middle)

    span_pair_copy = send(span_part, span_pair, span_pair_sem.at[0], span_pair_sem.at[1], partner)
    for h in range(2):
        @pl.when(z == roots[h])
        def _():
            total = mine[h].astype(F32)
            for side, there in ((0, roots[h] > 0), (1, roots[h] < zs - 1)):
                if there:
                    span_arrival(h, side)
                    total = total + span_in[h, side].astype(F32)
            span_part[...] = total.astype(BF16)
            span_pair_copy.start()
    first_swap()
    embed_step(1)

    start_pairs(pairs_sent(stops[5]) + middle, pairs_sent(stops[5]) + 3 * middle)
    relay_range(stops[5], stops[6], 3 * middle)

    def all_copy(h, d):
        return send(span_all.at[h], span_all.at[h], all_send, all_recv.at[h], lax.rem(z + d, zs) * 2 + x)
    for h in range(2):
        @pl.when(z == roots[h])
        def _():
            span_pair_copy.wait_recv()
            span_all[h] = (span_part[...].astype(F32) + span_pair[...].astype(F32)).astype(BF16)
            for d in range(1, zs):
                all_copy(h, d).start()
    for j in range(2, zs - 1):
        embed_step(j)

    relay_range(stops[6], stops[7], 3 * middle)
    start_pairs(pairs_sent(relays) + 3 * middle, zs * q)
    square = jnp.zeros((8, emit), F32)
    square = first_finish(square)
    square = lax.fori_loop(0, 5, finish, square)

    for j in range(1, zs):
        for right, near_end, there in ((1, before_last, z - j >= 0), (0, after_first, z + j <= zs - 1)):
            source = z + j - 2 * right * j
            @pl.when(there if j == zs - 1 else (near_end == 0) & there)
            def _():
                wait_all(embed_all.at[source], embed_recv.at[source])
    for right, near_end, last in ((1, before_last, z), (0, after_first, zs - 1 - z)):
        for j in range(zs - 1):
            @pl.when((near_end == 1) & (last == j))
            def _():
                embed_copy(j, right).wait_send()
    wait_all(ids_all.at[pl.ds(0, n - 1)], ids_recv)
    wanted = lax.broadcasted_iota(jnp.int32, (clients, clients), 0) + me * clients
    embed_raw = jnp.zeros((clients, emit), F32)
    for c in range(n):
        chosen = (jnp.broadcast_to(ids_all[c], (clients, clients)) == wanted).astype(F32).astype(BF16)
        embed_raw = embed_raw + jnp.dot(chosen, embed_all[c // 2, c % 2], preferred_element_type=F32)
    embed_v[...] = embed_raw
    embed_write = pltpu.make_async_copy(embed_v, embed_out, write_sem.at[0])
    embed_write.start()
    embed_square = jnp.sum(embed_raw * embed_raw)

    rest_square = jnp.zeros((), F32)
    for h in range(2):
        @pl.when(z != roots[h])
        def _():
            wait_all(span_all.at[h], all_recv.at[h])
        value = span_all[h].astype(F32)
        rest_v[:, pl.ds(h * half, half)] = value
        rest_square = rest_square + jnp.sum(value * value)
    rest_write = pltpu.make_async_copy(rest_v, rest_out, write_sem.at[1])
    rest_write.start()

    square = lax.fori_loop(5, q, finish, square)
    head_total = jnp.sum(square)

    lane = lax.broadcasted_iota(jnp.int32, (1, 128), 1)
    stat_all[flat] = jnp.where(lane == 0, head_total, jnp.where(lane == 1, embed_square, rest_square / n))
    def tell(client, head):
        pltpu.make_async_remote_copy(
            src_ref=stat_all.at[flat], dst_ref=stat_all.at[flat], send_sem=stat_send, recv_sem=stat_recv,
            device_id={"client": client, "head": head}, device_id_type=MESH).start()
    each_other(tell)

    @pl.when(swaps * middle == 0)
    def _():
        wait_all(part.at[pl.ds(0, zs * q * sub)], pair_send)
    if cross:
        @pl.when(middle == 1)
        def _():
            wait_all(part.at[pl.ds(0, (zs * q - 1) * sub)], pair_send)
            cross_copy.wait_send()
    def line_sent(r, carry):
        line_copy(r).wait_send()
        return carry
    lax.fori_loop(relays - queue, relays, line_sent, 0)
    wait_all(part.at[pl.ds(0, firsts * sub)], first_send)
    swap_copy.wait_send()
    embed_pair.wait_send()
    wait_all(small.at[pl.ds(0, heads - 1)], head_send)
    wait_all(ids_all.at[pl.ds(0, n - 1)], ids_send)
    for h in range(2):
        @pl.when(z < roots[h])
        def _():
            span_copy(h, 1).wait_send()
        @pl.when(z > roots[h])
        def _():
            span_copy(h, 0).wait_send()
        @pl.when(z == roots[h])
        def _():
            span_pair_copy.wait_send()
            wait_all(part.at[pl.ds(0, (zs - 1) * mine.shape[1] // 2)], all_send)
    embed_write.wait()
    rest_write.wait()
    pltpu.make_async_copy(head_v, head_out, out_sem).wait()

    wait_all(stat_all.at[pl.ds(0, devices - 1)], stat_recv)
    stat_out[...] = jnp.sum(stat_all[...], axis=0)
    wait_all(stat_all.at[pl.ds(0, devices - 1)], stat_send)


def scale_kernel(sizes, stat_ref, head_ref, rest_ref, embed_ref, head_out, bias_out, embed_out, span_out,
                 stat, head, rest, embed, in_sem, out_sem):
    head_size, embed_size, rest_size = sizes
    spans = span_out.shape[0]
    steps = in_sem.shape[0] - 3
    rows = head.shape[0] // steps
    stat_in = pltpu.make_async_copy(stat_ref, stat, in_sem.at[steps])
    rest_in = pltpu.make_async_copy(rest_ref, rest, in_sem.at[steps + 1])
    embed_in = pltpu.make_async_copy(embed_ref, embed, in_sem.at[steps + 2])
    def part(ref, i):
        return ref.at[pl.ds(i * rows, rows), :]
    stat_in.start()
    rest_in.start()
    embed_in.start()
    heads_in = [pltpu.make_async_copy(part(head_ref, i), part(head, i), in_sem.at[i]) for i in range(steps)]
    heads_out = [pltpu.make_async_copy(part(head, i), part(head_out, i), out_sem.at[i]) for i in range(steps)]
    for copy in heads_in:
        copy.start()
    stat_in.wait()
    factor = clip_factor(stat[0:1, 0:1], head_size)
    embed_factor = clip_factor(stat[0:1, 1:2], embed_size)
    rest_factor = clip_factor(stat[0:1, 2:3], rest_size)
    rest_in.wait()
    rest[...] = rest_factor * rest[...]
    bias_copy = pltpu.make_async_copy(rest.at[pl.ds(spans, 1), :], bias_out, out_sem.at[steps])
    span_copy = pltpu.make_async_copy(rest.at[pl.ds(0, spans), :], span_out, out_sem.at[steps + 1])
    bias_copy.start()
    span_copy.start()
    embed_in.wait()
    embed[...] = embed_factor * embed[...]
    embed_copy = pltpu.make_async_copy(embed, embed_out, out_sem.at[steps + 2])
    embed_copy.start()
    for i in range(steps):
        heads_in[i].wait()
        head[pl.ds(i * rows, rows), :] = factor * head[pl.ds(i * rows, rows), :]
        heads_out[i].start()
    for copy in heads_out + [bias_copy, span_copy, embed_copy]:
        copy.wait()


def per_device(n, heads, pre, delta, head_weight, client_ids):
    rows, hidden_width = pre.shape
    emit = delta.shape[1]
    clients = client_ids.shape[0]
    spans = rows // clients
    block = hidden_width // n
    piece = min(256, block)
    hq = block // piece
    zs = n // 2
    q = 7
    sub = block // (q + 1)
    padded = (spans + 16) // 16 * 16
    half = emit // 2
    cfg = (n, heads, block, piece, spans, clients)
    ids = client_ids.reshape(1, clients)
    hbm = pl.BlockSpec(memory_space=pl.ANY)
    vmem = pl.BlockSpec(memory_space=pltpu.VMEM)
    dma = pltpu.SemaphoreType.DMA
    chunk = math.gcd(rows, 256)
    head_raw, rest_raw, embed_raw, stats = pl.pallas_call(
        functools.partial(kernel, cfg),
        out_shape=(
            jax.ShapeDtypeStruct((block, emit), F32),
            jax.ShapeDtypeStruct((padded, emit), F32),
            jax.ShapeDtypeStruct((clients, emit), F32),
            jax.ShapeDtypeStruct((1, 128), F32),
        ),
        in_specs=[hbm, hbm, hbm, hbm],
        out_specs=(hbm, hbm, hbm, vmem),
        scratch_shapes=[
            pltpu.VMEM((n, rows, block), BF16),
            pltpu.VMEM((rows, emit), F32),
            pltpu.VMEM((rows, emit), BF16),
            pltpu.VMEM((hidden_width, emit), BF16),
            pltpu.VMEM((hidden_width, emit), BF16),
            pltpu.VMEM((zs * q, sub, emit), BF16),
            pltpu.VMEM(((zs + 2) * q, sub, emit), BF16),
            pltpu.VMEM(((zs + 2) * 2, sub, emit), BF16),
            pltpu.VMEM((sub, emit), BF16),
            pltpu.VMEM((sub, emit), BF16),
            pltpu.VMEM((block, emit), F32),
            pltpu.VMEM((heads, spans + clients, emit), BF16),
            pltpu.VMEM((heads - 1, spans + clients, emit), BF16),
            pltpu.VMEM((2, padded, half), BF16),
            pltpu.VMEM((2, 2, padded, half), BF16),
            pltpu.VMEM((padded, half), BF16),
            pltpu.VMEM((padded, half), BF16),
            pltpu.VMEM((2, padded, half), BF16),
            pltpu.VMEM((zs, 2, clients, emit), BF16),
            pltpu.VMEM((n, 1, clients), jnp.int32),
            pltpu.VMEM((clients, emit), F32),
            pltpu.VMEM((padded, emit), F32),
            pltpu.VMEM((n * heads, 1, 128), F32),
            dma((2,)), dma((rows // chunk,)), dma((rows // chunk,)), dma, dma,
            dma, dma((zs * q,)), dma((4,)), dma(((zs + 1) * q,)),
            dma, dma(((zs + 1) * 2,)), dma((2,)), dma((2,)), dma, dma,
            dma((2,)), dma((4,)), dma((2,)), dma, dma((2,)), dma((2,)), dma((2,)), dma((2,)), dma((zs,)),
            dma, dma, dma, dma, dma,
        ],
        compiler_params=pltpu.CompilerParams(
            collective_id=0, has_side_effects=True, vmem_limit_bytes=62 * 2**20
        ),
        name="clipped_grads",
    )(pre, delta, head_weight, ids)
    sizes = (hidden_width * emit * heads, clients * n * hidden_width, spans * hidden_width + emit * heads)
    steps = 4
    head_grad, bias_grad, embed_grad, span_grad = pl.pallas_call(
        functools.partial(scale_kernel, sizes),
        out_shape=(
            jax.ShapeDtypeStruct((block, emit), F32),
            jax.ShapeDtypeStruct((1, emit), F32),
            jax.ShapeDtypeStruct((clients, emit), F32),
            jax.ShapeDtypeStruct((spans, emit), F32),
        ),
        in_specs=[hbm] * 4,
        out_specs=(hbm,) * 4,
        scratch_shapes=[
            pltpu.VMEM((1, 128), F32),
            pltpu.VMEM((block, emit), F32),
            pltpu.VMEM((padded, emit), F32),
            pltpu.VMEM((clients, emit), F32),
            dma((steps + 3,)), dma((steps + 3,)),
        ],
        name="scaled",
    )(stats, head_raw, rest_raw, embed_raw)
    return head_grad, bias_grad.reshape(emit), embed_grad, span_grad


def solution(mesh):
    placed = (P("client", None), P("client", "head"), P(None, "head"), P("client"))
    return jax.shard_map(
        functools.partial(per_device, mesh.shape["client"], mesh.shape["head"]),
        mesh=mesh,
        in_specs=placed,
        out_specs=(P("client", "head"), P("head"), P("client", "head"), P(None, "head")),
        check_vma=False,
    )
```

```python
import functools
import math

import jax
import jax.numpy as jnp
from jax import lax
from jax.experimental import pallas as pl
from jax.experimental.pallas import tpu as pltpu
from jax.sharding import PartitionSpec as P

EPSILON = 1e-06
MESH = pl.DeviceIdType.MESH
F32 = jnp.float32
BF16 = jnp.bfloat16


def clip_factor(total, number):
    return jnp.minimum(1.0, 1.0 / jnp.sqrt(total / number + EPSILON))


def kernel(cfg, pre_ref, delta_ref, weight_ref, ids_ref, head_out, rest_out, embed_out, stat_out,
           pre_v, delta_v, low, weight_v, part, pair_in, line_in, first_in, swap_in, cross_in, sum_v, head_v,
           small, small_in, mine, span_in, span_part, span_pair, span_all, embed_all, ids_all,
           embed_v, rest_v, stat_all,
           pre_sem, delta_sem, weight_sem, out_sem, pair_send, pair_recv, line_send, line_recv,
           first_send, first_recv, swap_sem, cross_sem, head_send, head_recv, span_send, span_recv, span_pair_sem,
           all_send, all_recv, write_sem, embed_pair_sem, embed_send, embed_recv, ids_sem, ids_send, ids_recv,
           stat_send, stat_recv):
    n, heads, block, piece, spans, clients = cfg
    zs = n // 2
    q = 7
    sub = block // (q + 1)
    hq = block // piece
    rows, emit = low.shape
    half = emit // 2
    me = lax.axis_index("client")
    my_head = lax.axis_index("head")
    z = me // 2
    x = me % 2
    relays = (zs - 1) * q
    firsts = 2 * (zs - 1)
    slopes = 2 * zs * hq
    devices = n * heads
    flat = me * heads + my_head

    after_first = (z + zs - 1) // zs
    before_last = (2 * zs - 2 - z) // zs
    middle = after_first * before_last
    upper = 2 * z // zs
    near = z + upper * (zs - 1 - 2 * z)
    partner = z * 2 + 1 - x

    def wait_all(ref, sem):
        pltpu.make_async_copy(ref, ref, sem).wait()

    def send(src, dst, send_sem, recv_sem, client):
        return pltpu.make_async_remote_copy(
            src_ref=src, dst_ref=dst, send_sem=send_sem, recv_sem=recv_sem,
            device_id={"client": client}, device_id_type=MESH)

    def dest(k):
        both = (2 * near - k - 1 + zs) // zs
        odd = k % 2
        out = both * (odd * (k // 2) + (1 - odd) * (zs - 1 - k // 2)) + (1 - both) * (zs - 1 - k + near)
        return out + upper * (zs - 1 - 2 * out)

    def block_row(place, side):
        return (place * 2 + side) * block

    def piece_row(place, side, s):
        return pl.multiple_of(block_row(place, side) + (s + 1) * sub, sub)

    def landing(place):
        right = (place - z + zs) // zs
        target = z + 2 * right - 1
        gap = right * (place - target) + (1 - right) * (target - place)
        away = (gap + zs - 1) // zs
        slot = away * place + (1 - away) * (zs + 1 - right)
        sem = away * place + (1 - away) * (right * zs + (1 - right) * place)
        return target * 2 + x, slot, sem

    def unit_side(u):
        return (x + 1 - u % 2) % 2

    def unit_row(u):
        return pl.multiple_of(block_row(dest(u // 2), unit_side(u)), block)

    def pre_copy(u, h, sem):
        columns = pl.ds(pl.multiple_of(unit_row(u) + h * piece, piece), piece)
        return pltpu.make_async_copy(
            pre_ref.at[:, columns], pre_v.at[u, :, pl.ds(pl.multiple_of(h * piece, piece), piece)], pre_sem.at[sem])

    chunk = math.gcd(rows, 256)
    delta_copies = [
        pltpu.make_async_copy(delta_ref.at[pl.ds(c * chunk, chunk), :], delta_v.at[pl.ds(c * chunk, chunk), :],
                              delta_sem.at[c])
        for c in range(rows // chunk)]
    weight_copy = pltpu.make_async_copy(weight_ref, weight_v, weight_sem)
    ids_copy = pltpu.make_async_copy(ids_ref, ids_all.at[me], ids_sem)
    opened = min(128, piece)
    first_column = pl.multiple_of(unit_row(0), opened)
    rest_columns = piece - opened
    rest_copy = None
    if rest_columns > 0:
        rest_copy = pltpu.make_async_copy(
            pre_ref.at[:, pl.ds(pl.multiple_of(first_column + opened, opened), rest_columns)],
            pre_v.at[0, :, pl.ds(opened, rest_columns)], pre_sem.at[2])
    first_copies = [
        pltpu.make_async_copy(pre_ref.at[pl.ds(c * chunk, chunk), pl.ds(first_column, opened)],
                              pre_v.at[0, pl.ds(c * chunk, chunk), pl.ds(0, opened)], delta_sem.at[c])
        for c in range(rows // chunk)]
    for c in range(rows // chunk):
        first_copies[c].start()
        delta_copies[c].start()

    def each_other(action):
        columns = [lax.rem(my_head + d, heads) for d in range(heads - 1, -1, -1)]
        def body(j, carry):
            client = dest(j // 2) * 2 + unit_side(j)
            for column in columns:
                action(client, column)
            return carry
        lax.fori_loop(0, n - 1, body, 0)
        for column in columns[:-1]:
            action(me, column)

    barrier = pltpu.get_barrier_semaphore()
    def greet(client, head):
        pl.semaphore_signal(barrier, inc=1, device_id={"client": client, "head": head}, device_id_type=MESH)
    each_other(greet)

    def load(u, carry):
        pre_copy(u, 0, 0).start()
        return carry
    def load_rest(u, carry):
        @pl.when(u >= firsts)
        def _():
            pre_copy(u, 0, 1).start()
        for h in range(1, hq):
            pre_copy(u, h, 1).start()
        return carry

    def product(u, h):
        p = pre_v[u, :, pl.ds(pl.multiple_of(h * piece, piece), piece)].astype(F32)
        hidden = (p * jax.nn.sigmoid(p)).astype(BF16)
        value = lax.dot_general(hidden, low[...], (((0,), (0,)), ((), ())), preferred_element_type=F32)
        part[pl.ds(pl.multiple_of(unit_row(u) + h * piece, piece), piece), :] = value.astype(BF16)

    def slope_sums(t):
        u = t // hq
        h = t % hq
        p = pre_v[u, :, pl.ds(pl.multiple_of(h * piece, piece), piece)].astype(F32)
        row = pl.multiple_of(unit_row(u) + h * piece, piece)
        value = lax.dot_general(
            low[...], weight_v[pl.ds(row, piece), :], (((1,), (1,)), ((), ())), preferred_element_type=F32)
        s = jax.nn.sigmoid(p)
        grad = value.astype(BF16).astype(F32) * (s * (1.0 + p * (1.0 - s)))
        grad = grad.reshape(clients, spans, piece)
        to = row // emit
        columns = pl.ds(pl.multiple_of(row % emit, piece), piece)
        small[to, pl.ds(0, spans), columns] = jnp.sum(grad, axis=0).astype(BF16)
        small[to, pl.ds(spans, clients), columns] = jnp.sum(grad, axis=1).astype(BF16)

    def pair_copy(i):
        return send(part.at[pl.ds(piece_row(dest(i // q), 1 - x, i % q), sub), :], pair_in.at[i],
                    pair_send, pair_recv.at[i], partner)

    queue = 3 + middle
    cross = zs == 4
    swaps = 1 if cross else 0
    skip = q - 1

    def order(r):
        m = r - q
        late = swaps * middle * ((m + relays) // relays)
        return late * (q + m % 2 * q + m // 2) + (1 - late) * r

    def pairs_sent(r):
        late = swaps * middle * ((r - q + relays) // relays)
        return late * (2 * q + 3 + (r - q) // 2) + (1 - late) * (r + q + (2 + swaps) * middle)

    def line_copy(r):
        i = order(r)
        place = dest(i // q)
        target, slot, sem = landing(place)
        return send(part.at[pl.ds(piece_row(place, x, i % q), sub), :], line_in.at[slot * q + i % q],
                    line_send.at[r % queue], line_recv.at[sem * q + i % q], target)

    step_rows = min(32, sub)

    def start_pairs(start, stop):
        def body(i, carry):
            @pl.when((i < zs * q) & (swaps * middle * (skip + 1) != i + 1))
            def _():
                pair_copy(i).start()
            return carry
        lax.fori_loop(start, stop, body, 0)

    cross_copy = send(part.at[pl.ds(piece_row(dest(0), 1 - x, skip), sub), :], cross_in,
                      cross_sem.at[0], cross_sem.at[1], landing(dest(0))[0])

    def cross_add():
        row = piece_row(dest(1), 1 - x, skip)
        cross_copy.wait_recv()
        def add(r, carry):
            at = pl.ds(pl.multiple_of(r * step_rows, step_rows), step_rows)
            mine_at = pl.ds(pl.multiple_of(row + r * step_rows, step_rows), step_rows)
            part[mine_at, :] = (part[mine_at, :].astype(F32) + cross_in[at, :].astype(F32)).astype(BF16)
            return carry
        lax.fori_loop(0, sub // step_rows, add, 0)

    def relay(r, extra):
        i = order(r)
        place = dest(i // q)
        row = piece_row(place, x, i % q)
        @pl.when(swaps * middle * (skip + 1) != i + 1)
        def _():
            pair_copy(i).wait_recv()
        @pl.when(middle == 1)
        def _():
            wait_all(line_in.at[place * q + i % q], line_recv.at[place * q + i % q])
        slot = middle * (place * q + i % q) + (1 - middle) * z * q
        def add(r, carry):
            at = pl.ds(pl.multiple_of(r * step_rows, step_rows), step_rows)
            mine_at = pl.ds(pl.multiple_of(row + r * step_rows, step_rows), step_rows)
            total = part[mine_at, :].astype(F32) + pair_in[i, at, :].astype(F32)
            part[mine_at, :] = (total + line_in[slot, at, :].astype(F32)).astype(BF16)
            return carry
        lax.fori_loop(0, sub // step_rows, add, 0)
        @pl.when(r >= queue)
        def _():
            line_copy(r - queue).wait_send()
        line_copy(r).start()
        start_pairs(pairs_sent(r) + extra, pairs_sent(r + 1) + extra)

    def relay_range(start, stop, extra):
        def body(r, carry):
            relay(r, extra)
            return carry
        lax.fori_loop(start, stop, body, 0)

    def finish(s, square):
        i = relays + s
        row = piece_row(z, x, s)
        pair_copy(i).wait_recv()
        @pl.when(after_first == 1)
        def _():
            wait_all(line_in.at[zs * q + s], line_recv.at[zs * q + s])
        @pl.when(before_last == 1)
        def _():
            wait_all(line_in.at[(zs + 1) * q + s], line_recv.at[z * q + s])
        left = after_first * (zs * q + s) + (1 - after_first) * z * q
        right = before_last * ((zs + 1) * q + s) + (1 - before_last) * z * q
        def add(r, carry):
            at = pl.ds(pl.multiple_of(r * step_rows, step_rows), step_rows)
            mine_at = pl.ds(pl.multiple_of(row + r * step_rows, step_rows), step_rows)
            out_at = pl.ds(pl.multiple_of((s + 1) * sub + r * step_rows, step_rows), step_rows)
            total = part[mine_at, :].astype(F32) + pair_in[i, at, :].astype(F32)
            total = total + line_in[left, at, :].astype(F32) + line_in[right, at, :].astype(F32)
            head_v[out_at, :] = total.astype(BF16)
            return carry + jnp.sum((total * total).reshape(step_rows // 8, 8, emit), axis=0)
        square = lax.fori_loop(0, sub // step_rows, add, square)
        at = pl.ds(pl.multiple_of((s + 1) * sub, sub), sub)
        pltpu.make_async_copy(head_v.at[at, :], head_out.at[at, :], out_sem).start()
        return square

    def first_copy(j):
        place = dest(j // 2)
        side = unit_side(j)
        target, slot, sem = landing(place)
        return send(part.at[pl.ds(pl.multiple_of(block_row(place, side), sub), sub), :],
                    first_in.at[slot * 2 + side], first_send, first_recv.at[sem * 2 + side], target)

    def first_relay(j):
        @pl.when(middle == 1)
        def _():
            place = dest(j // 2)
            side = unit_side(j)
            row = pl.multiple_of(block_row(place, side), sub)
            wait_all(first_in.at[place * 2 + side], first_recv.at[place * 2 + side])
            def add(r, carry):
                at = pl.ds(pl.multiple_of(r * step_rows, step_rows), step_rows)
                mine_at = pl.ds(pl.multiple_of(row + r * step_rows, step_rows), step_rows)
                part[mine_at, :] = (
                    part[mine_at, :].astype(F32) + first_in[place * 2 + side, at, :].astype(F32)).astype(BF16)
                return carry
            lax.fori_loop(0, sub // step_rows, add, 0)
            first_copy(j).start()

    swap_copy = send(part.at[pl.ds(pl.multiple_of(block_row(z, 1 - x), sub), sub), :], swap_in,
                     swap_sem.at[0], swap_sem.at[1], partner)

    def first_wait(side):
        @pl.when(after_first == 1)
        def _():
            wait_all(first_in.at[zs * 2 + side], first_recv.at[zs * 2 + side])
        @pl.when(before_last == 1)
        def _():
            wait_all(first_in.at[(zs + 1) * 2 + side], first_recv.at[z * 2 + side])
        left = after_first * (zs * 2 + side) + (1 - after_first) * z * 2
        right = before_last * ((zs + 1) * 2 + side) + (1 - before_last) * z * 2
        return left, right

    def first_swap():
        row = block_row(z, 1 - x)
        left, right = first_wait(1 - x)
        def add(r, carry):
            at = pl.ds(pl.multiple_of(r * step_rows, step_rows), step_rows)
            mine_at = pl.ds(pl.multiple_of(row + r * step_rows, step_rows), step_rows)
            total = part[mine_at, :].astype(F32) + first_in[left, at, :].astype(F32)
            part[mine_at, :] = (total + first_in[right, at, :].astype(F32)).astype(BF16)
            return carry
        lax.fori_loop(0, sub // step_rows, add, 0)
        swap_copy.start()

    def first_finish(square):
        row = block_row(z, x)
        left, right = first_wait(x)
        swap_copy.wait_recv()
        def add(r, carry):
            at = pl.ds(pl.multiple_of(r * step_rows, step_rows), step_rows)
            mine_at = pl.ds(pl.multiple_of(row + r * step_rows, step_rows), step_rows)
            total = part[mine_at, :].astype(F32) + first_in[left, at, :].astype(F32)
            total = total + first_in[right, at, :].astype(F32) + swap_in[at, :].astype(F32)
            head_v[at, :] = total.astype(BF16)
            return carry + jnp.sum((total * total).reshape(step_rows // 8, 8, emit), axis=0)
        square = lax.fori_loop(0, sub // step_rows, add, square)
        pltpu.make_async_copy(head_v.at[pl.ds(0, sub), :], head_out.at[pl.ds(0, sub), :], out_sem).start()
        return square

    if rest_columns > 0:
        rest_copy.start()
    lax.fori_loop(1, firsts, load, 0)
    step = 64
    for c in range(rows // chunk):
        wait_all(delta_v.at[pl.ds(0, chunk + chunk * opened // (2 * emit)), :], delta_sem.at[c])
        def narrow(r, carry):
            at = pl.ds(pl.multiple_of(c * chunk + r * step, step), step)
            low[at, :] = delta_v[at, :].astype(BF16)
            return carry
        lax.fori_loop(0, chunk // step, narrow, 0)
        at = pl.ds(c * chunk, chunk)
        p = pre_v[0, at, pl.ds(0, opened)].astype(F32)
        hidden = (p * jax.nn.sigmoid(p)).astype(BF16)
        value = lax.dot_general(hidden, low[at, :], (((0,), (0,)), ((), ())), preferred_element_type=F32)
        if c > 0:
            value = value + sum_v[...]
        if c < len(delta_copies) - 1:
            sum_v[...] = value
        else:
            part[pl.ds(pl.multiple_of(unit_row(0), opened), opened), :] = value.astype(BF16)

    pl.semaphore_wait(barrier, devices - 1)

    ready = min(piece // sub - 1, q)
    soon = min(opened // sub - 1, q)
    @pl.when(middle == 0)
    def _():
        first_copy(0).start()
    for i in range(soon):
        pair_copy(i).start()
    if rest_columns > 0:
        rest_copy.wait()
        p = pre_v[0, :, pl.ds(opened, rest_columns)].astype(F32)
        hidden = (p * jax.nn.sigmoid(p)).astype(BF16)
        value = lax.dot_general(hidden, low[...], (((0,), (0,)), ((), ())), preferred_element_type=F32)
        part[pl.ds(pl.multiple_of(unit_row(0) + opened, opened), rest_columns), :] = value.astype(BF16)
    for i in range(soon, ready):
        pair_copy(i).start()
    lax.fori_loop(0 if hq > 1 else firsts, 2 * zs, load_rest, 0)
    weight_copy.start()
    ids_copy.start()
    line_in[z * q] = jnp.zeros((sub, emit), BF16)
    first_in[z * 2] = jnp.zeros((sub, emit), BF16)

    wait_all(pre_v.at[pl.ds(0, firsts - 1), :, pl.ds(0, piece)], pre_sem.at[0])
    def opening(u, carry):
        product(u, 0)
        @pl.when(middle == 0)
        def _():
            first_copy(u).start()
        return carry
    lax.fori_loop(1, firsts, opening, 0)
    wait_all(pre_v.at[pl.ds(0, (2 * zs * hq - firsts) // hq)], pre_sem.at[1])
    if hq > 1:
        def second(t, carry):
            product(t // (hq - 1), 1 + t % (hq - 1))
            return carry
        lax.fori_loop(0, 3 * (hq - 1), second, 0)
    if cross:
        @pl.when(middle == 1)
        def _():
            pair_in[skip] = jnp.zeros((sub, emit), BF16)
            cross_copy.start()
    start_pairs(ready, pairs_sent(0))
    first_relay(0)
    first_relay(1)
    weight_copy.wait()

    ids_copy.wait()
    for d in range(1, n):
        send(ids_all.at[me], ids_all.at[me], ids_send, ids_recv, lax.rem(me + d, n)).start()

    base = 3 + middle * (slopes - 8)
    stride = 3 - middle
    def main(t, carry):
        slope_sums(t)
        @pl.when((t >= 4) & (t % 2 == 0) & (t // 2 < firsts))
        def _():
            first_relay(t // 2)
        @pl.when((t >= base) & ((t - base) % stride == 0))
        def _():
            relay((t - base) // stride, 0)
        return carry
    lax.fori_loop(0, slopes, main, 0)

    for d in range(1, heads):
        target = lax.rem(my_head + d, heads)
        pltpu.make_async_remote_copy(
            src_ref=small.at[target], dst_ref=small_in.at[lax.rem(my_head - target + heads, heads) - 1],
            send_sem=head_send, recv_sem=head_recv, device_id={"head": target}, device_id_type=MESH).start()

    if cross:
        @pl.when(middle == 1)
        def _():
            cross_add()

    done = slopes // 2
    if done < firsts:
        def rest_first(j, carry):
            first_relay(j)
            return carry
        lax.fori_loop(done, firsts, rest_first, 0)

    def add_rows(r, total):
        value = delta_v[pl.ds(pl.multiple_of(r * step, step), step), :]
        return total + jnp.sum(value.reshape(step // 8, 8, emit), axis=0)
    bias = lax.fori_loop(0, rows // step, add_rows, jnp.zeros((8, emit), F32))
    bias = jnp.sum(bias, axis=0, keepdims=True)
    pad = mine.shape[1] - spans
    tail = jnp.where(
        lax.broadcasted_iota(jnp.int32, (pad, emit), 0) == 0, jnp.broadcast_to(bias, (pad, emit)), 0.0
    ).astype(BF16)
    for h in range(2):
        mine[h, pl.ds(spans, pad), :] = tail[:, h * half:(h + 1) * half]

    ends = [(slopes - 4) // 3 + 1] + [(slopes - 4) // 3 + 1 + k for k in (2, 4, 4, 8, 13, 16)]
    inner = [3] + [3 + k for k in (1, 2, 3, 8, 15, 18)]
    stops = [(1 - middle) * e + middle * i for e, i in zip(ends, inner)] + [relays]

    if hq > 1:
        def third(t, carry):
            product(3 + t // (hq - 1), 1 + t % (hq - 1))
            return carry
        lax.fori_loop(0, (2 * zs - 5) * (hq - 1), third, 0)
    relay_range(stops[0], stops[1], 0)
    def fourth(t, carry):
        product(2 * zs - 2 + t // hq, t % hq)
        return carry
    lax.fori_loop(0, 2 * hq, fourth, 0)
    relay_range(stops[1], stops[2], 0)
    relay_range(stops[2], stops[3], 0)

    wait_all(small_in, head_recv)
    total = small[my_head].astype(F32)
    for d in range(heads - 1):
        total = total + small_in[d].astype(F32)
    for h in range(2):
        mine[h, pl.ds(0, spans), :] = total[:spans, h * half:(h + 1) * half].astype(BF16)
    embed_all[z, x] = total[spans:].astype(BF16)

    embed_pair = send(embed_all.at[z, x], embed_all.at[z, x], embed_pair_sem.at[0], embed_pair_sem.at[1], partner)
    embed_pair.start()

    roots = [zs // 2 - 1, zs // 2]
    def span_copy(h, right):
        return send(mine.at[h], span_in.at[h, 1 - right], span_send.at[h], span_recv.at[2 * h + 1 - right],
                    (z + 2 * right - 1) * 2 + x)
    def span_arrival(h, side):
        wait_all(span_in.at[h, side], span_recv.at[2 * h + side])
    for h in range(2):
        @pl.when(z == 0)
        def _():
            if roots[h] != 0:
                span_copy(h, 1).start()
        @pl.when(z == zs - 1)
        def _():
            if roots[h] != zs - 1:
                span_copy(h, 0).start()

    start_pairs(pairs_sent(stops[3]), pairs_sent(stops[3]) + middle)
    relay_range(stops[3], stops[4], middle)

    def embed_copy(j, right):
        source = z + j - 2 * right * j
        return send(embed_all.at[source], embed_all.at[source], embed_send.at[right], embed_recv.at[source],
                    (z + 2 * right - 1) * 2 + x)

    def embed_step(j):
        for right, near_end, there in ((1, before_last, z - j >= 0), (0, after_first, z + j <= zs - 1)):
            @pl.when((near_end == 1) & there)
            def _():
                if j > 0:
                    source = z + j - 2 * right * j
                    wait_all(embed_all.at[source], embed_recv.at[source])
                    embed_copy(j - 1, right).wait_send()
                embed_copy(j, right).start()

    embed_pair.wait_recv()
    for h in range(2):
        for right, between in ((1, (z > 0) & (z < roots[h])), (0, (z < zs - 1) & (z > roots[h]))):
            @pl.when(between)
            def _():
                span_arrival(h, 1 - right)
                mine[h] = (mine[h].astype(F32) + span_in[h, 1 - right].astype(F32)).astype(BF16)
                span_copy(h, right).start()
    embed_step(0)

    relay_range(stops[4], stops[5], middle)

    span_pair_copy = send(span_part, span_pair, span_pair_sem.at[0], span_pair_sem.at[1], partner)
    for h in range(2):
        @pl.when(z == roots[h])
        def _():
            total = mine[h].astype(F32)
            for side, there in ((0, roots[h] > 0), (1, roots[h] < zs - 1)):
                if there:
                    span_arrival(h, side)
                    total = total + span_in[h, side].astype(F32)
            span_part[...] = total.astype(BF16)
            span_pair_copy.start()
    first_swap()
    embed_step(1)

    start_pairs(pairs_sent(stops[5]) + middle, pairs_sent(stops[5]) + 3 * middle)
    relay_range(stops[5], stops[6], 3 * middle)

    def all_copy(h, d):
        return send(span_all.at[h], span_all.at[h], all_send, all_recv.at[h], lax.rem(z + d, zs) * 2 + x)
    for h in range(2):
        @pl.when(z == roots[h])
        def _():
            span_pair_copy.wait_recv()
            span_all[h] = (span_part[...].astype(F32) + span_pair[...].astype(F32)).astype(BF16)
            for d in range(1, zs):
                all_copy(h, d).start()
    for j in range(2, zs - 1):
        embed_step(j)

    relay_range(stops[6], stops[7], 3 * middle)
    start_pairs(pairs_sent(relays) + 3 * middle, zs * q)
    square = jnp.zeros((8, emit), F32)
    square = first_finish(square)
    square = lax.fori_loop(0, 5, finish, square)

    for j in range(1, zs):
        for right, near_end, there in ((1, before_last, z - j >= 0), (0, after_first, z + j <= zs - 1)):
            source = z + j - 2 * right * j
            @pl.when(there if j == zs - 1 else (near_end == 0) & there)
            def _():
                wait_all(embed_all.at[source], embed_recv.at[source])
    for right, near_end, last in ((1, before_last, z), (0, after_first, zs - 1 - z)):
        for j in range(zs - 1):
            @pl.when((near_end == 1) & (last == j))
            def _():
                embed_copy(j, right).wait_send()
    wait_all(ids_all.at[pl.ds(0, n - 1)], ids_recv)
    wanted = lax.broadcasted_iota(jnp.int32, (clients, clients), 0) + me * clients
    embed_raw = jnp.zeros((clients, emit), F32)
    for c in range(n):
        chosen = (jnp.broadcast_to(ids_all[c], (clients, clients)) == wanted).astype(F32).astype(BF16)
        embed_raw = embed_raw + jnp.dot(chosen, embed_all[c // 2, c % 2], preferred_element_type=F32)
    embed_v[...] = embed_raw
    embed_write = pltpu.make_async_copy(embed_v, embed_out, write_sem.at[0])
    embed_write.start()
    embed_square = jnp.sum(embed_raw * embed_raw)

    rest_square = jnp.zeros((), F32)
    for h in range(2):
        @pl.when(z != roots[h])
        def _():
            wait_all(span_all.at[h], all_recv.at[h])
        value = span_all[h].astype(F32)
        rest_v[:, pl.ds(h * half, half)] = value
        rest_square = rest_square + jnp.sum(value * value)
    rest_write = pltpu.make_async_copy(rest_v, rest_out, write_sem.at[1])
    rest_write.start()

    square = lax.fori_loop(5, q, finish, square)
    head_total = jnp.sum(square)

    lane = lax.broadcasted_iota(jnp.int32, (1, 128), 1)
    stat_all[flat] = jnp.where(lane == 0, head_total, jnp.where(lane == 1, embed_square, rest_square / n))
    def tell(client, head):
        pltpu.make_async_remote_copy(
            src_ref=stat_all.at[flat], dst_ref=stat_all.at[flat], send_sem=stat_send, recv_sem=stat_recv,
            device_id={"client": client, "head": head}, device_id_type=MESH).start()
    each_other(tell)

    @pl.when(swaps * middle == 0)
    def _():
        wait_all(part.at[pl.ds(0, zs * q * sub)], pair_send)
    if cross:
        @pl.when(middle == 1)
        def _():
            wait_all(part.at[pl.ds(0, (zs * q - 1) * sub)], pair_send)
            cross_copy.wait_send()
    def line_sent(r, carry):
        line_copy(r).wait_send()
        return carry
    lax.fori_loop(relays - queue, relays, line_sent, 0)
    wait_all(part.at[pl.ds(0, firsts * sub)], first_send)
    swap_copy.wait_send()
    embed_pair.wait_send()
    wait_all(small.at[pl.ds(0, heads - 1)], head_send)
    wait_all(ids_all.at[pl.ds(0, n - 1)], ids_send)
    for h in range(2):
        @pl.when(z < roots[h])
        def _():
            span_copy(h, 1).wait_send()
        @pl.when(z > roots[h])
        def _():
            span_copy(h, 0).wait_send()
        @pl.when(z == roots[h])
        def _():
            span_pair_copy.wait_send()
            wait_all(part.at[pl.ds(0, (zs - 1) * mine.shape[1] // 2)], all_send)
    embed_write.wait()
    rest_write.wait()
    pltpu.make_async_copy(head_v, head_out, out_sem).wait()

    wait_all(stat_all.at[pl.ds(0, devices - 1)], stat_recv)
    stat_out[...] = jnp.sum(stat_all[...], axis=0)
    wait_all(stat_all.at[pl.ds(0, devices - 1)], stat_send)


def scale_kernel(sizes, stat_ref, head_ref, rest_ref, embed_ref, head_out, bias_out, embed_out, span_out,
                 stat, head_in, head, rest, embed, in_sem, out_sem):
    head_size, embed_size, rest_size = sizes
    spans = span_out.shape[0]
    steps = in_sem.shape[0] - 3
    rows = head.shape[0] // steps
    stat_in = pltpu.make_async_copy(stat_ref, stat, in_sem.at[steps])
    rest_in = pltpu.make_async_copy(rest_ref, rest, in_sem.at[steps + 1])
    embed_in = pltpu.make_async_copy(embed_ref, embed, in_sem.at[steps + 2])
    def part(ref, i):
        return ref.at[pl.ds(i * rows, rows), :]
    stat_in.start()
    heads_in = [pltpu.make_async_copy(part(head_ref, i), part(head_in, i), in_sem.at[i]) for i in range(steps)]
    heads_out = [pltpu.make_async_copy(part(head, i), part(head_out, i), out_sem.at[i]) for i in range(steps)]
    for copy in heads_in:
        copy.start()
    rest_in.start()
    embed_in.start()
    stat_in.wait()
    factor = clip_factor(stat[0:1, 0:1], head_size)
    embed_factor = clip_factor(stat[0:1, 1:2], embed_size)
    rest_factor = clip_factor(stat[0:1, 2:3], rest_size)
    for i in range(steps):
        heads_in[i].wait()
        head[pl.ds(i * rows, rows), :] = factor * head_in[pl.ds(i * rows, rows), :].astype(F32)
        heads_out[i].start()
    rest_in.wait()
    rest[...] = rest_factor * rest[...]
    bias_copy = pltpu.make_async_copy(rest.at[pl.ds(spans, 1), :], bias_out, out_sem.at[steps])
    span_copy = pltpu.make_async_copy(rest.at[pl.ds(0, spans), :], span_out, out_sem.at[steps + 1])
    bias_copy.start()
    span_copy.start()
    embed_in.wait()
    embed[...] = embed_factor * embed[...]
    embed_copy = pltpu.make_async_copy(embed, embed_out, out_sem.at[steps + 2])
    embed_copy.start()
    for copy in heads_out + [bias_copy, span_copy, embed_copy]:
        copy.wait()


def per_device(n, heads, pre, delta, head_weight, client_ids):
    rows, hidden_width = pre.shape
    emit = delta.shape[1]
    clients = client_ids.shape[0]
    spans = rows // clients
    block = hidden_width // n
    piece = min(256, block)
    hq = block // piece
    zs = n // 2
    q = 7
    sub = block // (q + 1)
    padded = (spans + 16) // 16 * 16
    half = emit // 2
    cfg = (n, heads, block, piece, spans, clients)
    ids = client_ids.reshape(1, clients)
    hbm = pl.BlockSpec(memory_space=pl.ANY)
    vmem = pl.BlockSpec(memory_space=pltpu.VMEM)
    dma = pltpu.SemaphoreType.DMA
    chunk = math.gcd(rows, 256)
    head_raw, rest_raw, embed_raw, stats = pl.pallas_call(
        functools.partial(kernel, cfg),
        out_shape=(
            jax.ShapeDtypeStruct((block, emit), BF16),
            jax.ShapeDtypeStruct((padded, emit), F32),
            jax.ShapeDtypeStruct((clients, emit), F32),
            jax.ShapeDtypeStruct((1, 128), F32),
        ),
        in_specs=[hbm, hbm, hbm, hbm],
        out_specs=(hbm, hbm, hbm, vmem),
        scratch_shapes=[
            pltpu.VMEM((n, rows, block), BF16),
            pltpu.VMEM((rows, emit), F32),
            pltpu.VMEM((rows, emit), BF16),
            pltpu.VMEM((hidden_width, emit), BF16),
            pltpu.VMEM((hidden_width, emit), BF16),
            pltpu.VMEM((zs * q, sub, emit), BF16),
            pltpu.VMEM(((zs + 2) * q, sub, emit), BF16),
            pltpu.VMEM(((zs + 2) * 2, sub, emit), BF16),
            pltpu.VMEM((sub, emit), BF16),
            pltpu.VMEM((sub, emit), BF16),
            pltpu.VMEM((min(128, piece), emit), F32),
            pltpu.VMEM((block, emit), BF16),
            pltpu.VMEM((heads, spans + clients, emit), BF16),
            pltpu.VMEM((heads - 1, spans + clients, emit), BF16),
            pltpu.VMEM((2, padded, half), BF16),
            pltpu.VMEM((2, 2, padded, half), BF16),
            pltpu.VMEM((padded, half), BF16),
            pltpu.VMEM((padded, half), BF16),
            pltpu.VMEM((2, padded, half), BF16),
            pltpu.VMEM((zs, 2, clients, emit), BF16),
            pltpu.VMEM((n, 1, clients), jnp.int32),
            pltpu.VMEM((clients, emit), F32),
            pltpu.VMEM((padded, emit), F32),
            pltpu.VMEM((n * heads, 1, 128), F32),
            dma((3,)), dma((rows // chunk,)), dma, dma,
            dma, dma((zs * q,)), dma((4,)), dma(((zs + 1) * q,)),
            dma, dma(((zs + 1) * 2,)), dma((2,)), dma((2,)), dma, dma,
            dma((2,)), dma((4,)), dma((2,)), dma, dma((2,)), dma((2,)), dma((2,)), dma((2,)), dma((zs,)),
            dma, dma, dma, dma, dma,
        ],
        compiler_params=pltpu.CompilerParams(
            collective_id=0, has_side_effects=True, vmem_limit_bytes=62 * 2**20
        ),
        name="clipped_grads",
    )(pre, delta, head_weight, ids)
    sizes = (hidden_width * emit * heads, clients * n * hidden_width, spans * hidden_width + emit * heads)
    steps = 4
    head_grad, bias_grad, embed_grad, span_grad = pl.pallas_call(
        functools.partial(scale_kernel, sizes),
        out_shape=(
            jax.ShapeDtypeStruct((block, emit), F32),
            jax.ShapeDtypeStruct((1, emit), F32),
            jax.ShapeDtypeStruct((clients, emit), F32),
            jax.ShapeDtypeStruct((spans, emit), F32),
        ),
        in_specs=[hbm] * 4,
        out_specs=(hbm,) * 4,
        scratch_shapes=[
            pltpu.VMEM((1, 128), F32),
            pltpu.VMEM((block, emit), BF16),
            pltpu.VMEM((block, emit), F32),
            pltpu.VMEM((padded, emit), F32),
            pltpu.VMEM((clients, emit), F32),
            dma((steps + 3,)), dma((steps + 3,)),
        ],
        name="scaled",
    )(stats, head_raw, rest_raw, embed_raw)
    return head_grad, bias_grad.reshape(emit), embed_grad, span_grad


def solution(mesh):
    placed = (P("client", None), P("client", "head"), P(None, "head"), P("client"))
    return jax.shard_map(
        functools.partial(per_device, mesh.shape["client"], mesh.shape["head"]),
        mesh=mesh,
        in_specs=placed,
        out_specs=(P("client", "head"), P("head"), P("client", "head"), P(None, "head")),
        check_vma=False,
    )
```

```python
import functools
import math

import jax
import jax.numpy as jnp
from jax import lax
from jax.experimental import pallas as pl
from jax.experimental.pallas import tpu as pltpu
from jax.sharding import PartitionSpec as P

EPSILON = 1e-06
MESH = pl.DeviceIdType.MESH
F32 = jnp.float32
BF16 = jnp.bfloat16


def clip_factor(total, number):
    return jnp.minimum(1.0, 1.0 / jnp.sqrt(total / number + EPSILON))


def kernel(cfg, pre_ref, delta_ref, weight_ref, ids_ref, head_out, rest_out, embed_out, stat_out,
           pre_v, delta_v, low, weight_v, part, pair_in, line_in, first_in, swap_in, cross_in, sum_v, head_v,
           small, small_in, mine, span_in, span_part, span_pair, span_all, embed_all, ids_all,
           embed_v, rest_v, stat_all,
           pre_sem, delta_sem, weight_sem, out_sem, pair_send, pair_recv, line_send, line_recv,
           first_send, first_recv, swap_sem, cross_sem, head_send, head_recv, span_send, span_recv, span_pair_sem,
           all_send, all_recv, write_sem, embed_pair_sem, embed_send, embed_recv, ids_sem, ids_send, ids_recv,
           stat_send, stat_recv):
    n, heads, block, piece, spans, clients = cfg
    zs = n // 2
    q = 7
    sub = block // (q + 1)
    hq = block // piece
    rows, emit = low.shape
    half = emit // 2
    me = lax.axis_index("client")
    my_head = lax.axis_index("head")
    z = me // 2
    x = me % 2
    relays = (zs - 1) * q
    firsts = 2 * (zs - 1)
    slopes = 2 * zs * hq
    devices = n * heads
    flat = me * heads + my_head

    after_first = (z + zs - 1) // zs
    before_last = (2 * zs - 2 - z) // zs
    middle = after_first * before_last
    upper = 2 * z // zs
    near = z + upper * (zs - 1 - 2 * z)
    partner = z * 2 + 1 - x

    def wait_all(ref, sem):
        pltpu.make_async_copy(ref, ref, sem).wait()

    def send(src, dst, send_sem, recv_sem, client):
        return pltpu.make_async_remote_copy(
            src_ref=src, dst_ref=dst, send_sem=send_sem, recv_sem=recv_sem,
            device_id={"client": client}, device_id_type=MESH)

    def dest(k):
        both = (2 * near - k - 1 + zs) // zs
        odd = k % 2
        out = both * (odd * (k // 2) + (1 - odd) * (zs - 1 - k // 2)) + (1 - both) * (zs - 1 - k + near)
        return out + upper * (zs - 1 - 2 * out)

    def block_row(place, side):
        return (place * 2 + side) * block

    def piece_row(place, side, s):
        return pl.multiple_of(block_row(place, side) + (s + 1) * sub, sub)

    def landing(place):
        right = (place - z + zs) // zs
        target = z + 2 * right - 1
        gap = right * (place - target) + (1 - right) * (target - place)
        away = (gap + zs - 1) // zs
        slot = away * place + (1 - away) * (zs + 1 - right)
        sem = away * place + (1 - away) * (right * zs + (1 - right) * place)
        return target * 2 + x, slot, sem

    def unit_side(u):
        return (x + 1 - u % 2) % 2

    def unit_row(u):
        return pl.multiple_of(block_row(dest(u // 2), unit_side(u)), block)

    def pre_copy(u, h, sem):
        columns = pl.ds(pl.multiple_of(unit_row(u) + h * piece, piece), piece)
        return pltpu.make_async_copy(
            pre_ref.at[:, columns], pre_v.at[u, :, pl.ds(pl.multiple_of(h * piece, piece), piece)], pre_sem.at[sem])

    chunk = math.gcd(rows, 256)
    delta_copies = [
        pltpu.make_async_copy(delta_ref.at[pl.ds(c * chunk, chunk), :], delta_v.at[pl.ds(c * chunk, chunk), :],
                              delta_sem.at[c])
        for c in range(rows // chunk)]
    weight_copy = pltpu.make_async_copy(weight_ref, weight_v, weight_sem)
    ids_copy = pltpu.make_async_copy(ids_ref, ids_all.at[me], ids_sem)
    opened = min(128, piece)
    first_column = pl.multiple_of(unit_row(0), opened)
    rest_columns = piece - opened
    rest_copy = None
    if rest_columns > 0:
        rest_copy = pltpu.make_async_copy(
            pre_ref.at[:, pl.ds(pl.multiple_of(first_column + opened, opened), rest_columns)],
            pre_v.at[0, :, pl.ds(opened, rest_columns)], pre_sem.at[2])
    first_copies = [
        pltpu.make_async_copy(pre_ref.at[pl.ds(c * chunk, chunk), pl.ds(first_column, opened)],
                              pre_v.at[0, pl.ds(c * chunk, chunk), pl.ds(0, opened)], delta_sem.at[c])
        for c in range(rows // chunk)]
    for c in range(rows // chunk):
        first_copies[c].start()
        delta_copies[c].start()

    def each_other(action):
        columns = [lax.rem(my_head + d, heads) for d in range(heads - 1, -1, -1)]
        def body(j, carry):
            client = dest(j // 2) * 2 + unit_side(j)
            for column in columns:
                action(client, column)
            return carry
        for j in range(n - 1):
            body(j, 0)
        for column in columns[:-1]:
            action(me, column)

    barrier = pltpu.get_barrier_semaphore()
    def greet(client, head):
        pl.semaphore_signal(barrier, inc=1, device_id={"client": client, "head": head}, device_id_type=MESH)
    each_other(greet)

    def load(u, carry):
        pre_copy(u, 0, 0).start()
        return carry
    def load_rest(u, carry):
        @pl.when(u >= firsts)
        def _():
            pre_copy(u, 0, 1).start()
        for h in range(1, hq):
            pre_copy(u, h, 1).start()
        return carry

    def product(u, h):
        p = pre_v[u, :, pl.ds(pl.multiple_of(h * piece, piece), piece)].astype(F32)
        hidden = (p * jax.nn.sigmoid(p)).astype(BF16)
        value = lax.dot_general(hidden, low[...], (((0,), (0,)), ((), ())), preferred_element_type=F32)
        part[pl.ds(pl.multiple_of(unit_row(u) + h * piece, piece), piece), :] = value.astype(BF16)

    def slope_sums(t):
        u = t // hq
        h = t % hq
        p = pre_v[u, :, pl.ds(pl.multiple_of(h * piece, piece), piece)].astype(F32)
        row = pl.multiple_of(unit_row(u) + h * piece, piece)
        value = lax.dot_general(
            low[...], weight_v[pl.ds(row, piece), :], (((1,), (1,)), ((), ())), preferred_element_type=F32)
        s = jax.nn.sigmoid(p)
        grad = value.astype(BF16).astype(F32) * (s * (1.0 + p * (1.0 - s)))
        grad = grad.reshape(clients, spans, piece)
        to = row // emit
        columns = pl.ds(pl.multiple_of(row % emit, piece), piece)
        small[to, pl.ds(0, spans), columns] = jnp.sum(grad, axis=0).astype(BF16)
        small[to, pl.ds(spans, clients), columns] = jnp.sum(grad, axis=1).astype(BF16)

    def pair_copy(i):
        return send(part.at[pl.ds(piece_row(dest(i // q), 1 - x, i % q), sub), :], pair_in.at[i],
                    pair_send, pair_recv.at[i], partner)

    queue = 3 + middle
    cross = zs == 4
    swaps = 1 if cross else 0
    skip = q - 1

    def order(r):
        m = r - q
        late = swaps * middle * ((m + relays) // relays)
        return late * (q + m % 2 * q + m // 2) + (1 - late) * r

    def pairs_sent(r):
        late = swaps * middle * ((r - q + relays) // relays)
        return late * (2 * q + 3 + (r - q) // 2) + (1 - late) * (r + q + (2 + swaps) * middle)

    def line_copy(r):
        i = order(r)
        place = dest(i // q)
        target, slot, sem = landing(place)
        return send(part.at[pl.ds(piece_row(place, x, i % q), sub), :], line_in.at[slot * q + i % q],
                    line_send.at[r % queue], line_recv.at[sem * q + i % q], target)

    step_rows = min(64, sub)

    def start_pairs(start, stop):
        def body(i, carry):
            @pl.when((i < zs * q) & (swaps * middle * (skip + 1) != i + 1))
            def _():
                pair_copy(i).start()
            return carry
        lax.fori_loop(start, stop, body, 0)

    cross_copy = send(part.at[pl.ds(piece_row(dest(0), 1 - x, skip), sub), :], cross_in,
                      cross_sem.at[0], cross_sem.at[1], landing(dest(0))[0])

    def cross_add():
        row = piece_row(dest(1), 1 - x, skip)
        cross_copy.wait_recv()
        def add(r, carry):
            at = pl.ds(pl.multiple_of(r * step_rows, step_rows), step_rows)
            mine_at = pl.ds(pl.multiple_of(row + r * step_rows, step_rows), step_rows)
            part[mine_at, :] = (part[mine_at, :].astype(F32) + cross_in[at, :].astype(F32)).astype(BF16)
            return carry
        lax.fori_loop(0, sub // step_rows, add, 0)

    def relay(r, extra):
        i = order(r)
        place = dest(i // q)
        row = piece_row(place, x, i % q)
        @pl.when(swaps * middle * (skip + 1) != i + 1)
        def _():
            pair_copy(i).wait_recv()
        @pl.when(middle == 1)
        def _():
            wait_all(line_in.at[place * q + i % q], line_recv.at[place * q + i % q])
        slot = middle * (place * q + i % q) + (1 - middle) * z * q
        def add(r, carry):
            at = pl.ds(pl.multiple_of(r * step_rows, step_rows), step_rows)
            mine_at = pl.ds(pl.multiple_of(row + r * step_rows, step_rows), step_rows)
            total = part[mine_at, :].astype(F32) + pair_in[i, at, :].astype(F32)
            part[mine_at, :] = (total + line_in[slot, at, :].astype(F32)).astype(BF16)
            return carry
        lax.fori_loop(0, sub // step_rows, add, 0)
        @pl.when(r >= queue)
        def _():
            line_copy(r - queue).wait_send()
        line_copy(r).start()
        start_pairs(pairs_sent(r) + extra, pairs_sent(r + 1) + extra)

    def relay_range(start, stop, extra):
        def body(r, carry):
            relay(r, extra)
            return carry
        lax.fori_loop(start, stop, body, 0)

    def finish(s, square):
        i = relays + s
        row = piece_row(z, x, s)
        pair_copy(i).wait_recv()
        @pl.when(after_first == 1)
        def _():
            wait_all(line_in.at[zs * q + s], line_recv.at[zs * q + s])
        @pl.when(before_last == 1)
        def _():
            wait_all(line_in.at[(zs + 1) * q + s], line_recv.at[z * q + s])
        left = after_first * (zs * q + s) + (1 - after_first) * z * q
        right = before_last * ((zs + 1) * q + s) + (1 - before_last) * z * q
        def add(r, carry):
            at = pl.ds(pl.multiple_of(r * step_rows, step_rows), step_rows)
            mine_at = pl.ds(pl.multiple_of(row + r * step_rows, step_rows), step_rows)
            out_at = pl.ds(pl.multiple_of((s + 1) * sub + r * step_rows, step_rows), step_rows)
            total = part[mine_at, :].astype(F32) + pair_in[i, at, :].astype(F32)
            total = total + line_in[left, at, :].astype(F32) + line_in[right, at, :].astype(F32)
            head_v[out_at, :] = total.astype(BF16)
            return carry + jnp.sum((total * total).reshape(step_rows // 8, 8, emit), axis=0)
        square = lax.fori_loop(0, sub // step_rows, add, square)
        at = pl.ds(pl.multiple_of((s + 1) * sub, sub), sub)
        pltpu.make_async_copy(head_v.at[at, :], head_out.at[at, :], out_sem).start()
        return square

    def first_copy(j):
        place = dest(j // 2)
        side = unit_side(j)
        target, slot, sem = landing(place)
        return send(part.at[pl.ds(pl.multiple_of(block_row(place, side), sub), sub), :],
                    first_in.at[slot * 2 + side], first_send, first_recv.at[sem * 2 + side], target)

    def first_relay(j):
        @pl.when(middle == 1)
        def _():
            place = dest(j // 2)
            side = unit_side(j)
            row = pl.multiple_of(block_row(place, side), sub)
            wait_all(first_in.at[place * 2 + side], first_recv.at[place * 2 + side])
            def add(r, carry):
                at = pl.ds(pl.multiple_of(r * step_rows, step_rows), step_rows)
                mine_at = pl.ds(pl.multiple_of(row + r * step_rows, step_rows), step_rows)
                part[mine_at, :] = (
                    part[mine_at, :].astype(F32) + first_in[place * 2 + side, at, :].astype(F32)).astype(BF16)
                return carry
            lax.fori_loop(0, sub // step_rows, add, 0)
            first_copy(j).start()

    swap_copy = send(part.at[pl.ds(pl.multiple_of(block_row(z, 1 - x), sub), sub), :], swap_in,
                     swap_sem.at[0], swap_sem.at[1], partner)

    def first_wait(side):
        @pl.when(after_first == 1)
        def _():
            wait_all(first_in.at[zs * 2 + side], first_recv.at[zs * 2 + side])
        @pl.when(before_last == 1)
        def _():
            wait_all(first_in.at[(zs + 1) * 2 + side], first_recv.at[z * 2 + side])
        left = after_first * (zs * 2 + side) + (1 - after_first) * z * 2
        right = before_last * ((zs + 1) * 2 + side) + (1 - before_last) * z * 2
        return left, right

    def first_swap():
        row = block_row(z, 1 - x)
        left, right = first_wait(1 - x)
        def add(r, carry):
            at = pl.ds(pl.multiple_of(r * step_rows, step_rows), step_rows)
            mine_at = pl.ds(pl.multiple_of(row + r * step_rows, step_rows), step_rows)
            total = part[mine_at, :].astype(F32) + first_in[left, at, :].astype(F32)
            part[mine_at, :] = (total + first_in[right, at, :].astype(F32)).astype(BF16)
            return carry
        lax.fori_loop(0, sub // step_rows, add, 0)
        swap_copy.start()

    def first_finish(square):
        row = block_row(z, x)
        left, right = first_wait(x)
        swap_copy.wait_recv()
        def add(r, carry):
            at = pl.ds(pl.multiple_of(r * step_rows, step_rows), step_rows)
            mine_at = pl.ds(pl.multiple_of(row + r * step_rows, step_rows), step_rows)
            total = part[mine_at, :].astype(F32) + first_in[left, at, :].astype(F32)
            total = total + first_in[right, at, :].astype(F32) + swap_in[at, :].astype(F32)
            head_v[at, :] = total.astype(BF16)
            return carry + jnp.sum((total * total).reshape(step_rows // 8, 8, emit), axis=0)
        square = lax.fori_loop(0, sub // step_rows, add, square)
        pltpu.make_async_copy(head_v.at[pl.ds(0, sub), :], head_out.at[pl.ds(0, sub), :], out_sem).start()
        return square

    if rest_columns > 0:
        rest_copy.start()
    lax.fori_loop(1, firsts, load, 0)
    step = 64
    for c in range(rows // chunk):
        wait_all(delta_v.at[pl.ds(0, chunk + chunk * opened // (2 * emit)), :], delta_sem.at[c])
        def narrow(r, carry):
            at = pl.ds(pl.multiple_of(c * chunk + r * step, step), step)
            low[at, :] = delta_v[at, :].astype(BF16)
            return carry
        lax.fori_loop(0, chunk // step, narrow, 0)
        at = pl.ds(c * chunk, chunk)
        p = pre_v[0, at, pl.ds(0, opened)].astype(F32)
        hidden = (p * jax.nn.sigmoid(p)).astype(BF16)
        value = lax.dot_general(hidden, low[at, :], (((0,), (0,)), ((), ())), preferred_element_type=F32)
        if c > 0:
            value = value + sum_v[...]
        if c < len(delta_copies) - 1:
            sum_v[...] = value
        else:
            part[pl.ds(pl.multiple_of(unit_row(0), opened), opened), :] = value.astype(BF16)

    pl.semaphore_wait(barrier, devices - 1)

    ready = min(piece // sub - 1, q)
    soon = min(opened // sub - 1, q)
    @pl.when(middle == 0)
    def _():
        first_copy(0).start()
    for i in range(soon):
        pair_copy(i).start()
    if rest_columns > 0:
        rest_copy.wait()
        p = pre_v[0, :, pl.ds(opened, rest_columns)].astype(F32)
        hidden = (p * jax.nn.sigmoid(p)).astype(BF16)
        value = lax.dot_general(hidden, low[...], (((0,), (0,)), ((), ())), preferred_element_type=F32)
        part[pl.ds(pl.multiple_of(unit_row(0) + opened, opened), rest_columns), :] = value.astype(BF16)
    for i in range(soon, ready):
        pair_copy(i).start()
    lax.fori_loop(0 if hq > 1 else firsts, 2 * zs, load_rest, 0)
    weight_copy.start()
    ids_copy.start()
    line_in[z * q] = jnp.zeros((sub, emit), BF16)
    first_in[z * 2] = jnp.zeros((sub, emit), BF16)

    wait_all(pre_v.at[pl.ds(0, firsts - 1), :, pl.ds(0, piece)], pre_sem.at[0])
    def opening(u, carry):
        product(u, 0)
        @pl.when(middle == 0)
        def _():
            first_copy(u).start()
        return carry
    lax.fori_loop(1, firsts, opening, 0)
    wait_all(pre_v.at[pl.ds(0, (2 * zs * hq - firsts) // hq)], pre_sem.at[1])
    if hq > 1:
        def second(t, carry):
            product(t // (hq - 1), 1 + t % (hq - 1))
            return carry
        lax.fori_loop(0, 3 * (hq - 1), second, 0)
    if cross:
        @pl.when(middle == 1)
        def _():
            pair_in[skip] = jnp.zeros((sub, emit), BF16)
            cross_copy.start()
    start_pairs(ready, pairs_sent(0))
    first_relay(0)
    first_relay(1)
    weight_copy.wait()

    ids_copy.wait()
    for d in range(1, n):
        send(ids_all.at[me], ids_all.at[me], ids_send, ids_recv, lax.rem(me + d, n)).start()

    base = 3 + middle * (slopes - 8)
    stride = 3 - middle
    def main(t, carry):
        slope_sums(t)
        @pl.when((t >= 4) & (t % 2 == 0) & (t // 2 < firsts))
        def _():
            first_relay(t // 2)
        @pl.when((t >= base) & ((t - base) % stride == 0))
        def _():
            relay((t - base) // stride, 0)
        return carry
    lax.fori_loop(0, slopes, main, 0)

    for d in range(1, heads):
        target = lax.rem(my_head + d, heads)
        pltpu.make_async_remote_copy(
            src_ref=small.at[target], dst_ref=small_in.at[lax.rem(my_head - target + heads, heads) - 1],
            send_sem=head_send, recv_sem=head_recv, device_id={"head": target}, device_id_type=MESH).start()

    if cross:
        @pl.when(middle == 1)
        def _():
            cross_add()

    done = slopes // 2
    if done < firsts:
        def rest_first(j, carry):
            first_relay(j)
            return carry
        lax.fori_loop(done, firsts, rest_first, 0)

    def add_rows(r, total):
        value = delta_v[pl.ds(pl.multiple_of(r * step, step), step), :]
        return total + jnp.sum(value.reshape(step // 8, 8, emit), axis=0)
    bias = lax.fori_loop(0, rows // step, add_rows, jnp.zeros((8, emit), F32))
    bias = jnp.sum(bias, axis=0, keepdims=True)
    pad = mine.shape[1] - spans
    tail = jnp.where(
        lax.broadcasted_iota(jnp.int32, (pad, emit), 0) == 0, jnp.broadcast_to(bias, (pad, emit)), 0.0
    ).astype(BF16)
    for h in range(2):
        mine[h, pl.ds(spans, pad), :] = tail[:, h * half:(h + 1) * half]

    ends = [(slopes - 4) // 3 + 1] + [(slopes - 4) // 3 + 1 + k for k in (2, 4, 4, 8, 13, 16)]
    inner = [3] + [3 + k for k in (1, 2, 3, 8, 15, 18)]
    stops = [(1 - middle) * e + middle * i for e, i in zip(ends, inner)] + [relays]

    if hq > 1:
        def third(t, carry):
            product(3 + t // (hq - 1), 1 + t % (hq - 1))
            return carry
        lax.fori_loop(0, (2 * zs - 5) * (hq - 1), third, 0)
    relay_range(stops[0], stops[1], 0)
    def fourth(t, carry):
        product(2 * zs - 2 + t // hq, t % hq)
        return carry
    lax.fori_loop(0, 2 * hq, fourth, 0)
    relay_range(stops[1], stops[2], 0)
    relay_range(stops[2], stops[3], 0)

    wait_all(small_in, head_recv)
    total = small[my_head].astype(F32)
    for d in range(heads - 1):
        total = total + small_in[d].astype(F32)
    for h in range(2):
        mine[h, pl.ds(0, spans), :] = total[:spans, h * half:(h + 1) * half].astype(BF16)
    embed_all[z, x] = total[spans:].astype(BF16)

    embed_pair = send(embed_all.at[z, x], embed_all.at[z, x], embed_pair_sem.at[0], embed_pair_sem.at[1], partner)
    embed_pair.start()

    roots = [zs // 2 - 1, zs // 2]
    def span_copy(h, right):
        return send(mine.at[h], span_in.at[h, 1 - right], span_send.at[h], span_recv.at[2 * h + 1 - right],
                    (z + 2 * right - 1) * 2 + x)
    def span_arrival(h, side):
        wait_all(span_in.at[h, side], span_recv.at[2 * h + side])
    for h in range(2):
        @pl.when(z == 0)
        def _():
            if roots[h] != 0:
                span_copy(h, 1).start()
        @pl.when(z == zs - 1)
        def _():
            if roots[h] != zs - 1:
                span_copy(h, 0).start()

    start_pairs(pairs_sent(stops[3]), pairs_sent(stops[3]) + middle)
    relay_range(stops[3], stops[4], middle)

    def embed_copy(j, right):
        source = z + j - 2 * right * j
        return send(embed_all.at[source], embed_all.at[source], embed_send.at[right], embed_recv.at[source],
                    (z + 2 * right - 1) * 2 + x)

    def embed_step(j):
        for right, near_end, there in ((1, before_last, z - j >= 0), (0, after_first, z + j <= zs - 1)):
            @pl.when((near_end == 1) & there)
            def _():
                if j > 0:
                    source = z + j - 2 * right * j
                    wait_all(embed_all.at[source], embed_recv.at[source])
                    embed_copy(j - 1, right).wait_send()
                embed_copy(j, right).start()

    embed_pair.wait_recv()
    for h in range(2):
        for right, between in ((1, (z > 0) & (z < roots[h])), (0, (z < zs - 1) & (z > roots[h]))):
            @pl.when(between)
            def _():
                span_arrival(h, 1 - right)
                mine[h] = (mine[h].astype(F32) + span_in[h, 1 - right].astype(F32)).astype(BF16)
                span_copy(h, right).start()
    embed_step(0)

    relay_range(stops[4], stops[5], middle)

    span_pair_copy = send(span_part, span_pair, span_pair_sem.at[0], span_pair_sem.at[1], partner)
    for h in range(2):
        @pl.when(z == roots[h])
        def _():
            total = mine[h].astype(F32)
            for side, there in ((0, roots[h] > 0), (1, roots[h] < zs - 1)):
                if there:
                    span_arrival(h, side)
                    total = total + span_in[h, side].astype(F32)
            span_part[...] = total.astype(BF16)
            span_pair_copy.start()
    first_swap()
    embed_step(1)

    start_pairs(pairs_sent(stops[5]) + middle, pairs_sent(stops[5]) + 3 * middle)
    relay_range(stops[5], stops[6], 3 * middle)

    def all_copy(h, d):
        return send(span_all.at[h], span_all.at[h], all_send, all_recv.at[h], lax.rem(z + d, zs) * 2 + x)
    for h in range(2):
        @pl.when(z == roots[h])
        def _():
            span_pair_copy.wait_recv()
            span_all[h] = (span_part[...].astype(F32) + span_pair[...].astype(F32)).astype(BF16)
            for d in range(1, zs):
                all_copy(h, d).start()
    for j in range(2, zs - 1):
        embed_step(j)

    relay_range(stops[6], stops[7], 3 * middle)
    start_pairs(pairs_sent(relays) + 3 * middle, zs * q)
    square = jnp.zeros((8, emit), F32)
    square = first_finish(square)
    square = lax.fori_loop(0, 5, finish, square)

    for j in range(1, zs):
        for right, near_end, there in ((1, before_last, z - j >= 0), (0, after_first, z + j <= zs - 1)):
            source = z + j - 2 * right * j
            @pl.when(there if j == zs - 1 else (near_end == 0) & there)
            def _():
                wait_all(embed_all.at[source], embed_recv.at[source])
    for right, near_end, last in ((1, before_last, z), (0, after_first, zs - 1 - z)):
        for j in range(zs - 1):
            @pl.when((near_end == 1) & (last == j))
            def _():
                embed_copy(j, right).wait_send()
    wait_all(ids_all.at[pl.ds(0, n - 1)], ids_recv)
    wanted = lax.broadcasted_iota(jnp.int32, (clients, clients), 0) + me * clients
    embed_raw = jnp.zeros((clients, emit), F32)
    for c in range(n):
        chosen = (jnp.broadcast_to(ids_all[c], (clients, clients)) == wanted).astype(F32).astype(BF16)
        embed_raw = embed_raw + jnp.dot(chosen, embed_all[c // 2, c % 2], preferred_element_type=F32)
    embed_v[...] = embed_raw
    embed_write = pltpu.make_async_copy(embed_v, embed_out, write_sem.at[0])
    embed_write.start()
    embed_square = jnp.sum(embed_raw * embed_raw)

    rest_square = jnp.zeros((), F32)
    for h in range(2):
        @pl.when(z != roots[h])
        def _():
            wait_all(span_all.at[h], all_recv.at[h])
        value = span_all[h].astype(F32)
        rest_v[:, pl.ds(h * half, half)] = value
        rest_square = rest_square + jnp.sum(value * value)
    rest_write = pltpu.make_async_copy(rest_v, rest_out, write_sem.at[1])
    rest_write.start()

    square = lax.fori_loop(5, q, finish, square)
    head_total = jnp.sum(square)

    lane = lax.broadcasted_iota(jnp.int32, (1, 128), 1)
    stat_all[flat] = jnp.where(lane == 0, head_total, jnp.where(lane == 1, embed_square, rest_square / n))
    def tell(client, head):
        pltpu.make_async_remote_copy(
            src_ref=stat_all.at[flat], dst_ref=stat_all.at[flat], send_sem=stat_send, recv_sem=stat_recv,
            device_id={"client": client, "head": head}, device_id_type=MESH).start()
    each_other(tell)

    @pl.when(swaps * middle == 0)
    def _():
        wait_all(part.at[pl.ds(0, zs * q * sub)], pair_send)
    if cross:
        @pl.when(middle == 1)
        def _():
            wait_all(part.at[pl.ds(0, (zs * q - 1) * sub)], pair_send)
            cross_copy.wait_send()
    def line_sent(r, carry):
        line_copy(r).wait_send()
        return carry
    lax.fori_loop(relays - queue, relays, line_sent, 0)
    wait_all(part.at[pl.ds(0, firsts * sub)], first_send)
    swap_copy.wait_send()
    embed_pair.wait_send()
    wait_all(small.at[pl.ds(0, heads - 1)], head_send)
    wait_all(ids_all.at[pl.ds(0, n - 1)], ids_send)
    for h in range(2):
        @pl.when(z < roots[h])
        def _():
            span_copy(h, 1).wait_send()
        @pl.when(z > roots[h])
        def _():
            span_copy(h, 0).wait_send()
        @pl.when(z == roots[h])
        def _():
            span_pair_copy.wait_send()
            wait_all(part.at[pl.ds(0, (zs - 1) * mine.shape[1] // 2)], all_send)
    embed_write.wait()
    rest_write.wait()
    pltpu.make_async_copy(head_v, head_out, out_sem).wait()

    wait_all(stat_all.at[pl.ds(0, devices - 1)], stat_recv)
    stat_out[...] = jnp.sum(stat_all[...], axis=0)
    wait_all(stat_all.at[pl.ds(0, devices - 1)], stat_send)


def scale_kernel(sizes, stat_ref, head_ref, rest_ref, embed_ref, head_out, bias_out, embed_out, span_out,
                 stat, head_in, head, rest, embed, in_sem, out_sem):
    head_size, embed_size, rest_size = sizes
    spans = span_out.shape[0]
    steps = in_sem.shape[0] - 3
    rows = head.shape[0] // steps
    stat_in = pltpu.make_async_copy(stat_ref, stat, in_sem.at[steps])
    rest_in = pltpu.make_async_copy(rest_ref, rest, in_sem.at[steps + 1])
    embed_in = pltpu.make_async_copy(embed_ref, embed, in_sem.at[steps + 2])
    def part(ref, i):
        return ref.at[pl.ds(i * rows, rows), :]
    stat_in.start()
    heads_in = [pltpu.make_async_copy(part(head_ref, i), part(head_in, i), in_sem.at[i]) for i in range(steps)]
    heads_out = [pltpu.make_async_copy(part(head, i), part(head_out, i), out_sem.at[i]) for i in range(steps)]
    for copy in heads_in:
        copy.start()
    rest_in.start()
    embed_in.start()
    stat_in.wait()
    factor = clip_factor(stat[0:1, 0:1], head_size)
    embed_factor = clip_factor(stat[0:1, 1:2], embed_size)
    rest_factor = clip_factor(stat[0:1, 2:3], rest_size)
    for i in range(steps):
        heads_in[i].wait()
        head[pl.ds(i * rows, rows), :] = factor * head_in[pl.ds(i * rows, rows), :].astype(F32)
        heads_out[i].start()
    rest_in.wait()
    rest[...] = rest_factor * rest[...]
    bias_copy = pltpu.make_async_copy(rest.at[pl.ds(spans, 1), :], bias_out, out_sem.at[steps])
    span_copy = pltpu.make_async_copy(rest.at[pl.ds(0, spans), :], span_out, out_sem.at[steps + 1])
    bias_copy.start()
    span_copy.start()
    embed_in.wait()
    embed[...] = embed_factor * embed[...]
    embed_copy = pltpu.make_async_copy(embed, embed_out, out_sem.at[steps + 2])
    embed_copy.start()
    for copy in heads_out + [bias_copy, span_copy, embed_copy]:
        copy.wait()


def per_device(n, heads, pre, delta, head_weight, client_ids):
    rows, hidden_width = pre.shape
    emit = delta.shape[1]
    clients = client_ids.shape[0]
    spans = rows // clients
    block = hidden_width // n
    piece = min(256, block)
    hq = block // piece
    zs = n // 2
    q = 7
    sub = block // (q + 1)
    padded = (spans + 16) // 16 * 16
    half = emit // 2
    cfg = (n, heads, block, piece, spans, clients)
    ids = client_ids.reshape(1, clients)
    hbm = pl.BlockSpec(memory_space=pl.ANY)
    vmem = pl.BlockSpec(memory_space=pltpu.VMEM)
    dma = pltpu.SemaphoreType.DMA
    chunk = math.gcd(rows, 256)
    head_raw, rest_raw, embed_raw, stats = pl.pallas_call(
        functools.partial(kernel, cfg),
        out_shape=(
            jax.ShapeDtypeStruct((block, emit), BF16),
            jax.ShapeDtypeStruct((padded, emit), F32),
            jax.ShapeDtypeStruct((clients, emit), F32),
            jax.ShapeDtypeStruct((1, 128), F32),
        ),
        in_specs=[hbm, hbm, hbm, hbm],
        out_specs=(hbm, hbm, hbm, vmem),
        scratch_shapes=[
            pltpu.VMEM((n, rows, block), BF16),
            pltpu.VMEM((rows, emit), F32),
            pltpu.VMEM((rows, emit), BF16),
            pltpu.VMEM((hidden_width, emit), BF16),
            pltpu.VMEM((hidden_width, emit), BF16),
            pltpu.VMEM((zs * q, sub, emit), BF16),
            pltpu.VMEM(((zs + 2) * q, sub, emit), BF16),
            pltpu.VMEM(((zs + 2) * 2, sub, emit), BF16),
            pltpu.VMEM((sub, emit), BF16),
            pltpu.VMEM((sub, emit), BF16),
            pltpu.VMEM((min(128, piece), emit), F32),
            pltpu.VMEM((block, emit), BF16),
            pltpu.VMEM((heads, spans + clients, emit), BF16),
            pltpu.VMEM((heads - 1, spans + clients, emit), BF16),
            pltpu.VMEM((2, padded, half), BF16),
            pltpu.VMEM((2, 2, padded, half), BF16),
            pltpu.VMEM((padded, half), BF16),
            pltpu.VMEM((padded, half), BF16),
            pltpu.VMEM((2, padded, half), BF16),
            pltpu.VMEM((zs, 2, clients, emit), BF16),
            pltpu.VMEM((n, 1, clients), jnp.int32),
            pltpu.VMEM((clients, emit), F32),
            pltpu.VMEM((padded, emit), F32),
            pltpu.VMEM((n * heads, 1, 128), F32),
            dma((3,)), dma((rows // chunk,)), dma, dma,
            dma, dma((zs * q,)), dma((4,)), dma(((zs + 1) * q,)),
            dma, dma(((zs + 1) * 2,)), dma((2,)), dma((2,)), dma, dma,
            dma((2,)), dma((4,)), dma((2,)), dma, dma((2,)), dma((2,)), dma((2,)), dma((2,)), dma((zs,)),
            dma, dma, dma, dma, dma,
        ],
        compiler_params=pltpu.CompilerParams(
            collective_id=0, has_side_effects=True, vmem_limit_bytes=62 * 2**20
        ),
        name="clipped_grads",
    )(pre, delta, head_weight, ids)
    sizes = (hidden_width * emit * heads, clients * n * hidden_width, spans * hidden_width + emit * heads)
    steps = 2
    head_grad, bias_grad, embed_grad, span_grad = pl.pallas_call(
        functools.partial(scale_kernel, sizes),
        out_shape=(
            jax.ShapeDtypeStruct((block, emit), F32),
            jax.ShapeDtypeStruct((1, emit), F32),
            jax.ShapeDtypeStruct((clients, emit), F32),
            jax.ShapeDtypeStruct((spans, emit), F32),
        ),
        in_specs=[hbm] * 4,
        out_specs=(hbm,) * 4,
        scratch_shapes=[
            pltpu.VMEM((1, 128), F32),
            pltpu.VMEM((block, emit), BF16),
            pltpu.VMEM((block, emit), F32),
            pltpu.VMEM((padded, emit), F32),
            pltpu.VMEM((clients, emit), F32),
            dma((steps + 3,)), dma((steps + 3,)),
        ],
        name="scaled",
    )(stats, head_raw, rest_raw, embed_raw)
    return head_grad, bias_grad.reshape(emit), embed_grad, span_grad


def solution(mesh):
    placed = (P("client", None), P("client", "head"), P(None, "head"), P("client"))
    return jax.shard_map(
        functools.partial(per_device, mesh.shape["client"], mesh.shape["head"]),
        mesh=mesh,
        in_specs=placed,
        out_specs=(P("client", "head"), P("head"), P("client", "head"), P(None, "head")),
        check_vma=False,
    )
```
